128 devices in a mesh: gx: 32 (over z, x, core), gy: 4 (over y).
Axes of the slice: x: 4, y: 4, z: 4, core: 2. Of those that a mesh axis runs over, the one named last changes fastest.
Arguments:
- right_side: float32 [192, 64, 16, 128], P(None, 'gx', 'gy'), may hold values from -6 to 6
- coefficient: float32 [64, 16, 128], P('gx', 'gy'), may hold values from 0.5 to 2
- orientation: int32 [6, 64, 16, 128], P(None, 'gx', 'gy'), may hold values from 0 to 1
- aggregate_map: int32 [64, 16, 128], P('gx', 'gy'), may hold values from 0 to 511
- owner_map: int32 [65536, 1], P(('gx', 'gy')), may hold values from 0 to 31; in each aligned block of 512 rows (0 to 511, 512 to 1023, ...) at most 32 rows name the same one
- stiffness: float32 [192, 192], replicated, may hold values from -1 to 2
- face_blocks: float32 [6, 2, 192, 48], replicated, may hold values from -0.21875 to 0.21875
- prolong_basis: float32 [192, 24], replicated, may hold values from -0.4375 to 0.4375
- coarse_inverse: float32 [128, 32, 32, 24, 24], P(('gx', 'gy')), may hold values from -3 to 3
Outputs:
- solution_field: float32 [192, 64, 16, 128], P(None, 'gx', 'gy')
- residual: float32 [192, 64, 16, 128], P(None, 'gx', 'gy')
The draws below stay inside these ranges and needn't reach their ends.
Inputs may be any that keep to these rules, and one draw needn't show every extreme that they name: `aggregate_map`: each value names an aggregate of the element's own device. `owner_map`: among the aggregates of one device (aligned blocks of 512 rows) no owner is named more than 32 times, a bound that some block reaches.
All inputs are finite; a program needn't handle non-finite values.
Results may differ from the reference program's by a relative error of at most 0.00011.
Values sent between devices are 32-bit elements; how exact they have to be, the bound alone decides.
No kernel may reach another device: no remote copies, remote signals or barrier semaphores. Data moves between devices by JAX's collectives and lax.ppermute only.
A program may use at most 128 MiB of HBM per device.

```python
import math
import jax
import jax.numpy as jnp
import numpy as np
from jax import lax

BLOCK = 192
TRACE = 48
CW = 24
DEGREE = 3
EX = 2
EY = 4
EZ = 128
AGG_DEV = 512
CAP = 32
NX = 64
NY = 16
AGGS = 65536
N_GX = 32
N_GY = 4
DEVICES = 128


def unit_noise(key, shape):
    return jnp.clip(jax.random.normal(key, shape, jnp.float32), -6.0, 6.0)


def draw_stiffness(key, part):
    noise = unit_noise(jax.random.fold_in(key, 11), (BLOCK, BLOCK))
    return jnp.eye(BLOCK, dtype=jnp.float32) + 0.3 * noise / jnp.sqrt(jnp.float32(BLOCK))


def draw_coarse_inverse(key, part):
    shape = (DEVICES, N_GX, CAP, CW, CW)
    noise = unit_noise(jax.random.fold_in(key, 23), shape)
    logs = jax.random.uniform(jax.random.fold_in(key, 29), (DEVICES, N_GX, CAP, CW, 1), jnp.float32, -0.69, 0.69)
    return jnp.exp(logs) * (jnp.eye(CW, dtype=jnp.float32) + 0.25 * noise / jnp.sqrt(jnp.float32(CW)))


def with_ends(drawn, stream_key, least, high):
    longest = drawn.shape.index(max(drawn.shape))
    spots = []
    for shift in (0, 1):
        where = [jax.random.randint(jax.random.fold_in(stream_key, axis), (), 0, length) for axis, length in enumerate(drawn.shape)]
        where[longest] = (where[longest] + shift) % drawn.shape[longest]
        spots.append(tuple(where))
    return drawn.at[spots[0]].set(least).at[spots[1]].set(high)


def levels(own_key, extent, cuts, least, top_value):
    level = 1.0
    for axis_at, shards_of in cuts:
        heights = jax.random.uniform(jax.random.fold_in(jax.random.fold_in(own_key, 6), axis_at), (shards_of,), jnp.float32, least / len(cuts), top_value / len(cuts))
        level = level * jnp.repeat(jnp.exp(heights), extent[axis_at] // shards_of).reshape((-1,) + (1,) * (len(extent) - 1 - axis_at))
    return level


def routed_block(own_key, own, number, rows, number_of, top, bound, skew):
    sequence = jax.random.permutation(own_key, number_of)
    crowded, ordinary = shares(number_of, rows * top, bound, skew, True), shares(number_of, rows * top, bound, skew, False)
    places = jnp.arange(number_of)

    def named(tallies, turn):
        used = int((tallies > 0).sum())
        fixed = max(1, used // 4)
        passed = fixed + (places - fixed + turn * (used - fixed)) % max(1, number_of - fixed)
        return jnp.zeros((number_of,), jnp.int32).at[sequence[jnp.where(places < fixed, places, passed)]].set(jnp.asarray(tallies, jnp.int32))

    tallies = jnp.where(number % 4 == 0, named(crowded, number // 4), named(ordinary, number - number // 4 - 1))
    mixed = jax.random.permutation(jax.random.fold_in(own, 3), number_of)
    giver, receiver = mixed[0:number_of // 2 * 2:2], mixed[1:number_of // 2 * 2:2]
    slack = jnp.minimum(tallies[giver] - 1, bound - tallies[receiver]) // 2
    slack = jnp.where((giver == sequence[0]) | (receiver == sequence[0]) | (tallies[receiver] == 0), 0, jnp.maximum(slack, 0))
    passed = jax.random.randint(jax.random.fold_in(own, 4), (number_of // 2,), 0, 1 << 20) % (slack + 1)
    tallies = tallies.at[giver].add(-passed).at[receiver].add(passed)
    items = jnp.searchsorted(jnp.cumsum(tallies), jnp.arange(rows * top), side="right").astype(jnp.int32)
    listing = items.reshape(top, rows).T
    listing = listing[jax.random.permutation(jax.random.fold_in(own, 1), rows)]
    turn = jax.random.randint(jax.random.fold_in(own, 2), (rows, 1), 0, top)
    return jnp.take_along_axis(listing, (jnp.arange(top)[None, :] + turn) % top, axis=1)


def shares(count, total, limit, skew, full):
    loads = [(1 << 20) // math.isqrt(standing ** skew) + 1 for standing in range(1, count + 1)]
    largest = limit if full else min(limit, max(-(-total // count), total * loads[0] // sum(loads)))
    least = 1 if total - largest >= count - 1 else 0
    holding, rest = [largest] + [least] * (count - 1), total - largest - least * (count - 1)
    while rest > 0:
        candidates = [i for i in range(1, count) if holding[i] < largest] or [i for i in range(1, count) if holding[i] < limit]
        whole, budget = sum([loads[i] for i in candidates]), rest
        for i in candidates:
            extra = min(limit - holding[i], max(1, budget * loads[i] // whole), rest)
            holding[i] = holding[i] + extra
            rest = rest - extra
    return np.array(holding)


def bell_draw(key, extent, scale, reach, cuts=(), kind=jnp.bfloat16):
    loudness = levels(key, extent, cuts, -0.22, 0.18) if cuts else 1.0
    drawn = jax.random.normal(key, extent, jnp.float32) * scale * loudness
    return jnp.minimum(jnp.maximum(drawn, -reach), reach).astype(kind)


def setup_inputs(seed: int = 0) -> dict:
    splits = jax.random.split(jax.random.key(seed), 10)
    right_side = bell_draw(splits[0], (BLOCK, NX, NY, EZ), 1.0, 6.0, ((1, 32), (2, 4)), jnp.float32)
    coefficient = jnp.clip(jnp.exp(math.log(2.0) - 1.3862944 * jax.random.uniform(splits[1], (NX, NY, EZ), jnp.float32) ** levels(splits[1], (NX, NY, EZ), ((0, 32), (1, 4)), -0.2, 0.2)), 0.5, 2.0)
    orientation = with_ends(jax.random.randint(splits[2], (6, NX, NY, EZ), 0, 2), jax.random.fold_in(splits[2], 1), 0, 1).astype(jnp.int32)
    aggregate_map = with_ends(jax.random.randint(splits[3], (NX, NY, EZ), 0, AGG_DEV), jax.random.fold_in(splits[3], 1), 0, AGG_DEV - 1).astype(jnp.int32)
    owner_map_keys = jax.random.split(jax.random.fold_in(splits[4], 1), AGGS // AGG_DEV)
    owner_map_turns = jax.random.permutation(jax.random.fold_in(splits[4], 3), AGGS // AGG_DEV)
    owner_map = jax.vmap(lambda own, number: routed_block(jax.random.fold_in(splits[4], 2), own, number, AGG_DEV, N_GX, 1, CAP, 2))(owner_map_keys, owner_map_turns).reshape((AGGS, 1))
    stiffness = draw_stiffness(jax.random.fold_in(splits[9], 71), 0)
    face_blocks = bell_draw(splits[6], (6, 2, BLOCK, TRACE), (16 * TRACE) ** -0.5, 0.21875, (), jnp.float32)
    prolong_basis = bell_draw(splits[7], (BLOCK, CW), BLOCK ** -0.5, 0.4375, (), jnp.float32)
    coarse_inverse = draw_coarse_inverse(jax.random.fold_in(splits[9], 71), 0)
    return dict(right_side=right_side, coefficient=coefficient, orientation=orientation, aggregate_map=aggregate_map, owner_map=owner_map, stiffness=stiffness, face_blocks=face_blocks, prolong_basis=prolong_basis, coarse_inverse=coarse_inverse)


low_bound = 0.25
high_bound = 4.0


def shifted(t, axis, forward):
    pads = [(0, 0)] * t.ndim
    if forward:
        pads[axis] = (1, 0)
        return lax.slice_in_dim(jnp.pad(t, pads), 0, t.shape[axis], axis=axis)
    pads[axis] = (0, 1)
    return lax.slice_in_dim(jnp.pad(t, pads), 1, t.shape[axis] + 1, axis=axis)


def operate(field, coefficient, orientation, stiffness, face_blocks):
    size_x, size_y, size_z = field.shape[1:]
    scaled = field * coefficient[None]
    nodes = scaled.reshape(3, 4, 4, 4, size_x, size_y, size_z)

    def flat(t):
        return t.reshape(48, size_x, size_y, size_z)

    neighbours = [
        shifted(flat(nodes[:, 3]), 1, True),
        shifted(flat(nodes[:, 0]), 1, False),
        shifted(flat(nodes[:, :, 3]), 2, True),
        shifted(flat(nodes[:, :, 0]), 2, False),
        shifted(flat(nodes[:, :, :, 3]), 3, True),
        shifted(flat(nodes[:, :, :, 0]), 3, False),
    ]
    result = jnp.dot(stiffness, scaled.reshape(192, -1), precision=lax.Precision.HIGHEST)
    for direction in range(6):
        pairs = face_blocks[direction].reshape(384, 48)
        both = jnp.dot(pairs, neighbours[direction].reshape(48, -1), precision=lax.Precision.HIGHEST)
        pick = orientation[direction].reshape(1, -1) == 1
        result = result + jnp.where(pick, both[192:], both[:192])
    return result.reshape(field.shape)


def smooth(state, resid, apply_op):
    theta = 0.5 * (high_bound + low_bound)
    delta = 0.5 * (high_bound - low_bound)
    sigma = theta / delta
    rho = 1.0 / sigma
    step_dir = resid / theta
    state = state + step_dir
    resid = resid - apply_op(step_dir)
    for turn in range(DEGREE - 1):
        rho_new = 1.0 / (2.0 * sigma - rho)
        step_dir = (rho_new * rho) * step_dir + (2.0 * rho_new / delta) * resid
        rho = rho_new
        state = state + step_dir
        resid = resid - apply_op(step_dir)
    return state, resid


def reference(right_side, coefficient, orientation, aggregate_map, owner_map, stiffness, face_blocks, prolong_basis, coarse_inverse):
    def apply_op(v):
        return operate(v, coefficient, orientation, stiffness, face_blocks)

    state, resid = smooth(jnp.zeros_like(right_side), right_side, apply_op)
    device_of = (jnp.arange(NX, dtype=jnp.int32) // EX)[:, None, None] * N_GY + (jnp.arange(NY, dtype=jnp.int32) // EY)[None, :, None]
    device_of = device_of + jnp.zeros((NX, NY, EZ), jnp.int32)
    global_agg = (device_of * AGG_DEV + aggregate_map).reshape(-1).astype(jnp.int32)
    projected = jnp.dot(prolong_basis.T, resid.reshape(192, -1), precision=lax.Precision.HIGHEST)
    coarse_rhs = jax.ops.segment_sum(projected.T, global_agg, num_segments=AGGS)
    owners = owner_map[:, 0].reshape(DEVICES, AGG_DEV)
    hot = (owners[:, :, None] == jnp.arange(N_GX, dtype=jnp.int32)[None, None, :]).astype(jnp.int32)
    before = jnp.cumsum(hot, axis=1) - hot
    slot = jnp.sum(before * hot, axis=2).reshape(-1).astype(jnp.int32)
    owner_flat = owners.reshape(-1)
    agg_device = jnp.arange(AGGS, dtype=jnp.int32) // AGG_DEV
    source = agg_device // N_GY
    row_index = agg_device % N_GY
    blocks = coarse_inverse[owner_flat * N_GY + row_index, source, slot]
    coarse_sol = jnp.einsum("aij,aj->ai", blocks, coarse_rhs, precision=lax.Precision.HIGHEST)
    lifted = jnp.dot(prolong_basis, coarse_sol[global_agg].T, precision=lax.Precision.HIGHEST).reshape(right_side.shape)
    state = state + lifted
    resid = resid - apply_op(lifted)
    return smooth(state, resid, apply_op)
```

```python
import functools

import jax
import jax.numpy as jnp
import ml_dtypes
import numpy as np
from jax import lax
from jax.experimental import pallas as pl
from jax.experimental.pallas import tpu as pltpu
from jax.sharding import PartitionSpec as P

BLOCK = 192
TRACE = 48
CW = 24
DEGREE = 3
COLS = 8
LANES = 128
ELEMS = COLS * LANES
OWNERS = 32
CAP = 32
AGG = 512

F32 = jnp.float32
BF16 = jnp.bfloat16

THETA = 0.5 * (4.0 + 0.25)
DELTA = 0.5 * (4.0 - 0.25)
SIGMA = THETA / DELTA


def chebyshev():
    rho = 1.0 / SIGMA
    steps = []
    for _ in range(DEGREE - 1):
        rho_new = 1.0 / (2.0 * SIGMA - rho)
        steps.append((rho_new * rho, 2.0 * rho_new / DELTA))
        rho = rho_new
    return steps


def selection():
    sel = np.zeros((192, 192), np.float32)
    t = np.arange(48)
    for group, rows in enumerate(
        (16 * (t // 4) + t % 4, 16 * (t // 4) + t % 4 + 12, 4 * t, 4 * t + 3)
    ):
        sel[48 * group + t, rows] = 1.0
    return sel.astype(ml_dtypes.bfloat16)


def dot(a, b):
    return jnp.dot(a, b, preferred_element_type=F32)


def dot_nt(a, b):
    return lax.dot_general(a, b, (((1,), (1,)), ((), ())), preferred_element_type=F32)


def split(v):
    high = v.astype(BF16)
    return high, (v - high.astype(F32)).astype(BF16)


def dot3(a_high, a_low, b_high, b_low):
    return dot(a_high, b_high) + dot(a_high, b_low) + dot(a_low, b_high)


def lanes(col):
    return slice(LANES * col, LANES * (col + 1))


def face_rows(v, node):
    at = 16 * node
    return jnp.concatenate([v[64 * c + at : 64 * c + at + 16] for c in range(3)], axis=0)


def tile_coef(coef_ref, col):
    return coef_ref[col : col + 1, :]


def emit_traces(w_of, sel_ref, par_ref, sends):
    sx_in, sx_out, sy_in, sy_out = sends
    even_x = par_ref[0] == 0
    even_y = par_ref[1] == 0
    for y in range(4):
        low = face_rows(w_of(y), 0)
        high = face_rows(w_of(4 + y), 3)
        sx_in[:, lanes(y)] = jnp.where(even_x, high, low)
        sx_out[:, lanes(y)] = jnp.where(even_x, low, high)
    pick = sel_ref[0:96, :]
    for x in range(2):
        ends = []
        for y, rows in ((0, slice(0, 48)), (3, slice(48, 96))):
            high, low = split(w_of(4 * x + y))
            ends.append(dot(pick[rows], high) + dot(pick[rows], low))
        sy_in[:, lanes(x)] = jnp.where(even_y, ends[1], ends[0])
        sy_out[:, lanes(x)] = jnp.where(even_y, ends[0], ends[1])


def first_kernel(rs_ref, coef_ref, sel_ref, par_ref, r_ref, d_ref, *sends):
    for col in range(COLS):
        v = rs_ref[pl.ds(col, BLOCK, stride=COLS), :]
        r_ref[:, lanes(col)] = v
        d_ref[:, lanes(col)] = v * (1.0 / THETA)
    emit_traces(
        lambda col: d_ref[:, lanes(col)] * tile_coef(coef_ref, col), sel_ref, par_ref, sends
    )


def weights_kernel(stiff_ref, faces_ref, pt_ref, wh_ref, wl_ref, pth_ref, ptl_ref, ph_ref, pl_ref):
    high, low = split(stiff_ref[...])
    wh_ref[:, 0:BLOCK] = high
    wl_ref[:, 0:BLOCK] = low
    for piece in range(3):
        high, low = split(faces_ref[192 * piece : 192 * (piece + 1), :].T)
        wh_ref[:, 192 * (piece + 1) : 192 * (piece + 2)] = high
        wl_ref[:, 192 * (piece + 1) : 192 * (piece + 2)] = low
    pt = pt_ref[...]
    high, low = split(pt)
    pth_ref[...] = high
    ptl_ref[...] = low
    row = lax.broadcasted_iota(jnp.int32, (CW, 32), 0)
    col = lax.broadcasted_iota(jnp.int32, (CW, 32), 1)
    spread = ((row & 3) * 8 + (row >> 2) == col).astype(F32)
    p = pt.T
    p_high, p_low = split(p)
    spread = spread.astype(BF16)
    ph_ref[...] = dot(p_high, spread).astype(BF16)
    pl_ref[...] = dot(p_low, spread).astype(BF16)


def interior_kernel(d_ref, coef_ref, ori_ref, wh_ref, wl_ref, sel_ref, out_ref, xh_ref, xl_ref, t_ref):
    for col in range(COLS):
        high, low = split(d_ref[:, lanes(col)] * tile_coef(coef_ref, col))
        xh_ref[0:BLOCK, lanes(col)] = high
        xl_ref[0:BLOCK, lanes(col)] = low
    lane = lax.broadcasted_iota(jnp.int32, (48, LANES), 1)
    for x_ref in (xh_ref, xl_ref):
        t_ref[...] = dot(sel_ref[...], x_ref[0:BLOCK, :])
        for col in range(COLS):
            x, y = col // 4, col % 4
            for direction in range(6):
                trace = None
                if direction == 0 and x == 1:
                    trace = face_rows(x_ref[0:BLOCK, lanes(col - 4)], 3).astype(F32)
                elif direction == 1 and x == 0:
                    trace = face_rows(x_ref[0:BLOCK, lanes(col + 4)], 0).astype(F32)
                elif direction == 2 and y > 0:
                    trace = t_ref[48:96, lanes(col - 1)]
                elif direction == 3 and y < 3:
                    trace = t_ref[0:48, lanes(col + 1)]
                elif direction == 4:
                    trace = jnp.where(lane == 0, 0.0, pltpu.roll(t_ref[144:192, lanes(col)], 1, 1))
                elif direction == 5:
                    trace = jnp.where(
                        lane == LANES - 1, 0.0, pltpu.roll(t_ref[96:144, lanes(col)], LANES - 1, 1)
                    )
                at = BLOCK + 96 * direction
                if trace is None:
                    x_ref[at : at + 96, lanes(col)] = jnp.zeros((96, LANES), BF16)
                    continue
                row = COLS * direction + col
                picked = ori_ref[row : row + 1, :] == 1
                x_ref[at : at + 48, lanes(col)] = jnp.where(picked, 0.0, trace).astype(BF16)
                x_ref[at + 48 : at + 96, lanes(col)] = jnp.where(picked, trace, 0.0).astype(BF16)
    for half in range(2):
        span = slice(512 * half, 512 * (half + 1))
        out_ref[:, span] = dot3(wh_ref[...], wl_ref[...], xh_ref[:, span], xl_ref[:, span])


def halo_product(halo, cols, direction, ori_ref, wh_ref, wl_ref):
    highs, lows = [], []
    for n, col in enumerate(cols):
        trace = halo(n)
        row = COLS * direction + col
        picked = ori_ref[row : row + 1, :] == 1
        both = jnp.concatenate([jnp.where(picked, 0.0, trace), jnp.where(picked, trace, 0.0)], axis=0)
        high, low = split(both)
        highs.append(high)
        lows.append(low)
    at = BLOCK + 96 * direction
    return dot3(
        wh_ref[:, at : at + 96],
        wl_ref[:, at : at + 96],
        jnp.concatenate(highs, axis=1),
        jnp.concatenate(lows, axis=1),
    )


def halo_sum(part_ref, ori_ref, wh_ref, wl_ref, par_ref, gets, ad_ref):
    gx_in, gx_out, gy_in, gy_out = gets
    even_x = par_ref[0] == 0
    even_y = par_ref[1] == 0

    def lower(inside, outside, even):
        return lambda n: jnp.where(even, outside[:, lanes(n)], inside[:, lanes(n)])

    def upper(inside, outside, even):
        return lambda n: jnp.where(even, inside[:, lanes(n)], outside[:, lanes(n)])

    weights = (ori_ref, wh_ref, wl_ref)
    ad_ref[:, 0:512] = part_ref[:, 0:512] + halo_product(
        lower(gx_in, gx_out, even_x), (0, 1, 2, 3), 0, *weights
    )
    ad_ref[:, 512:1024] = part_ref[:, 512:1024] + halo_product(
        upper(gx_in, gx_out, even_x), (4, 5, 6, 7), 1, *weights
    )
    for cols, direction, pick in (((0, 4), 2, lower), ((3, 7), 3, upper)):
        both = halo_product(pick(gy_in, gy_out, even_y), cols, direction, *weights)
        for n, col in enumerate(cols):
            ad_ref[:, lanes(col)] += both[:, lanes(n)]


def step_kernel(
    scales, part_ref, r_ref, d_ref, x_ref, coef_ref, ori_ref, wh_ref, wl_ref, sel_ref, par_ref,
    gx_in, gx_out, gy_in, gy_out, r_out, d_out, x_out, sx_in, sx_out, sy_in, sy_out, ad_ref,
):
    halo_sum(part_ref, ori_ref, wh_ref, wl_ref, par_ref, (gx_in, gx_out, gy_in, gy_out), ad_ref)
    keep, gain = scales
    for col in range(COLS):
        at = lanes(col)
        resid = r_ref[:, at] - ad_ref[:, at]
        step = gain * resid
        if keep:
            step = keep * d_ref[:, at] + step
        r_out[:, at] = resid
        d_out[:, at] = step
        x_out[:, at] = x_ref[:, at] + step
    emit_traces(
        lambda col: d_out[:, lanes(col)] * tile_coef(coef_ref, col),
        sel_ref,
        par_ref,
        (sx_in, sx_out, sy_in, sy_out),
    )


def last_kernel(
    part_ref, r_ref, x_ref, ori_ref, wh_ref, wl_ref, par_ref, gx_in, gx_out, gy_in, gy_out,
    x_out, r_out, ad_ref,
):
    halo_sum(part_ref, ori_ref, wh_ref, wl_ref, par_ref, (gx_in, gx_out, gy_in, gy_out), ad_ref)
    for col in range(COLS):
        at = lanes(col)
        rows = pl.ds(col, BLOCK, stride=COLS)
        x_out[rows, :] = x_ref[:, at]
        r_out[rows, :] = r_ref[:, at] - ad_ref[:, at]


def pack_kernel(in_ref, out_ref):
    for s in range(in_ref.shape[0]):
        for m in range(6):
            out_ref[s, m] = jnp.concatenate([in_ref[s, 4 * m + q] for q in range(4)], axis=-1)


def slots_kernel(agg_ref, owner_ref, hot_ref):
    owner = owner_ref[...]
    owner_hot = lax.broadcasted_iota(jnp.int32, (OWNERS, AGG), 0) == owner
    before = lax.broadcasted_iota(jnp.int32, (AGG, AGG), 0) < lax.broadcasted_iota(
        jnp.int32, (AGG, AGG), 1
    )
    counts = dot(owner_hot.astype(BF16), before.astype(BF16))
    slot = jnp.sum(jnp.where(owner_hot, counts, 0.0), axis=0, keepdims=True)
    first = lax.broadcasted_iota(jnp.int32, (8, AGG), 0) == 0
    table = jnp.where(first, owner.astype(F32), slot).astype(BF16)
    for col in range(COLS):
        at = lanes(col)
        member = lax.broadcasted_iota(jnp.int32, (AGG, LANES), 0) == agg_ref[col : col + 1, :]
        found = dot(table, member.astype(BF16))
        target = (found[0:1] * float(CAP) + found[1:2]).astype(jnp.int32)
        hot = lax.broadcasted_iota(jnp.int32, (OWNERS * CAP, LANES), 0) == target
        hot_ref[:, at] = hot.astype(BF16)


def coarse_kernel(
    r_ref, x_ref, coef_ref, hot_ref, inv_ref, pth_ref, ptl_ref, ph_ref, pl_ref, sel_ref, par_ref,
    d_out, x_out, sx_in, sx_out, sy_in, sy_out, y_ref, sol_ref,
):
    r_high, r_low = split(r_ref[...])
    proj = dot3(pth_ref[...], ptl_ref[...], r_high, r_low)
    p_high, p_low = split(proj)
    rhs = dot_nt(p_high, hot_ref[...]) + dot_nt(p_low, hot_ref[...])
    group = lax.broadcasted_iota(jnp.int32, (CW, LANES), 1) >> 5
    for o in range(OWNERS):
        part = jnp.where(group == o % 4, rhs[:, lanes(o // 4)], 0.0)
        part = part + pltpu.roll(part, 32, 1)
        part = part + pltpu.roll(part, 64, 1)
        y_ref[o, 0:6, :] = jnp.sum(inv_ref[o] * part[None], axis=1)
        y_ref[o, 6:8, :] = jnp.zeros((2, LANES), F32)
    group = lax.broadcasted_iota(jnp.int32, (8, LANES), 1) >> 5
    for q in range(4):
        for j in range(8):
            total = jnp.zeros((8, LANES), F32)
            for g in range(4):
                moved = y_ref[4 * j + g]
                if g != q:
                    moved = pltpu.roll(moved, 32 * ((g - q) % 4), 1)
                total = jnp.where(group == g, moved, total)
            sol_ref[8 * q : 8 * q + 8, lanes(j)] = total
    s_high, s_low = split(sol_ref[...])
    each = dot(s_high, hot_ref[...]) + dot(s_low, hot_ref[...])
    e_high, e_low = split(each)
    for half in range(2):
        span = slice(512 * half, 512 * (half + 1))
        lift = dot3(ph_ref[...], pl_ref[...], e_high[:, span], e_low[:, span])
        d_out[:, span] = lift
        x_out[:, span] = x_ref[:, span] + lift
    emit_traces(
        lambda col: d_out[:, lanes(col)] * tile_coef(coef_ref, col),
        sel_ref,
        par_ref,
        (sx_in, sx_out, sy_in, sy_out),
    )


def field(*shape, dtype=F32):
    return pltpu.VMEM(shape, dtype)


def call(kernel, outs, args, scratch=(), smem=(), limit=48):
    vmem = pl.BlockSpec(memory_space=pltpu.VMEM)
    scalar = pl.BlockSpec(memory_space=pltpu.SMEM)
    specs = [scalar if n in smem else vmem for n in range(len(args))]
    placed = [
        a if n in smem else pltpu.with_memory_space_constraint(a, pltpu.VMEM)
        for n, a in enumerate(args)
    ]
    return pl.pallas_call(
        kernel,
        out_shape=outs,
        in_specs=specs,
        out_specs=[vmem] * len(outs),
        scratch_shapes=list(scratch),
        compiler_params=pltpu.CompilerParams(vmem_limit_bytes=limit << 20),
    )(*placed)


def swap_even(v, axis):
    count = lax.axis_size(axis)
    return lax.ppermute(v, axis, [(i, i ^ 1) for i in range(count)])


def swap_odd(v, axis):
    count = lax.axis_size(axis)
    return lax.ppermute(v, axis, [(i, i + 1 if i % 2 else i - 1) for i in range(1, count - 1)])


def exchange(sends):
    return (
        swap_even(sends[0], "gx"),
        swap_odd(sends[1], "gx"),
        swap_even(sends[2], "gy"),
        swap_odd(sends[3], "gy"),
    )


SENDS = [field(48, 512), field(48, 512), field(48, 256), field(48, 256)]


def shards(
    right_side,
    coefficient,
    orientation,
    aggregate_map,
    owner_map,
    stiffness,
    face_blocks,
    prolong_basis,
    coarse_inverse,
):
    shape = right_side.shape
    par = jnp.stack([lax.axis_index("gx") & 1, lax.axis_index("gy") & 1]).astype(jnp.int32)
    sel = jnp.asarray(selection())
    coef = coefficient.reshape(COLS, LANES)
    ori = orientation.reshape(6 * COLS, LANES)

    packed = pl.pallas_call(
        pack_kernel,
        out_shape=jax.ShapeDtypeStruct((OWNERS, 6, CW, LANES), F32),
        grid=(8,),
        in_specs=[pl.BlockSpec((4, CW, CW, CAP), lambda s: (s, 0, 0, 0))],
        out_specs=pl.BlockSpec((4, 6, CW, LANES), lambda s: (s, 0, 0, 0)),
    )(jnp.transpose(coarse_inverse[0], (0, 2, 3, 1)))
    inverse = lax.all_to_all(packed, "gx", split_axis=0, concat_axis=0, tiled=True)

    full = field(BLOCK, ELEMS)
    r, d, *sends = call(
        first_kernel,
        [full, full, *SENDS],
        [right_side.reshape(BLOCK * COLS, LANES), coef, sel, par],
        smem=(3,),
    )
    wide = field(BLOCK, 768, dtype=BF16)
    wh, wl, pth, ptl, ph, plo = call(
        weights_kernel,
        [wide, wide, field(CW, BLOCK, dtype=BF16), field(CW, BLOCK, dtype=BF16),
         field(BLOCK, 32, dtype=BF16), field(BLOCK, 32, dtype=BF16)],
        [stiffness, jnp.transpose(face_blocks, (0, 1, 3, 2)).reshape(576, BLOCK), prolong_basis.T],
    )
    hot = call(
        slots_kernel,
        [field(ELEMS, ELEMS, dtype=BF16)],
        [aggregate_map.reshape(COLS, LANES), owner_map.reshape(1, AGG)],
    )[0]

    def interior(step):
        return call(
            interior_kernel,
            [full],
            [step, coef, ori, wh, wl, sel],
            scratch=[
                pltpu.VMEM((768, ELEMS), BF16),
                pltpu.VMEM((768, ELEMS), BF16),
                pltpu.VMEM((BLOCK, ELEMS), F32),
            ],
        )[0]

    accumulator = [pltpu.VMEM((BLOCK, ELEMS), F32)]

    def advance(scales, r, d, x, sends):
        gets = exchange(sends)
        part = interior(d)
        return call(
            functools.partial(step_kernel, scales),
            [full, full, full, *SENDS],
            [part, r, d, x, coef, ori, wh, wl, sel, par, *gets],
            scratch=accumulator,
            smem=(9,),
        )

    steps = chebyshev()
    x = d
    for scales in steps:
        r, d, x, *sends = advance(scales, r, d, x, sends)
    r, _, _, *_ = advance((0.0, 1.0 / THETA), r, d, x, sends)
    d, x, *sends = call(
        coarse_kernel,
        [full, full, *SENDS],
        [r, x, coef, hot, inverse, pth, ptl, ph, plo, sel, par],
        scratch=[pltpu.VMEM((OWNERS, 8, LANES), F32), pltpu.VMEM((32, ELEMS), F32)],
        smem=(10,),
    )
    r, d, x, *sends = advance((0.0, 1.0 / THETA), r, d, x, sends)
    for scales in steps:
        r, d, x, *sends = advance(scales, r, d, x, sends)
    gets = exchange(sends)
    part = interior(d)
    x, r = call(
        last_kernel,
        [jax.ShapeDtypeStruct((BLOCK * COLS, LANES), F32)] * 2,
        [part, r, x, ori, wh, wl, par, *gets],
        scratch=accumulator,
        smem=(6,),
    )
    return x.reshape(shape), r.reshape(shape)


def solution(mesh):
    in_specs = (
        P(None, "gx", "gy", None),
        P("gx", "gy", None),
        P(None, "gx", "gy", None),
        P("gx", "gy", None),
        P(("gx", "gy"), None),
        P(),
        P(),
        P(),
        P(("gx", "gy"), None, None, None, None),
    )
    out_specs = (P(None, "gx", "gy", None), P(None, "gx", "gy", None))
    return jax.shard_map(shards, mesh=mesh, in_specs=in_specs, out_specs=out_specs, check_vma=False)
```

```python
import functools

import jax
import jax.numpy as jnp
import ml_dtypes
import numpy as np
from jax import lax
from jax.experimental import pallas as pl
from jax.experimental.pallas import tpu as pltpu
from jax.sharding import PartitionSpec as P

BLOCK = 192
TRACE = 48
CW = 24
DEGREE = 3
COLS = 8
LANES = 128
ELEMS = COLS * LANES
OWNERS = 32
CAP = 32
AGG = 512

F32 = jnp.float32
BF16 = jnp.bfloat16

THETA = 0.5 * (4.0 + 0.25)
DELTA = 0.5 * (4.0 - 0.25)
SIGMA = THETA / DELTA


def chebyshev():
    rho = 1.0 / SIGMA
    steps = []
    for _ in range(DEGREE - 1):
        rho_new = 1.0 / (2.0 * SIGMA - rho)
        steps.append((rho_new * rho, 2.0 * rho_new / DELTA))
        rho = rho_new
    return steps


def selection():
    sel = np.zeros((192, 192), np.float32)
    t = np.arange(48)
    for group, rows in enumerate(
        (16 * (t // 4) + t % 4, 16 * (t // 4) + t % 4 + 12, 4 * t, 4 * t + 3)
    ):
        sel[48 * group + t, rows] = 1.0
    return sel.astype(ml_dtypes.bfloat16)


def dot(a, b):
    return jnp.dot(a, b, preferred_element_type=F32)


def dot_nt(a, b):
    return lax.dot_general(a, b, (((1,), (1,)), ((), ())), preferred_element_type=F32)


def split(v):
    high = v.astype(BF16)
    return high, (v - high.astype(F32)).astype(BF16)


def dot3(a_high, a_low, b_high, b_low):
    return dot(a_high, b_high) + dot(a_high, b_low) + dot(a_low, b_high)


def lanes(col):
    return slice(LANES * col, LANES * (col + 1))


def face_rows(v, node):
    at = 16 * node
    return jnp.concatenate([v[64 * c + at : 64 * c + at + 16] for c in range(3)], axis=0)


def tile_coef(coef_ref, col):
    return coef_ref[col : col + 1, :]


def emit_traces(w_of, sel_ref, par_ref, sends):
    sx_in, sx_out, sy_in, sy_out = sends
    even_x = par_ref[0] == 0
    even_y = par_ref[1] == 0
    for y in range(4):
        low = face_rows(w_of(y), 0)
        high = face_rows(w_of(4 + y), 3)
        sx_in[:, lanes(y)] = jnp.where(even_x, high, low)
        sx_out[:, lanes(y)] = jnp.where(even_x, low, high)
    pick = sel_ref[0:96, :]
    for x in range(2):
        ends = []
        for y, rows in ((0, slice(0, 48)), (3, slice(48, 96))):
            high, low = split(w_of(4 * x + y))
            ends.append(dot(pick[rows], high) + dot(pick[rows], low))
        sy_in[:, lanes(x)] = jnp.where(even_y, ends[1], ends[0])
        sy_out[:, lanes(x)] = jnp.where(even_y, ends[0], ends[1])


def first_kernel(rs_ref, coef_ref, sel_ref, par_ref, r_ref, d_ref, *sends):
    for col in range(COLS):
        v = rs_ref[pl.ds(col, BLOCK, stride=COLS), :]
        r_ref[:, lanes(col)] = v
        d_ref[:, lanes(col)] = v * (1.0 / THETA)
    emit_traces(
        lambda col: d_ref[:, lanes(col)] * tile_coef(coef_ref, col), sel_ref, par_ref, sends
    )


def weights_kernel(stiff_ref, faces_ref, pt_ref, wh_ref, wl_ref, pth_ref, ptl_ref, ph_ref, pl_ref):
    high, low = split(stiff_ref[...])
    wh_ref[:, 0:BLOCK] = high
    wl_ref[:, 0:BLOCK] = low
    for piece in range(3):
        high, low = split(faces_ref[192 * piece : 192 * (piece + 1), :].T)
        wh_ref[:, 192 * (piece + 1) : 192 * (piece + 2)] = high
        wl_ref[:, 192 * (piece + 1) : 192 * (piece + 2)] = low
    pt = pt_ref[...]
    high, low = split(pt)
    pth_ref[...] = high
    ptl_ref[...] = low
    high, low = split(pt.T)
    ph_ref[...] = high
    pl_ref[...] = low


def interior_kernel(d_ref, coef_ref, ori_ref, wh_ref, wl_ref, sel_ref, out_ref, xh_ref, xl_ref, t_ref):
    for col in range(COLS):
        high, low = split(d_ref[:, lanes(col)] * tile_coef(coef_ref, col))
        xh_ref[0:BLOCK, lanes(col)] = high
        xl_ref[0:BLOCK, lanes(col)] = low
    lane = lax.broadcasted_iota(jnp.int32, (48, LANES), 1)
    for x_ref in (xh_ref, xl_ref):
        t_ref[...] = dot(sel_ref[...], x_ref[0:BLOCK, :])
        for col in range(COLS):
            x, y = col // 4, col % 4
            for direction in range(6):
                trace = None
                if direction == 0 and x == 1:
                    trace = face_rows(x_ref[0:BLOCK, lanes(col - 4)], 3).astype(F32)
                elif direction == 1 and x == 0:
                    trace = face_rows(x_ref[0:BLOCK, lanes(col + 4)], 0).astype(F32)
                elif direction == 2 and y > 0:
                    trace = t_ref[48:96, lanes(col - 1)]
                elif direction == 3 and y < 3:
                    trace = t_ref[0:48, lanes(col + 1)]
                elif direction == 4:
                    trace = jnp.where(lane == 0, 0.0, pltpu.roll(t_ref[144:192, lanes(col)], 1, 1))
                elif direction == 5:
                    trace = jnp.where(
                        lane == LANES - 1, 0.0, pltpu.roll(t_ref[96:144, lanes(col)], LANES - 1, 1)
                    )
                at = BLOCK + 96 * direction
                if trace is None:
                    x_ref[at : at + 96, lanes(col)] = jnp.zeros((96, LANES), BF16)
                    continue
                row = COLS * direction + col
                picked = ori_ref[row : row + 1, :] == 1
                x_ref[at : at + 48, lanes(col)] = jnp.where(picked, 0.0, trace).astype(BF16)
                x_ref[at + 48 : at + 96, lanes(col)] = jnp.where(picked, trace, 0.0).astype(BF16)
    for half in range(2):
        span = slice(512 * half, 512 * (half + 1))
        out_ref[:, span] = dot3(wh_ref[...], wl_ref[...], xh_ref[:, span], xl_ref[:, span])


def halo_product(halo, cols, direction, ori_ref, wh_ref, wl_ref):
    highs, lows = [], []
    for n, col in enumerate(cols):
        trace = halo(n)
        row = COLS * direction + col
        picked = ori_ref[row : row + 1, :] == 1
        both = jnp.concatenate([jnp.where(picked, 0.0, trace), jnp.where(picked, trace, 0.0)], axis=0)
        high, low = split(both)
        highs.append(high)
        lows.append(low)
    at = BLOCK + 96 * direction
    return dot3(
        wh_ref[:, at : at + 96],
        wl_ref[:, at : at + 96],
        jnp.concatenate(highs, axis=1),
        jnp.concatenate(lows, axis=1),
    )


def halo_sum(part_ref, ori_ref, wh_ref, wl_ref, par_ref, gets, ad_ref):
    gx_in, gx_out, gy_in, gy_out = gets
    even_x = par_ref[0] == 0
    even_y = par_ref[1] == 0

    def lower(inside, outside, even, there):
        return lambda n: jnp.where(
            there, jnp.where(even, outside[:, lanes(n)], inside[:, lanes(n)]), 0.0
        )

    def upper(inside, outside, even, there):
        return lambda n: jnp.where(
            there, jnp.where(even, inside[:, lanes(n)], outside[:, lanes(n)]), 0.0
        )

    weights = (ori_ref, wh_ref, wl_ref)
    ad_ref[:, 0:512] = part_ref[:, 0:512] + halo_product(
        lower(gx_in, gx_out, even_x, par_ref[2] == 1), (0, 1, 2, 3), 0, *weights
    )
    ad_ref[:, 512:1024] = part_ref[:, 512:1024] + halo_product(
        upper(gx_in, gx_out, even_x, par_ref[3] == 1), (4, 5, 6, 7), 1, *weights
    )
    for cols, direction, pick in (((0, 4), 2, lower), ((3, 7), 3, upper)):
        there = par_ref[direction + 2] == 1
        both = halo_product(pick(gy_in, gy_out, even_y, there), cols, direction, *weights)
        for n, col in enumerate(cols):
            ad_ref[:, lanes(col)] += both[:, lanes(n)]


def step_kernel(
    scales, part_ref, r_ref, d_ref, x_ref, coef_ref, ori_ref, wh_ref, wl_ref, sel_ref, par_ref,
    gx_in, gx_out, gy_in, gy_out, r_out, d_out, x_out, sx_in, sx_out, sy_in, sy_out, ad_ref,
):
    halo_sum(part_ref, ori_ref, wh_ref, wl_ref, par_ref, (gx_in, gx_out, gy_in, gy_out), ad_ref)
    keep, gain = scales
    for col in range(COLS):
        at = lanes(col)
        resid = r_ref[:, at] - ad_ref[:, at]
        step = gain * resid
        if keep:
            step = keep * d_ref[:, at] + step
        r_out[:, at] = resid
        d_out[:, at] = step
        x_out[:, at] = x_ref[:, at] + step
    emit_traces(
        lambda col: d_out[:, lanes(col)] * tile_coef(coef_ref, col),
        sel_ref,
        par_ref,
        (sx_in, sx_out, sy_in, sy_out),
    )


def last_kernel(
    part_ref, r_ref, x_ref, ori_ref, wh_ref, wl_ref, par_ref, gx_in, gx_out, gy_in, gy_out,
    x_out, r_out, ad_ref,
):
    halo_sum(part_ref, ori_ref, wh_ref, wl_ref, par_ref, (gx_in, gx_out, gy_in, gy_out), ad_ref)
    for col in range(COLS):
        at = lanes(col)
        rows = pl.ds(col, BLOCK, stride=COLS)
        x_out[rows, :] = x_ref[:, at]
        r_out[rows, :] = r_ref[:, at] - ad_ref[:, at]


def pack_kernel(in_ref, out_ref):
    for s in range(in_ref.shape[0]):
        for column in range(CW):
            tiles = [in_ref[s, 8 * q : 8 * q + 8, column, :] for q in range(3)]
            tiles.append(jnp.zeros((8, CAP), F32))
            out_ref[s, column] = jnp.concatenate(tiles, axis=-1)


def slots_kernel(agg_ref, owner_ref, hot_ref):
    owner = owner_ref[...]
    owner_hot = lax.broadcasted_iota(jnp.int32, (OWNERS, AGG), 0) == owner
    before = lax.broadcasted_iota(jnp.int32, (AGG, AGG), 0) < lax.broadcasted_iota(
        jnp.int32, (AGG, AGG), 1
    )
    counts = dot(owner_hot.astype(BF16), before.astype(BF16))
    slot = jnp.sum(jnp.where(owner_hot, counts, 0.0), axis=0, keepdims=True)
    first = lax.broadcasted_iota(jnp.int32, (8, AGG), 0) == 0
    table = jnp.where(first, owner.astype(F32), slot).astype(BF16)
    for col in range(COLS):
        at = lanes(col)
        member = lax.broadcasted_iota(jnp.int32, (AGG, LANES), 0) == agg_ref[col : col + 1, :]
        found = dot(table, member.astype(BF16))
        target = (found[0:1] * float(CAP) + found[1:2]).astype(jnp.int32)
        hot = lax.broadcasted_iota(jnp.int32, (OWNERS * CAP, LANES), 0) == target
        hot_ref[:, at] = hot.astype(BF16)


def restrict_kernel(r_ref, hot_ref, pth_ref, ptl_ref, out_ref, rhs_ref):
    r_high, r_low = split(r_ref[...])
    proj = dot3(pth_ref[...], ptl_ref[...], r_high, r_low)
    p_high, p_low = split(proj)
    rhs_ref[...] = dot_nt(p_high, hot_ref[...]) + dot_nt(p_low, hot_ref[...])
    group = lax.broadcasted_iota(jnp.int32, (8, LANES), 1) >> 5
    for o in range(OWNERS):
        total = jnp.zeros((8, LANES), F32)
        for q in range(3):
            moved = rhs_ref[8 * q : 8 * q + 8, lanes(o // 4)]
            if q != o % 4:
                moved = pltpu.roll(moved, 32 * ((q - o) % 4), 1)
            total = jnp.where(group == q, moved, total)
        out_ref[o] = total


def solve_kernel(rhs_ref, inv_ref, out_ref, wide_ref):
    group = lax.broadcasted_iota(jnp.int32, (8, LANES), 1) >> 5
    for s in range(OWNERS):
        tile = rhs_ref[s]
        for q in range(3):
            part = jnp.where(group == q, tile, 0.0)
            part = part + pltpu.roll(part, 32, 1)
            wide_ref[s, 8 * q : 8 * q + 8, :] = part + pltpu.roll(part, 64, 1)
        total = None
        for b in range(CW):
            term = inv_ref[s, b] * wide_ref[s, b : b + 1, :]
            total = term if total is None else total + term
        out_ref[s] = total


def lift_kernel(
    sol_in, x_ref, coef_ref, hot_ref, ph_ref, pl_ref, sel_ref, par_ref,
    d_out, x_out, sx_in, sx_out, sy_in, sy_out, sol_ref,
):
    group = lax.broadcasted_iota(jnp.int32, (8, LANES), 1) >> 5
    for q in range(3):
        for j in range(8):
            total = jnp.zeros((8, LANES), F32)
            for g in range(4):
                moved = sol_in[4 * j + g]
                if g != q:
                    moved = pltpu.roll(moved, 32 * ((g - q) % 4), 1)
                total = jnp.where(group == g, moved, total)
            sol_ref[8 * q : 8 * q + 8, lanes(j)] = total
    s_high, s_low = split(sol_ref[...])
    each = dot(s_high, hot_ref[...]) + dot(s_low, hot_ref[...])
    e_high, e_low = split(each)
    for half in range(2):
        span = slice(512 * half, 512 * (half + 1))
        lift = dot3(ph_ref[...], pl_ref[...], e_high[:, span], e_low[:, span])
        d_out[:, span] = lift
        x_out[:, span] = x_ref[:, span] + lift
    emit_traces(
        lambda col: d_out[:, lanes(col)] * tile_coef(coef_ref, col),
        sel_ref,
        par_ref,
        (sx_in, sx_out, sy_in, sy_out),
    )


def field(*shape, dtype=F32):
    return pltpu.VMEM(shape, dtype)


def call(kernel, outs, args, scratch=(), smem=(), limit=20):
    vmem = pl.BlockSpec(memory_space=pltpu.VMEM)
    scalar = pl.BlockSpec(memory_space=pltpu.SMEM)
    specs = [scalar if n in smem else vmem for n in range(len(args))]
    placed = [
        a if n in smem else pltpu.with_memory_space_constraint(a, pltpu.VMEM)
        for n, a in enumerate(args)
    ]
    return pl.pallas_call(
        kernel,
        out_shape=outs,
        in_specs=specs,
        out_specs=[vmem] * len(outs),
        scratch_shapes=list(scratch),
        compiler_params=pltpu.CompilerParams(vmem_limit_bytes=limit << 20),
    )(*placed)


def swap_even(v, axis):
    count = lax.axis_size(axis)
    return lax.ppermute(v, axis, [(i, i ^ 1) for i in range(count)])


def swap_odd(v, axis):
    count = lax.axis_size(axis)
    return lax.ppermute(
        v, axis, [(i, (i + 1 if i % 2 else i - 1) % count) for i in range(count)]
    )


def exchange(sends):
    return (
        swap_even(sends[0], "gx"),
        swap_odd(sends[1], "gx"),
        swap_even(sends[2], "gy"),
        swap_odd(sends[3], "gy"),
    )


SENDS = [field(48, 512), field(48, 512), field(48, 256), field(48, 256)]


def shards(
    right_side,
    coefficient,
    orientation,
    aggregate_map,
    owner_map,
    stiffness,
    face_blocks,
    prolong_basis,
    coarse_inverse,
):
    shape = right_side.shape
    at_x, at_y = lax.axis_index("gx"), lax.axis_index("gy")
    par = jnp.stack(
        [
            at_x & 1,
            at_y & 1,
            at_x > 0,
            at_x < lax.axis_size("gx") - 1,
            at_y > 0,
            at_y < lax.axis_size("gy") - 1,
        ]
    ).astype(jnp.int32)
    sel = jnp.asarray(selection())
    coef = coefficient.reshape(COLS, LANES)
    ori = orientation.reshape(6 * COLS, LANES)

    full = field(BLOCK, ELEMS)
    r, d, *sends = call(
        first_kernel,
        [full, full, *SENDS],
        [right_side.reshape(BLOCK * COLS, LANES), coef, sel, par],
        smem=(3,),
    )
    wide = field(BLOCK, 768, dtype=BF16)
    wh, wl, pth, ptl, ph, plo = call(
        weights_kernel,
        [wide, wide, field(CW, BLOCK, dtype=BF16), field(CW, BLOCK, dtype=BF16),
         field(BLOCK, CW, dtype=BF16), field(BLOCK, CW, dtype=BF16)],
        [stiffness, jnp.transpose(face_blocks, (0, 1, 3, 2)).reshape(576, BLOCK), prolong_basis.T],
    )
    hot = call(
        slots_kernel,
        [field(ELEMS, ELEMS, dtype=BF16)],
        [aggregate_map.reshape(COLS, LANES), owner_map.reshape(1, AGG)],
    )[0]

    def interior(step):
        return call(
            interior_kernel,
            [full],
            [step, coef, ori, wh, wl, sel],
            scratch=[
                pltpu.VMEM((768, ELEMS), BF16),
                pltpu.VMEM((768, ELEMS), BF16),
                pltpu.VMEM((BLOCK, ELEMS), F32),
            ],
        )[0]

    accumulator = [pltpu.VMEM((BLOCK, ELEMS), F32)]

    def advance(scales, r, d, x, sends):
        gets = exchange(sends)
        part = interior(d)
        return call(
            functools.partial(step_kernel, scales),
            [full, full, full, *SENDS],
            [part, r, d, x, coef, ori, wh, wl, sel, par, *gets],
            scratch=accumulator,
            smem=(9,),
        )

    steps = chebyshev()
    x = d
    for scales in steps:
        r, d, x, *sends = advance(scales, r, d, x, sends)
    r, _, _, *_ = advance((0.0, 1.0 / THETA), r, d, x, sends)
    packets = field(OWNERS, 8, LANES)
    rhs = call(
        restrict_kernel, [packets], [r, hot, pth, ptl], scratch=[pltpu.VMEM((CW, ELEMS), F32)]
    )[0]
    rhs = lax.all_to_all(rhs, "gx", split_axis=0, concat_axis=0, tiled=True)
    inverse = pl.pallas_call(
        pack_kernel,
        out_shape=field(OWNERS, CW, 8, LANES),
        grid=(8,),
        in_specs=[pl.BlockSpec((4, CW, CW, CAP), lambda s: (s, 0, 0, 0))],
        out_specs=pl.BlockSpec((4, CW, 8, LANES), lambda s: (s, 0, 0, 0)),
        compiler_params=pltpu.CompilerParams(vmem_limit_bytes=16 << 20),
    )(jnp.transpose(coarse_inverse[0], (0, 2, 3, 1)))
    sol = call(
        solve_kernel, [packets], [rhs, inverse], scratch=[pltpu.VMEM((OWNERS, CW, LANES), F32)]
    )[0]
    sol = lax.all_to_all(sol, "gx", split_axis=0, concat_axis=0, tiled=True)
    d, x, *sends = call(
        lift_kernel,
        [full, full, *SENDS],
        [sol, x, coef, hot, ph, plo, sel, par],
        scratch=[pltpu.VMEM((CW, ELEMS), F32)],
        smem=(7,),
    )
    r, d, x, *sends = advance((0.0, 1.0 / THETA), r, d, x, sends)
    for scales in steps:
        r, d, x, *sends = advance(scales, r, d, x, sends)
    gets = exchange(sends)
    part = interior(d)
    x, r = call(
        last_kernel,
        [jax.ShapeDtypeStruct((BLOCK * COLS, LANES), F32)] * 2,
        [part, r, x, ori, wh, wl, par, *gets],
        scratch=accumulator,
        smem=(6,),
    )
    return x.reshape(shape), r.reshape(shape)


def solution(mesh):
    in_specs = (
        P(None, "gx", "gy", None),
        P("gx", "gy", None),
        P(None, "gx", "gy", None),
        P("gx", "gy", None),
        P(("gx", "gy"), None),
        P(),
        P(),
        P(),
        P(("gx", "gy"), None, None, None, None),
    )
    out_specs = (P(None, "gx", "gy", None), P(None, "gx", "gy", None))
    return jax.shard_map(shards, mesh=mesh, in_specs=in_specs, out_specs=out_specs, check_vma=False)
```

```python
import functools

import jax
import jax.numpy as jnp
import ml_dtypes
import numpy as np
from jax import lax
from jax.experimental import pallas as pl
from jax.experimental.pallas import tpu as pltpu
from jax.sharding import PartitionSpec as P

BLOCK = 192
TRACE = 48
CW = 24
DEGREE = 3
COLS = 8
LANES = 128
ELEMS = COLS * LANES
OWNERS = 32
CAP = 32
AGG = 512

F32 = jnp.float32
BF16 = jnp.bfloat16

THETA = 0.5 * (4.0 + 0.25)
DELTA = 0.5 * (4.0 - 0.25)
SIGMA = THETA / DELTA


def chebyshev():
    rho = 1.0 / SIGMA
    steps = []
    for _ in range(DEGREE - 1):
        rho_new = 1.0 / (2.0 * SIGMA - rho)
        steps.append((rho_new * rho, 2.0 * rho_new / DELTA))
        rho = rho_new
    return steps


def selection():
    sel = np.zeros((192, 192), np.float32)
    t = np.arange(48)
    for group, rows in enumerate(
        (16 * (t // 4) + t % 4, 16 * (t // 4) + t % 4 + 12, 4 * t, 4 * t + 3)
    ):
        sel[48 * group + t, rows] = 1.0
    return sel.astype(ml_dtypes.bfloat16)


def dot(a, b):
    return jnp.dot(a, b, preferred_element_type=F32)


def dot_nt(a, b):
    return lax.dot_general(a, b, (((1,), (1,)), ((), ())), preferred_element_type=F32)


def split(v):
    high = v.astype(BF16)
    return high, (v - high.astype(F32)).astype(BF16)


def dot3(a_high, a_low, b_high, b_low):
    return dot(a_high, b_high) + dot(a_high, b_low) + dot(a_low, b_high)


def lanes(col):
    return slice(LANES * col, LANES * (col + 1))


def face_rows(v, node):
    at = 16 * node
    return jnp.concatenate([v[64 * c + at : 64 * c + at + 16] for c in range(3)], axis=0)


def tile_coef(coef_ref, col):
    return coef_ref[col : col + 1, :]


def sides(place_ref):
    at_x, at_y = place_ref[0], place_ref[1]
    last_x, last_y = place_ref[2], place_ref[3]
    return at_x % 2 == 0, at_y % 2 == 0, (at_x > 0, at_x < last_x, at_y > 0, at_y < last_y)


def emit_traces(w_of, sel_ref, place_ref, sends):
    sx_in, sx_out, sy_in, sy_out = sends
    even_x, even_y, _ = sides(place_ref)
    for y in range(4):
        low = face_rows(w_of(y), 0)
        high = face_rows(w_of(4 + y), 3)
        sx_in[:, lanes(y)] = jnp.where(even_x, high, low)
        sx_out[:, lanes(y)] = jnp.where(even_x, low, high)
    pick = sel_ref[0:96, :]
    for x in range(2):
        ends = []
        for y, rows in ((0, slice(0, 48)), (3, slice(48, 96))):
            high, low = split(w_of(4 * x + y))
            ends.append(dot(pick[rows], high) + dot(pick[rows], low))
        sy_in[:, lanes(x)] = jnp.where(even_y, ends[1], ends[0])
        sy_out[:, lanes(x)] = jnp.where(even_y, ends[0], ends[1])


def fetch(pairs, sems):
    copies = [pltpu.make_async_copy(a, b, sems.at[n]) for n, (a, b) in enumerate(pairs)]
    for copy in copies:
        copy.start()
    return copies


def first_kernel(
    rs_hbm, coef_hbm, ori_hbm, sel_hbm, place_ref,
    r_ref, d_ref, coef_ref, ori_ref, sel_ref, sx_in, sx_out, sy_in, sy_out, rs_ref, sems,
):
    copies = fetch(
        ((rs_hbm, rs_ref), (coef_hbm, coef_ref), (sel_hbm, sel_ref), (ori_hbm, ori_ref)), sems
    )
    for copy in copies[:3]:
        copy.wait()
    for col in range(COLS):
        v = rs_ref[pl.ds(col, BLOCK, stride=COLS), :]
        r_ref[:, lanes(col)] = v
        d_ref[:, lanes(col)] = v * (1.0 / THETA)
    emit_traces(
        lambda col: d_ref[:, lanes(col)] * tile_coef(coef_ref, col),
        sel_ref,
        place_ref,
        (sx_in, sx_out, sy_in, sy_out),
    )
    copies[3].wait()


def weights_kernel(
    stiff_hbm, faces_hbm, pt_hbm, wh_ref, wl_ref, pth_ref, ptl_ref, ph_ref, pl_ref,
    stiff_ref, faces_ref, pt_ref, sems,
):
    copies = fetch(((stiff_hbm, stiff_ref), (pt_hbm, pt_ref), (faces_hbm, faces_ref)), sems)
    copies[0].wait()
    high, low = split(stiff_ref[...])
    wh_ref[:, 0:BLOCK] = high
    wl_ref[:, 0:BLOCK] = low
    copies[1].wait()
    pt = pt_ref[...]
    high, low = split(pt)
    pth_ref[...] = high
    ptl_ref[...] = low
    high, low = split(pt.T)
    ph_ref[...] = high
    pl_ref[...] = low
    copies[2].wait()
    for piece in range(3):
        high, low = split(faces_ref[192 * piece : 192 * (piece + 1), :].T)
        wh_ref[:, 192 * (piece + 1) : 192 * (piece + 2)] = high
        wl_ref[:, 192 * (piece + 1) : 192 * (piece + 2)] = low


def interior_kernel(d_ref, coef_ref, ori_ref, wh_ref, wl_ref, sel_ref, out_ref, xh_ref, xl_ref, t_ref):
    for col in range(COLS):
        high, low = split(d_ref[:, lanes(col)] * tile_coef(coef_ref, col))
        xh_ref[0:BLOCK, lanes(col)] = high
        xl_ref[0:BLOCK, lanes(col)] = low
    lane = lax.broadcasted_iota(jnp.int32, (48, LANES), 1)
    for x_ref in (xh_ref, xl_ref):
        t_ref[...] = dot(sel_ref[...], x_ref[0:BLOCK, :])
        for col in range(COLS):
            x, y = col // 4, col % 4
            for direction in range(6):
                trace = None
                if direction == 0 and x == 1:
                    trace = face_rows(x_ref[0:BLOCK, lanes(col - 4)], 3).astype(F32)
                elif direction == 1 and x == 0:
                    trace = face_rows(x_ref[0:BLOCK, lanes(col + 4)], 0).astype(F32)
                elif direction == 2 and y > 0:
                    trace = t_ref[48:96, lanes(col - 1)]
                elif direction == 3 and y < 3:
                    trace = t_ref[0:48, lanes(col + 1)]
                elif direction == 4:
                    trace = jnp.where(lane == 0, 0.0, pltpu.roll(t_ref[144:192, lanes(col)], 1, 1))
                elif direction == 5:
                    trace = jnp.where(
                        lane == LANES - 1, 0.0, pltpu.roll(t_ref[96:144, lanes(col)], LANES - 1, 1)
                    )
                at = BLOCK + 96 * direction
                if trace is None:
                    x_ref[at : at + 96, lanes(col)] = jnp.zeros((96, LANES), BF16)
                    continue
                row = COLS * direction + col
                picked = ori_ref[row : row + 1, :] == 1
                x_ref[at : at + 48, lanes(col)] = jnp.where(picked, 0.0, trace).astype(BF16)
                x_ref[at + 48 : at + 96, lanes(col)] = jnp.where(picked, trace, 0.0).astype(BF16)
    for half in range(2):
        span = slice(512 * half, 512 * (half + 1))
        out_ref[:, span] = dot3(wh_ref[...], wl_ref[...], xh_ref[:, span], xl_ref[:, span])


def halo_product(halo, cols, direction, ori_ref, wh_ref, wl_ref):
    highs, lows = [], []
    for n, col in enumerate(cols):
        trace = halo(n)
        row = COLS * direction + col
        picked = ori_ref[row : row + 1, :] == 1
        both = jnp.concatenate([jnp.where(picked, 0.0, trace), jnp.where(picked, trace, 0.0)], axis=0)
        high, low = split(both)
        highs.append(high)
        lows.append(low)
    at = BLOCK + 96 * direction
    return dot3(
        wh_ref[:, at : at + 96],
        wl_ref[:, at : at + 96],
        jnp.concatenate(highs, axis=1),
        jnp.concatenate(lows, axis=1),
    )


def halo_sum(part_ref, ori_ref, wh_ref, wl_ref, place_ref, gets, ad_ref):
    gx_in, gx_out, gy_in, gy_out = gets
    even_x, even_y, there = sides(place_ref)

    def lower(inside, outside, even, found):
        return lambda n: jnp.where(
            found, jnp.where(even, outside[:, lanes(n)], inside[:, lanes(n)]), 0.0
        )

    def upper(inside, outside, even, found):
        return lambda n: jnp.where(
            found, jnp.where(even, inside[:, lanes(n)], outside[:, lanes(n)]), 0.0
        )

    weights = (ori_ref, wh_ref, wl_ref)
    ad_ref[:, 0:512] = part_ref[:, 0:512] + halo_product(
        lower(gx_in, gx_out, even_x, there[0]), (0, 1, 2, 3), 0, *weights
    )
    ad_ref[:, 512:1024] = part_ref[:, 512:1024] + halo_product(
        upper(gx_in, gx_out, even_x, there[1]), (4, 5, 6, 7), 1, *weights
    )
    for cols, direction, pick in (((0, 4), 2, lower), ((3, 7), 3, upper)):
        halo = pick(gy_in, gy_out, even_y, there[direction])
        both = halo_product(halo, cols, direction, *weights)
        for n, col in enumerate(cols):
            ad_ref[:, lanes(col)] += both[:, lanes(n)]


def step_kernel(
    scales, part_ref, r_ref, d_ref, x_ref, coef_ref, ori_ref, wh_ref, wl_ref, sel_ref, place_ref,
    gx_in, gx_out, gy_in, gy_out, r_out, d_out, x_out, sx_in, sx_out, sy_in, sy_out, ad_ref,
):
    halo_sum(part_ref, ori_ref, wh_ref, wl_ref, place_ref, (gx_in, gx_out, gy_in, gy_out), ad_ref)
    keep, gain = scales
    for col in range(COLS):
        at = lanes(col)
        resid = r_ref[:, at] - ad_ref[:, at]
        step = gain * resid
        if keep:
            step = keep * d_ref[:, at] + step
        r_out[:, at] = resid
        d_out[:, at] = step
        x_out[:, at] = x_ref[:, at] + step
    emit_traces(
        lambda col: d_out[:, lanes(col)] * tile_coef(coef_ref, col),
        sel_ref,
        place_ref,
        (sx_in, sx_out, sy_in, sy_out),
    )


def last_kernel(
    part_ref, r_ref, x_ref, ori_ref, wh_ref, wl_ref, place_ref, gx_in, gx_out, gy_in, gy_out,
    x_out, r_out, ad_ref,
):
    halo_sum(part_ref, ori_ref, wh_ref, wl_ref, place_ref, (gx_in, gx_out, gy_in, gy_out), ad_ref)
    for col in range(COLS):
        at = lanes(col)
        rows = pl.ds(col, BLOCK, stride=COLS)
        x_out[rows, :] = x_ref[:, at]
        r_out[rows, :] = r_ref[:, at] - ad_ref[:, at]


def slots_kernel(agg_hbm, owner_hbm, hot_ref, agg_ref, owner_ref, sems):
    for copy in fetch(((agg_hbm, agg_ref), (owner_hbm, owner_ref)), sems):
        copy.wait()
    owner = owner_ref[...]
    owner_hot = lax.broadcasted_iota(jnp.int32, (OWNERS, AGG), 0) == owner
    before = lax.broadcasted_iota(jnp.int32, (AGG, AGG), 0) < lax.broadcasted_iota(
        jnp.int32, (AGG, AGG), 1
    )
    counts = dot(owner_hot.astype(BF16), before.astype(BF16))
    slot = jnp.sum(jnp.where(owner_hot, counts, 0.0), axis=0, keepdims=True)
    first = lax.broadcasted_iota(jnp.int32, (8, AGG), 0) == 0
    table = jnp.where(first, owner.astype(F32), slot).astype(BF16)
    for col in range(COLS):
        at = lanes(col)
        member = lax.broadcasted_iota(jnp.int32, (AGG, LANES), 0) == agg_ref[col : col + 1, :]
        found = dot(table, member.astype(BF16))
        target = (found[0:1] * float(CAP) + found[1:2]).astype(jnp.int32)
        hot = lax.broadcasted_iota(jnp.int32, (OWNERS * CAP, LANES), 0) == target
        hot_ref[:, at] = hot.astype(BF16)


def restrict_kernel(
    part_ref, r_ref, ori_ref, wh_ref, wl_ref, hot_ref, pth_ref, ptl_ref, place_ref,
    gx_in, gx_out, gy_in, gy_out, r_out, out_ref, ad_ref, rhs_ref,
):
    halo_sum(part_ref, ori_ref, wh_ref, wl_ref, place_ref, (gx_in, gx_out, gy_in, gy_out), ad_ref)
    resid = r_ref[...] - ad_ref[...]
    r_out[...] = resid
    r_high, r_low = split(resid)
    proj = dot3(pth_ref[...], ptl_ref[...], r_high, r_low)
    p_high, p_low = split(proj)
    rhs_ref[...] = dot_nt(p_high, hot_ref[...]) + dot_nt(p_low, hot_ref[...])
    group = lax.broadcasted_iota(jnp.int32, (8, LANES), 1) >> 5
    for o in range(OWNERS):
        total = jnp.zeros((8, LANES), F32)
        for q in range(3):
            moved = rhs_ref[8 * q : 8 * q + 8, lanes(o // 4)]
            if q != o % 4:
                moved = pltpu.roll(moved, 32 * ((q - o) % 4), 1)
            total = jnp.where(group == q, moved, total)
        out_ref[o] = total


def solve_kernel(rhs_ref, inv_ref, out_ref):
    pad = jnp.zeros((8, CAP), F32)
    for s in range(OWNERS):
        tile = rhs_ref[s]
        rhs = jnp.concatenate([tile[:, CAP * q : CAP * (q + 1)] for q in range(3)], axis=0)
        rows = [jnp.sum(inv_ref[s, 8 * q : 8 * q + 8] * rhs[None], axis=1) for q in range(3)]
        out_ref[s] = jnp.concatenate([*rows, pad], axis=1)


def lift_kernel(
    sol_in, x_ref, coef_ref, hot_ref, ph_ref, pl_ref, sel_ref, place_ref,
    d_out, x_out, sx_in, sx_out, sy_in, sy_out, sol_ref,
):
    group = lax.broadcasted_iota(jnp.int32, (8, LANES), 1) >> 5
    for q in range(3):
        for j in range(8):
            total = jnp.zeros((8, LANES), F32)
            for g in range(4):
                moved = sol_in[4 * j + g]
                if g != q:
                    moved = pltpu.roll(moved, 32 * ((g - q) % 4), 1)
                total = jnp.where(group == g, moved, total)
            sol_ref[8 * q : 8 * q + 8, lanes(j)] = total
    s_high, s_low = split(sol_ref[...])
    each = dot(s_high, hot_ref[...]) + dot(s_low, hot_ref[...])
    e_high, e_low = split(each)
    for half in range(2):
        span = slice(512 * half, 512 * (half + 1))
        lift = dot3(ph_ref[...], pl_ref[...], e_high[:, span], e_low[:, span])
        d_out[:, span] = lift
        x_out[:, span] = x_ref[:, span] + lift
    emit_traces(
        lambda col: d_out[:, lanes(col)] * tile_coef(coef_ref, col),
        sel_ref,
        place_ref,
        (sx_in, sx_out, sy_in, sy_out),
    )


def field(*shape, dtype=F32):
    return pltpu.VMEM(shape, dtype)


def call(kernel, outs, args, scratch=(), smem=(), hbm=(), limit=20):
    specs, placed = [], []
    for n, a in enumerate(args):
        space = pltpu.SMEM if n in smem else pltpu.HBM if n in hbm else pltpu.VMEM
        specs.append(pl.BlockSpec(memory_space=space))
        placed.append(a if n in smem else pltpu.with_memory_space_constraint(a, space))
    return pl.pallas_call(
        kernel,
        out_shape=outs,
        in_specs=specs,
        out_specs=[pl.BlockSpec(memory_space=pltpu.VMEM)] * len(outs),
        scratch_shapes=list(scratch),
        compiler_params=pltpu.CompilerParams(vmem_limit_bytes=limit << 20),
    )(*placed)


def swap_even(v, axis):
    count = lax.axis_size(axis)
    return lax.ppermute(v, axis, [(i, i ^ 1) for i in range(count)])


def swap_odd(v, axis):
    count = lax.axis_size(axis)
    return lax.ppermute(
        v, axis, [(i, (i + 1 if i % 2 else i - 1) % count) for i in range(count)]
    )


def exchange(sends):
    return (
        swap_even(sends[0], "gx"),
        swap_odd(sends[1], "gx"),
        swap_even(sends[2], "gy"),
        swap_odd(sends[3], "gy"),
    )


SENDS = [field(48, 512), field(48, 512), field(48, 256), field(48, 256)]


def shards(
    right_side,
    coefficient,
    orientation,
    aggregate_map,
    owner_map,
    stiffness,
    face_blocks,
    prolong_basis,
    coarse_inverse,
):
    shape = right_side.shape
    place = jnp.stack([lax.axis_index("gx"), lax.axis_index("gy")])
    place = jnp.concatenate(
        [place, jnp.array([lax.axis_size("gx") - 1, lax.axis_size("gy") - 1], jnp.int32)]
    )
    dma = pltpu.SemaphoreType.DMA
    full = field(BLOCK, ELEMS)
    rows = (BLOCK * COLS, LANES)
    r, d, coef, ori, sel, *sends = call(
        first_kernel,
        [full, full, field(COLS, LANES), field(6 * COLS, LANES, dtype=jnp.int32),
         field(BLOCK, BLOCK, dtype=BF16), *SENDS],
        [right_side.reshape(rows), coefficient.reshape(COLS, LANES),
         orientation.reshape(6 * COLS, LANES), jnp.asarray(selection()), place],
        scratch=[field(*rows), dma((4,))],
        smem=(4,),
        hbm=(0, 1, 2, 3),
    )
    wide = field(BLOCK, 768, dtype=BF16)
    down, up = field(CW, BLOCK, dtype=BF16), field(BLOCK, CW, dtype=BF16)
    wh, wl, pth, ptl, ph, plo = call(
        weights_kernel,
        [wide, wide, down, down, up, up],
        [stiffness, jnp.transpose(face_blocks, (0, 1, 3, 2)).reshape(576, BLOCK), prolong_basis.T],
        scratch=[field(BLOCK, BLOCK), field(576, BLOCK), field(CW, BLOCK), dma((3,))],
        hbm=(0, 1, 2),
    )
    hot = call(
        slots_kernel,
        [field(ELEMS, ELEMS, dtype=BF16)],
        [aggregate_map.reshape(COLS, LANES), owner_map.reshape(1, AGG)],
        scratch=[field(COLS, LANES, dtype=jnp.int32), field(1, AGG, dtype=jnp.int32), dma((2,))],
        hbm=(0, 1),
    )[0]

    def interior(step):
        return call(
            interior_kernel,
            [full],
            [step, coef, ori, wh, wl, sel],
            scratch=[
                pltpu.VMEM((768, ELEMS), BF16),
                pltpu.VMEM((768, ELEMS), BF16),
                pltpu.VMEM((BLOCK, ELEMS), F32),
            ],
        )[0]

    accumulator = [pltpu.VMEM((BLOCK, ELEMS), F32)]

    def advance(scales, r, d, x, sends):
        gets = exchange(sends)
        part = interior(d)
        return call(
            functools.partial(step_kernel, scales),
            [full, full, full, *SENDS],
            [part, r, d, x, coef, ori, wh, wl, sel, place, *gets],
            scratch=accumulator,
            smem=(9,),
        )

    steps = chebyshev()
    x = d
    for scales in steps:
        r, d, x, *sends = advance(scales, r, d, x, sends)
    gets = exchange(sends)
    part = interior(d)
    packets = field(OWNERS, 8, LANES)
    r, rhs = call(
        restrict_kernel,
        [full, packets],
        [part, r, ori, wh, wl, hot, pth, ptl, place, *gets],
        scratch=[*accumulator, field(CW, ELEMS)],
        smem=(8,),
    )
    rhs = lax.all_to_all(rhs, "gx", split_axis=0, concat_axis=0, tiled=True)
    inverse = jnp.transpose(coarse_inverse[0], (0, 2, 3, 1))
    sol = call(solve_kernel, [packets], [rhs, inverse])[0]
    sol = lax.all_to_all(sol, "gx", split_axis=0, concat_axis=0, tiled=True)
    d, x, *sends = call(
        lift_kernel,
        [full, full, *SENDS],
        [sol, x, coef, hot, ph, plo, sel, place],
        scratch=[pltpu.VMEM((CW, ELEMS), F32)],
        smem=(7,),
    )
    r, d, x, *sends = advance((0.0, 1.0 / THETA), r, d, x, sends)
    for scales in steps:
        r, d, x, *sends = advance(scales, r, d, x, sends)
    gets = exchange(sends)
    part = interior(d)
    x, r = call(
        last_kernel,
        [jax.ShapeDtypeStruct((BLOCK * COLS, LANES), F32)] * 2,
        [part, r, x, ori, wh, wl, place, *gets],
        scratch=accumulator,
        smem=(6,),
    )
    return x.reshape(shape), r.reshape(shape)


def solution(mesh):
    in_specs = (
        P(None, "gx", "gy", None),
        P("gx", "gy", None),
        P(None, "gx", "gy", None),
        P("gx", "gy", None),
        P(("gx", "gy"), None),
        P(),
        P(),
        P(),
        P(("gx", "gy"), None, None, None, None),
    )
    out_specs = (P(None, "gx", "gy", None), P(None, "gx", "gy", None))
    return jax.shard_map(shards, mesh=mesh, in_specs=in_specs, out_specs=out_specs, check_vma=False)
```

```python
import functools

import jax
import jax.numpy as jnp
import ml_dtypes
import numpy as np
from jax import lax
from jax.experimental import pallas as pl
from jax.experimental.pallas import tpu as pltpu
from jax.sharding import PartitionSpec as P

BLOCK = 192
TRACE = 48
CW = 24
DEGREE = 3
COLS = 8
LANES = 128
ELEMS = COLS * LANES
OWNERS = 32
CAP = 32
AGG = 512

F32 = jnp.float32
BF16 = jnp.bfloat16

THETA = 0.5 * (4.0 + 0.25)
DELTA = 0.5 * (4.0 - 0.25)
SIGMA = THETA / DELTA


def chebyshev():
    rho = 1.0 / SIGMA
    steps = []
    for _ in range(DEGREE - 1):
        rho_new = 1.0 / (2.0 * SIGMA - rho)
        steps.append((rho_new * rho, 2.0 * rho_new / DELTA))
        rho = rho_new
    return steps


def selection():
    sel = np.zeros((192, 192), np.float32)
    t = np.arange(48)
    for group, rows in enumerate(
        (16 * (t // 4) + t % 4, 16 * (t // 4) + t % 4 + 12, 4 * t, 4 * t + 3)
    ):
        sel[48 * group + t, rows] = 1.0
    return sel.astype(ml_dtypes.bfloat16)


def dot(a, b):
    return jnp.dot(a, b, preferred_element_type=F32)


def dot_nt(a, b):
    return lax.dot_general(a, b, (((1,), (1,)), ((), ())), preferred_element_type=F32)


def split(v):
    high = v.astype(BF16)
    return high, (v - high.astype(F32)).astype(BF16)


def dot3(a_high, a_low, b_high, b_low):
    return dot(a_high, b_high) + dot(a_high, b_low) + dot(a_low, b_high)


def lanes(col):
    return slice(LANES * col, LANES * (col + 1))


def face_rows(v, node):
    at = 16 * node
    return jnp.concatenate([v[64 * c + at : 64 * c + at + 16] for c in range(3)], axis=0)


def tile_coef(coef_ref, col):
    return coef_ref[col : col + 1, :]


def sides():
    at_x, at_y = lax.axis_index("gx"), lax.axis_index("gy")
    last_x, last_y = lax.axis_size("gx") - 1, lax.axis_size("gy") - 1
    return at_x % 2 == 0, at_y % 2 == 0, (at_x > 0, at_x < last_x, at_y > 0, at_y < last_y)


def y_traces(w_of, sel_ref):
    ends = []
    for y, rows in ((0, slice(0, 48)), (3, slice(48, 96))):
        high, low = split(jnp.concatenate([w_of(y), w_of(4 + y)], axis=1))
        pick = sel_ref[rows, :]
        ends.append(dot(pick, high) + dot(pick, low))
    return ends


def post(lower_x, upper_x, lower_y, upper_y, sends):
    sx_in, sx_out, sy_in, sy_out = sends
    even_x, even_y, _ = sides()
    sx_in[...] = jnp.where(even_x, upper_x, lower_x)
    sx_out[...] = jnp.where(even_x, lower_x, upper_x)
    sy_in[...] = jnp.where(even_y, upper_y, lower_y)
    sy_out[...] = jnp.where(even_y, lower_y, upper_y)


def edge_traces(w_of, sel_ref):
    lower_x = jnp.concatenate([face_rows(w_of(y), 0) for y in range(4)], axis=1)
    upper_x = jnp.concatenate([face_rows(w_of(4 + y), 3) for y in range(4)], axis=1)
    return (lower_x, upper_x, *y_traces(w_of, sel_ref))


def fetch(pairs, sems):
    copies = [pltpu.make_async_copy(a, b, sems.at[n]) for n, (a, b) in enumerate(pairs)]
    for copy in copies:
        copy.start()
    return copies


def first_kernel(
    rs_hbm, coef_hbm, ori_hbm, sel_hbm, agg_hbm, owner_hbm,
    r_ref, d_ref, coef_ref, ori_ref, sel_ref, agg_ref, owner_ref, sx_in, sx_out, sy_in, sy_out,
    rs_ref, sems,
):
    copies = fetch(
        (
            (rs_hbm, rs_ref),
            (coef_hbm, coef_ref),
            (sel_hbm, sel_ref),
            (ori_hbm, ori_ref),
            (agg_hbm, agg_ref),
            (owner_hbm, owner_ref),
        ),
        sems,
    )
    for copy in copies[:3]:
        copy.wait()
    for col in range(COLS):
        v = rs_ref[pl.ds(col, BLOCK, stride=COLS), :]
        r_ref[:, lanes(col)] = v
        d_ref[:, lanes(col)] = v * (1.0 / THETA)
    post(
        *edge_traces(lambda col: d_ref[:, lanes(col)] * tile_coef(coef_ref, col), sel_ref),
        (sx_in, sx_out, sy_in, sy_out),
    )
    for copy in copies[3:]:
        copy.wait()


def weights_kernel(
    stiff_hbm, faces_hbm, pt_hbm, sel_ref,
    wh_ref, wl_ref, halo_ref, rim_ref, pth_ref, ptl_ref, ph_ref, pl_ref,
    stiff_ref, faces_ref, pt_ref, sems,
):
    copies = fetch(((stiff_hbm, stiff_ref), (pt_hbm, pt_ref), (faces_hbm, faces_ref)), sems)
    copies[0].wait()
    high, low = split(stiff_ref[...])
    wh_ref[:, 0:BLOCK] = high
    wl_ref[:, 0:BLOCK] = low
    copies[1].wait()
    pt = pt_ref[...]
    high, low = split(pt)
    pth_ref[...] = high
    ptl_ref[...] = low
    high, low = split(pt.T)
    ph_ref[...] = high
    pl_ref[...] = low
    copies[2].wait()
    for piece in range(3):
        high, low = split(faces_ref[192 * piece : 192 * (piece + 1), :].T)
        wh_ref[:, 192 * (piece + 1) : 192 * (piece + 2)] = high
        wl_ref[:, 192 * (piece + 1) : 192 * (piece + 2)] = low
    for direction in range(4):
        at = BLOCK + 96 * direction
        high, low = wh_ref[:, at : at + 96], wl_ref[:, at : at + 96]
        stack = jnp.concatenate([high, high, low], axis=1)
        halo_ref[direction] = stack
        if direction < 2:
            near, far = face_rows(stack, 3 * direction), sel_ref[0:96, :]
            rim_ref[direction, 0:48, :] = near
            rim_ref[direction, 48:144, :] = dot(far, stack).astype(BF16)
        else:
            rim_ref[direction, 0:48, :] = face_rows(stack, 0)
            rim_ref[direction, 48:96, :] = face_rows(stack, 3)
            pick = sel_ref[48 * (direction - 2) : 48 * (direction - 1), :]
            rim_ref[direction, 96:144, :] = dot(pick, stack).astype(BF16)


def interior(d_ref, coef_ref, ori_ref, wh_ref, wl_ref, sel_ref, out_ref, xh_ref, xl_ref, t_ref):
    for col in range(COLS):
        high, low = split(d_ref[:, lanes(col)] * tile_coef(coef_ref, col))
        xh_ref[0:BLOCK, lanes(col)] = high
        xl_ref[0:BLOCK, lanes(col)] = low
    lane = lax.broadcasted_iota(jnp.int32, (48, LANES), 1)
    for x_ref in (xh_ref, xl_ref):
        t_ref[...] = dot(sel_ref[...], x_ref[0:BLOCK, :])
        for col in range(COLS):
            x, y = col // 4, col % 4
            for direction in range(6):
                trace = None
                if direction == 0 and x == 1:
                    trace = face_rows(x_ref[0:BLOCK, lanes(col - 4)], 3).astype(F32)
                elif direction == 1 and x == 0:
                    trace = face_rows(x_ref[0:BLOCK, lanes(col + 4)], 0).astype(F32)
                elif direction == 2 and y > 0:
                    trace = t_ref[48:96, lanes(col - 1)]
                elif direction == 3 and y < 3:
                    trace = t_ref[0:48, lanes(col + 1)]
                elif direction == 4:
                    trace = jnp.where(lane == 0, 0.0, pltpu.roll(t_ref[144:192, lanes(col)], 1, 1))
                elif direction == 5:
                    trace = jnp.where(
                        lane == LANES - 1, 0.0, pltpu.roll(t_ref[96:144, lanes(col)], LANES - 1, 1)
                    )
                at = BLOCK + 96 * direction
                if trace is None:
                    x_ref[at : at + 96, lanes(col)] = jnp.zeros((96, LANES), BF16)
                    continue
                row = COLS * direction + col
                picked = ori_ref[row : row + 1, :] == 1
                x_ref[at : at + 48, lanes(col)] = jnp.where(picked, 0.0, trace).astype(BF16)
                x_ref[at + 48 : at + 96, lanes(col)] = jnp.where(picked, trace, 0.0).astype(BF16)
    for half in range(2):
        span = slice(512 * half, 512 * (half + 1))
        out_ref[:, span] = dot3(wh_ref[...], wl_ref[...], xh_ref[:, span], xl_ref[:, span])


def ahead(scales, r_ref, d_ref, part_ref, coef_ref, sel_ref, pres):
    keep, gain = scales

    def w_of(col):
        at = lanes(col)
        step = gain * (r_ref[:, at] - part_ref[:, at])
        if keep:
            step = keep * d_ref[:, at] + step
        return step * tile_coef(coef_ref, col)

    for pre, value in zip(pres, edge_traces(w_of, sel_ref)):
        pre[...] = value


def start_kernel(
    scales, r_ref, d_ref, coef_ref, ori_ref, wh_ref, wl_ref, sel_ref, *rest,
):
    part_ref, *pres, xh_ref, xl_ref, t_ref = rest
    interior(d_ref, coef_ref, ori_ref, wh_ref, wl_ref, sel_ref, part_ref, xh_ref, xl_ref, t_ref)
    ahead(scales, r_ref, d_ref, part_ref, coef_ref, sel_ref, pres)


def halo_stacks(ori_ref, gets):
    gx_in, gx_out, gy_in, gy_out = gets
    even_x, even_y, found = sides()
    stacks = []
    for direction, cols in enumerate(((0, 1, 2, 3), (4, 5, 6, 7), (0, 4), (3, 7))):
        inside, outside, even = (gx_in, gx_out, even_x) if direction < 2 else (gy_in, gy_out, even_y)
        from_outside = even if direction % 2 == 0 else jnp.logical_not(even)
        parts = []
        for n, col in enumerate(cols):
            trace = jnp.where(from_outside, outside[:, lanes(n)], inside[:, lanes(n)])
            trace = jnp.where(found[direction], trace, 0.0)
            row = COLS * direction + col
            picked = ori_ref[row : row + 1, :] == 1
            both = jnp.concatenate(
                [jnp.where(picked, 0.0, trace), jnp.where(picked, trace, 0.0)], axis=0
            )
            high, low = split(both)
            parts.append(jnp.concatenate([high, low, high], axis=0))
        stacks.append(jnp.concatenate(parts, axis=1))
    return stacks


def send_kernel(gain, coef_ref, ori_ref, rim_ref, *rest):
    gets, pres, sends, stacks = rest[0:4], rest[4:8], rest[8:12], rest[12:16]
    values = halo_stacks(ori_ref, gets)
    for stack, value in zip(stacks, values):
        stack[...] = value
    from_x = [dot(rim_ref[n], values[n]) for n in range(2)]
    from_y = [dot(rim_ref[n], values[n]) for n in range(2, 4)]
    lower_x, upper_x, lower_y, upper_y = pres
    xs = []
    for x, pre in enumerate((lower_x, upper_x)):
        cols = []
        for y in range(4):
            halo = from_x[x][0:48, lanes(y)]
            if y in (0, 3):
                halo = halo + from_y[y // 3][48 * x : 48 * x + 48, lanes(x)]
            cols.append(pre[:, lanes(y)] - halo * (gain * tile_coef(coef_ref, 4 * x + y)))
        xs.append(jnp.concatenate(cols, axis=1))
    ys = []
    for end, pre in enumerate((lower_y, upper_y)):
        cols = []
        for x in range(2):
            halo = from_y[end][96:144, lanes(x)]
            halo = halo + from_x[x][48 + 48 * end : 96 + 48 * end, lanes(3 * end)]
            cols.append(pre[:, lanes(x)] - halo * (gain * tile_coef(coef_ref, 4 * x + 3 * end)))
        ys.append(jnp.concatenate(cols, axis=1))
    post(*xs, *ys, sends)


def add_halo(ad_ref, part_ref, halo_ref, values):
    ad_ref[:, 0:512] = part_ref[:, 0:512] + dot(halo_ref[0], values[0])
    ad_ref[:, 512:1024] = part_ref[:, 512:1024] + dot(halo_ref[1], values[1])
    for end in range(2):
        both = dot(halo_ref[2 + end], values[2 + end])
        for x in range(2):
            ad_ref[:, lanes(4 * x + 3 * end)] += both[:, lanes(x)]


def step_kernel(
    scales, onward, closing, part_ref, r_ref, d_ref, x_ref, coef_ref, ori_ref, wh_ref, wl_ref, sel_ref,
    halo_ref, lx_ref, ux_ref, ly_ref, uy_ref, r_out, d_out, x_out, part_out, *rest,
):
    *pres, xh_ref, xl_ref, t_ref, ad_ref = rest
    add_halo(ad_ref, part_ref, halo_ref, [v[...] for v in (lx_ref, ux_ref, ly_ref, uy_ref)])
    keep, gain = scales
    for col in range(COLS):
        at = lanes(col)
        resid = r_ref[:, at] - ad_ref[:, at]
        step = gain * resid
        if keep:
            step = keep * d_ref[:, at] + step
        r_out[:, at] = resid
        d_out[:, at] = step
        total = x_ref[:, at] + step
        if closing:
            x_out[pl.ds(col, BLOCK, stride=COLS), :] = total
        else:
            x_out[:, at] = total
    interior(d_out, coef_ref, ori_ref, wh_ref, wl_ref, sel_ref, part_out, xh_ref, xl_ref, t_ref)
    if onward is not None:
        ahead(onward, r_out, d_out, part_out, coef_ref, sel_ref, pres)


def last_kernel(part_ref, r_ref, ori_ref, halo_ref, gx_in, gx_out, gy_in, gy_out, r_out, ad_ref):
    add_halo(ad_ref, part_ref, halo_ref, halo_stacks(ori_ref, (gx_in, gx_out, gy_in, gy_out)))
    for col in range(COLS):
        at = lanes(col)
        r_out[pl.ds(col, BLOCK, stride=COLS), :] = r_ref[:, at] - ad_ref[:, at]


def slots_kernel(agg_ref, owner_ref, hot_ref):
    owner = owner_ref[...]
    owner_hot = lax.broadcasted_iota(jnp.int32, (OWNERS, AGG), 0) == owner
    before = lax.broadcasted_iota(jnp.int32, (AGG, AGG), 0) < lax.broadcasted_iota(
        jnp.int32, (AGG, AGG), 1
    )
    counts = dot(owner_hot.astype(BF16), before.astype(BF16))
    slot = jnp.sum(jnp.where(owner_hot, counts, 0.0), axis=0, keepdims=True)
    first = lax.broadcasted_iota(jnp.int32, (8, AGG), 0) == 0
    table = jnp.where(first, owner.astype(F32), slot).astype(BF16)
    for col in range(COLS):
        at = lanes(col)
        member = lax.broadcasted_iota(jnp.int32, (AGG, LANES), 0) == agg_ref[col : col + 1, :]
        found = dot(table, member.astype(BF16))
        target = (found[0:1] * float(CAP) + found[1:2]).astype(jnp.int32)
        hot = lax.broadcasted_iota(jnp.int32, (OWNERS * CAP, LANES), 0) == target
        hot_ref[:, at] = hot.astype(BF16)


def restrict_kernel(
    part_ref, r_ref, ori_ref, halo_ref, hot_ref, pth_ref, ptl_ref,
    gx_in, gx_out, gy_in, gy_out, r_out, out_ref, ad_ref, rhs_ref,
):
    add_halo(ad_ref, part_ref, halo_ref, halo_stacks(ori_ref, (gx_in, gx_out, gy_in, gy_out)))
    resid = r_ref[...] - ad_ref[...]
    r_out[...] = resid
    r_high, r_low = split(resid)
    proj = dot3(pth_ref[...], ptl_ref[...], r_high, r_low)
    p_high, p_low = split(proj)
    rhs_ref[...] = dot_nt(p_high, hot_ref[...]) + dot_nt(p_low, hot_ref[...])
    group = lax.broadcasted_iota(jnp.int32, (8, LANES), 1) >> 5
    for o in range(OWNERS):
        total = jnp.zeros((8, LANES), F32)
        for q in range(3):
            moved = rhs_ref[8 * q : 8 * q + 8, lanes(o // 4)]
            if q != o % 4:
                moved = pltpu.roll(moved, 32 * ((q - o) % 4), 1)
            total = jnp.where(group == q, moved, total)
        out_ref[o] = total


def solve_kernel(rhs_ref, inv_ref, out_ref):
    pad = jnp.zeros((8, CAP), F32)
    for s in range(OWNERS):
        tile = rhs_ref[s]
        rhs = jnp.concatenate([tile[:, CAP * q : CAP * (q + 1)] for q in range(3)], axis=0)
        rows = [jnp.sum(inv_ref[s, 8 * q : 8 * q + 8] * rhs[None], axis=1) for q in range(3)]
        out_ref[s] = jnp.concatenate([*rows, pad], axis=1)


def lift_kernel(
    sol_in, x_ref, coef_ref, hot_ref, ph_ref, pl_ref, sel_ref,
    d_out, x_out, sx_in, sx_out, sy_in, sy_out, sol_ref,
):
    group = lax.broadcasted_iota(jnp.int32, (8, LANES), 1) >> 5
    for q in range(3):
        for j in range(8):
            total = jnp.zeros((8, LANES), F32)
            for g in range(4):
                moved = sol_in[4 * j + g]
                if g != q:
                    moved = pltpu.roll(moved, 32 * ((g - q) % 4), 1)
                total = jnp.where(group == g, moved, total)
            sol_ref[8 * q : 8 * q + 8, lanes(j)] = total
    s_high, s_low = split(sol_ref[...])
    each = dot(s_high, hot_ref[...]) + dot(s_low, hot_ref[...])
    e_high, e_low = split(each)
    for half in range(2):
        span = slice(512 * half, 512 * (half + 1))
        lift = dot3(ph_ref[...], pl_ref[...], e_high[:, span], e_low[:, span])
        d_out[:, span] = lift
        x_out[:, span] = x_ref[:, span] + lift
    post(
        *edge_traces(lambda col: d_out[:, lanes(col)] * tile_coef(coef_ref, col), sel_ref),
        (sx_in, sx_out, sy_in, sy_out),
    )


def field(*shape, dtype=F32):
    return pltpu.VMEM(shape, dtype)


def call(kernel, outs, args, scratch=(), hbm=(), limit=20):
    specs, placed = [], []
    for n, a in enumerate(args):
        space = pltpu.HBM if n in hbm else pltpu.VMEM
        specs.append(pl.BlockSpec(memory_space=space))
        placed.append(pltpu.with_memory_space_constraint(a, space))
    return pl.pallas_call(
        kernel,
        out_shape=outs,
        in_specs=specs,
        out_specs=[pl.BlockSpec(memory_space=pltpu.VMEM)] * len(outs),
        scratch_shapes=list(scratch),
        compiler_params=pltpu.CompilerParams(vmem_limit_bytes=limit << 20),
    )(*placed)


def swap_even(v, axis):
    count = lax.axis_size(axis)
    return lax.ppermute(v, axis, [(i, i ^ 1) for i in range(count)])


def swap_odd(v, axis):
    count = lax.axis_size(axis)
    return lax.ppermute(
        v, axis, [(i, (i + 1 if i % 2 else i - 1) % count) for i in range(count)]
    )


def exchange(sends):
    return (
        swap_even(sends[0], "gx"),
        swap_odd(sends[1], "gx"),
        swap_even(sends[2], "gy"),
        swap_odd(sends[3], "gy"),
    )


SENDS = [field(48, 512), field(48, 512), field(48, 256), field(48, 256)]


def shards(
    right_side,
    coefficient,
    orientation,
    aggregate_map,
    owner_map,
    stiffness,
    face_blocks,
    prolong_basis,
    coarse_inverse,
):
    shape = right_side.shape
    dma = pltpu.SemaphoreType.DMA
    ints = functools.partial(field, dtype=jnp.int32)
    halves = functools.partial(field, dtype=BF16)
    full = field(BLOCK, ELEMS)
    rows = (BLOCK * COLS, LANES)
    r, d, coef, ori, sel, agg, owner, *sends = call(
        first_kernel,
        [full, full, field(COLS, LANES), ints(6 * COLS, LANES), halves(BLOCK, BLOCK),
         ints(COLS, LANES), ints(1, AGG), *SENDS],
        [right_side.reshape(rows), coefficient.reshape(COLS, LANES),
         orientation.reshape(6 * COLS, LANES), jnp.asarray(selection()),
         aggregate_map.reshape(COLS, LANES), owner_map.reshape(1, AGG)],
        scratch=[field(*rows), dma((6,))],
        hbm=(0, 1, 2, 3, 4, 5),
    )
    wide, down, up = halves(BLOCK, 768), halves(CW, BLOCK), halves(BLOCK, CW)
    wh, wl, halo, rim, pth, ptl, ph, plo = call(
        weights_kernel,
        [wide, wide, halves(4, BLOCK, 288), halves(4, 144, 288), down, down, up, up],
        [stiffness, jnp.transpose(face_blocks, (0, 1, 3, 2)).reshape(576, BLOCK), prolong_basis.T,
         sel],
        scratch=[field(BLOCK, BLOCK), field(576, BLOCK), field(CW, BLOCK), dma((3,))],
        hbm=(0, 1, 2),
    )
    hot = call(slots_kernel, [halves(ELEMS, ELEMS)], [agg, owner])[0]

    products = [halves(768, ELEMS), halves(768, ELEMS), full]
    stacks = [halves(288, 512), halves(288, 512), halves(288, 256), halves(288, 256)]
    tables = [coef, ori, wh, wl, sel]

    def start(scales, r, d):
        return call(functools.partial(start_kernel, scales), [full, *SENDS], [r, d, *tables], products)

    def step(scales, onward, part, r, d, x, gets, pres, closing=False):
        *sends, lx, ux, ly, uy = call(
            functools.partial(send_kernel, scales[1]),
            [*SENDS, *stacks],
            [coef, ori, rim, *gets, *pres],
        )
        gets = exchange(sends)
        x_out = jax.ShapeDtypeStruct(rows, F32) if closing else full
        outs = [full, full, x_out, full] + ([] if onward is None else SENDS)
        r, d, x, part, *pres = call(
            functools.partial(step_kernel, scales, onward, closing),
            outs,
            [part, r, d, x, *tables, halo, lx, ux, ly, uy],
            [*products, full],
        )
        return part, r, d, x, gets, pres

    second, third = chebyshev()
    opening = (0.0, 1.0 / THETA)
    gets = exchange(sends)
    part, *pres = start(second, r, d)
    part, r, d, x, gets, pres = step(second, third, part, r, d, d, gets, pres)
    part, r, d, x, gets, _ = step(third, None, part, r, d, x, gets, pres)
    packets = field(OWNERS, 8, LANES)
    r, rhs = call(
        restrict_kernel,
        [full, packets],
        [part, r, ori, halo, hot, pth, ptl, *gets],
        [full, field(CW, ELEMS)],
    )
    rhs = lax.all_to_all(rhs, "gx", split_axis=0, concat_axis=0, tiled=True)
    inverse = jnp.transpose(coarse_inverse[0], (0, 2, 3, 1))
    sol = call(solve_kernel, [packets], [rhs, inverse])[0]
    sol = lax.all_to_all(sol, "gx", split_axis=0, concat_axis=0, tiled=True)
    d, x, *sends = call(
        lift_kernel,
        [full, full, *SENDS],
        [sol, x, coef, hot, ph, plo, sel],
        [field(CW, ELEMS)],
    )
    gets = exchange(sends)
    part, *pres = start(opening, r, d)
    part, r, d, x, gets, pres = step(opening, second, part, r, d, x, gets, pres)
    part, r, d, x, gets, pres = step(second, third, part, r, d, x, gets, pres)
    part, r, _, x, gets, _ = step(third, None, part, r, d, x, gets, pres, closing=True)
    r = call(
        last_kernel,
        [jax.ShapeDtypeStruct(rows, F32)],
        [part, r, ori, halo, *gets],
        [full],
    )[0]
    return x.reshape(shape), r.reshape(shape)


def solution(mesh):
    in_specs = (
        P(None, "gx", "gy", None),
        P("gx", "gy", None),
        P(None, "gx", "gy", None),
        P("gx", "gy", None),
        P(("gx", "gy"), None),
        P(),
        P(),
        P(),
        P(("gx", "gy"), None, None, None, None),
    )
    out_specs = (P(None, "gx", "gy", None), P(None, "gx", "gy", None))
    return jax.shard_map(shards, mesh=mesh, in_specs=in_specs, out_specs=out_specs, check_vma=False)
```

```python
import functools

import jax
import jax.numpy as jnp
import ml_dtypes
import numpy as np
from jax import lax
from jax.experimental import pallas as pl
from jax.experimental.pallas import tpu as pltpu
from jax.sharding import PartitionSpec as P

BLOCK = 192
TRACE = 48
CW = 24
DEGREE = 3
COLS = 8
LANES = 128
ELEMS = COLS * LANES
OWNERS = 32
CAP = 32
AGG = 512

F32 = jnp.float32
BF16 = jnp.bfloat16

THETA = 0.5 * (4.0 + 0.25)
DELTA = 0.5 * (4.0 - 0.25)
SIGMA = THETA / DELTA


def chebyshev():
    rho = 1.0 / SIGMA
    steps = []
    for _ in range(DEGREE - 1):
        rho_new = 1.0 / (2.0 * SIGMA - rho)
        steps.append((rho_new * rho, 2.0 * rho_new / DELTA))
        rho = rho_new
    return steps


def selection():
    sel = np.zeros((192, 192), np.float32)
    t = np.arange(48)
    for group, rows in enumerate(
        (16 * (t // 4) + t % 4, 16 * (t // 4) + t % 4 + 12, 4 * t, 4 * t + 3)
    ):
        sel[48 * group + t, rows] = 1.0
    return sel.astype(ml_dtypes.bfloat16)


def dot(a, b):
    return jnp.dot(a, b, preferred_element_type=F32)


def dot_nt(a, b):
    return lax.dot_general(a, b, (((1,), (1,)), ((), ())), preferred_element_type=F32)


def split(v):
    high = v.astype(BF16)
    return high, (v - high.astype(F32)).astype(BF16)


def dot3(a_high, a_low, b_high, b_low):
    return dot(a_high, b_high) + dot(a_high, b_low) + dot(a_low, b_high)


def lanes(col):
    return slice(LANES * col, LANES * (col + 1))


def face_rows(v, node):
    at = 16 * node
    return jnp.concatenate([v[64 * c + at : 64 * c + at + 16] for c in range(3)], axis=0)


def tile_coef(coef_ref, col):
    return coef_ref[col : col + 1, :]


def sides():
    at_x, at_y = lax.axis_index("gx"), lax.axis_index("gy")
    last_x, last_y = lax.axis_size("gx") - 1, lax.axis_size("gy") - 1
    return at_x % 2 == 0, at_y % 2 == 0, (at_x > 0, at_x < last_x, at_y > 0, at_y < last_y)


def y_traces(w_of, sel_ref):
    ends = []
    for y, rows in ((0, slice(0, 48)), (3, slice(48, 96))):
        high, low = split(jnp.concatenate([w_of(y), w_of(4 + y)], axis=1))
        pick = sel_ref[rows, :]
        ends.append(dot(pick, high) + dot(pick, low))
    return ends


def post(lower_x, upper_x, lower_y, upper_y, sends):
    sx_in, sx_out, sy_in, sy_out = sends
    even_x, even_y, _ = sides()
    sx_in[...] = jnp.where(even_x, upper_x, lower_x)
    sx_out[...] = jnp.where(even_x, lower_x, upper_x)
    sy_in[...] = jnp.where(even_y, upper_y, lower_y)
    sy_out[...] = jnp.where(even_y, lower_y, upper_y)


def edge_traces(w_of, sel_ref):
    lower_x = jnp.concatenate([face_rows(w_of(y), 0) for y in range(4)], axis=1)
    upper_x = jnp.concatenate([face_rows(w_of(4 + y), 3) for y in range(4)], axis=1)
    return (lower_x, upper_x, *y_traces(w_of, sel_ref))


def fetch(pairs, sems):
    copies = [pltpu.make_async_copy(a, b, sems.at[n]) for n, (a, b) in enumerate(pairs)]
    for copy in copies:
        copy.start()
    return copies


def first_kernel(
    rs_hbm, coef_hbm, ori_hbm, sel_hbm, agg_hbm, owner_hbm,
    r_ref, d_ref, coef_ref, ori_ref, sel_ref, agg_ref, owner_ref, sx_in, sx_out, sy_in, sy_out,
    rs_ref, sems,
):
    copies = fetch(
        (
            (rs_hbm, rs_ref),
            (coef_hbm, coef_ref),
            (sel_hbm, sel_ref),
            (ori_hbm, ori_ref),
            (agg_hbm, agg_ref),
            (owner_hbm, owner_ref),
        ),
        sems,
    )
    for copy in copies[:3]:
        copy.wait()
    for col in range(COLS):
        v = rs_ref[pl.ds(col, BLOCK, stride=COLS), :]
        r_ref[:, lanes(col)] = v
        d_ref[:, lanes(col)] = v * (1.0 / THETA)
    post(
        *edge_traces(lambda col: d_ref[:, lanes(col)] * tile_coef(coef_ref, col), sel_ref),
        (sx_in, sx_out, sy_in, sy_out),
    )
    for copy in copies[3:]:
        copy.wait()


def stacked(v):
    high = v.astype(BF16).astype(F32)
    return jnp.concatenate([high, v - high], axis=0).astype(BF16)


def stacked3(v):
    high = v.astype(BF16).astype(F32)
    return jnp.concatenate([high, v - high, high], axis=0).astype(BF16)


def beside(v):
    high, low = split(v)
    return jnp.concatenate([high, high, low], axis=1)


def slot_table(agg_ref, owner_ref, te_ref):
    owner = owner_ref[...]
    owner_hot = lax.broadcasted_iota(jnp.int32, (OWNERS, AGG), 0) == owner
    before = lax.broadcasted_iota(jnp.int32, (AGG, AGG), 0) < lax.broadcasted_iota(
        jnp.int32, (AGG, AGG), 1
    )
    counts = dot(owner_hot.astype(BF16), before.astype(BF16))
    slot = jnp.sum(jnp.where(owner_hot, counts, 0.0), axis=0, keepdims=True)
    first = lax.broadcasted_iota(jnp.int32, (8, AGG), 0) == 0
    table = jnp.where(first, owner.astype(F32), slot).astype(BF16)
    for col in range(COLS):
        member = lax.broadcasted_iota(jnp.int32, (AGG, LANES), 0) == agg_ref[col : col + 1, :]
        found = dot(table, member.astype(BF16))
        te_ref[col : col + 1, :] = (found[0:1] * float(CAP) + found[1:2]).astype(jnp.int32)


def one_hots(te_ref, hot_ref, tall_ref):
    for col in range(COLS):
        te = te_ref[col : col + 1, :]
        hot = lax.broadcasted_iota(jnp.int32, (OWNERS * CAP, LANES), 0) == te
        hot_ref[:, lanes(col)] = hot.astype(BF16)
        te_down = jnp.broadcast_to(te, (LANES, LANES)).astype(F32).T.astype(jnp.int32)
        lane = lax.broadcasted_iota(jnp.int32, (LANES, LANES), 1)
        for tile in range(8):
            tall_ref[lanes(col), lanes(tile)] = (te_down == lane + LANES * tile).astype(BF16)


def weights_kernel(
    stiff_hbm, faces_hbm, pt_hbm, sel_ref, agg_ref, owner_ref,
    wh_ref, wl_ref, halo_ref, rim_ref, pf_ref, pt_ref, lift_ref, edge_ref, te_ref,
    stiff_ref, faces_ref, basis_ref, sems,
):
    copies = fetch(((stiff_hbm, stiff_ref), (pt_hbm, basis_ref), (faces_hbm, faces_ref)), sems)
    slot_table(agg_ref, owner_ref, te_ref)
    copies[0].wait()
    high, low = split(stiff_ref[...])
    wh_ref[:, 0:BLOCK] = high
    wl_ref[:, 0:BLOCK] = low
    copies[1].wait()
    pt = basis_ref[...]
    pt_ref[...] = stacked(pt)
    lift = beside(pt.T)
    lift_ref[...] = lift
    edge_ref[0:48, :] = face_rows(lift, 0)
    edge_ref[48:96, :] = face_rows(lift, 3)
    edge_ref[96:192, :] = dot(sel_ref[0:96, :], lift).astype(BF16)
    copies[2].wait()
    for piece in range(3):
        high, low = split(faces_ref[192 * piece : 192 * (piece + 1), :].T)
        wh_ref[:, 192 * (piece + 1) : 192 * (piece + 2)] = high
        wl_ref[:, 192 * (piece + 1) : 192 * (piece + 2)] = low
    pt_high, pt_low = split(pt)
    for direction in range(4):
        at = BLOCK + 96 * direction
        high, low = wh_ref[:, at : at + 96], wl_ref[:, at : at + 96]
        stack = jnp.concatenate([high, high, low], axis=1)
        halo_ref[direction] = stack
        pf_ref[direction] = beside(dot3(pt_high, pt_low, high, low))
        if direction < 2:
            rim_ref[direction, 0:48, :] = face_rows(stack, 3 * direction)
            rim_ref[direction, 48:144, :] = dot(sel_ref[0:96, :], stack).astype(BF16)
        else:
            rim_ref[direction, 0:48, :] = face_rows(stack, 0)
            rim_ref[direction, 48:96, :] = face_rows(stack, 3)
            pick = sel_ref[48 * (direction - 2) : 48 * (direction - 1), :]
            rim_ref[direction, 96:144, :] = dot(pick, stack).astype(BF16)


def interior(d_ref, coef_ref, ori_ref, wh_ref, wl_ref, sel_ref, out_ref, xh_ref, xl_ref, t_ref):
    for col in range(COLS):
        high, low = split(d_ref[:, lanes(col)] * tile_coef(coef_ref, col))
        xh_ref[0:BLOCK, lanes(col)] = high
        xl_ref[0:BLOCK, lanes(col)] = low
    lane = lax.broadcasted_iota(jnp.int32, (48, LANES), 1)
    for x_ref in (xh_ref, xl_ref):
        t_ref[...] = dot(sel_ref[...], x_ref[0:BLOCK, :])
        for col in range(COLS):
            x, y = col // 4, col % 4
            for direction in range(6):
                trace = None
                if direction == 0 and x == 1:
                    trace = face_rows(x_ref[0:BLOCK, lanes(col - 4)], 3).astype(F32)
                elif direction == 1 and x == 0:
                    trace = face_rows(x_ref[0:BLOCK, lanes(col + 4)], 0).astype(F32)
                elif direction == 2 and y > 0:
                    trace = t_ref[48:96, lanes(col - 1)]
                elif direction == 3 and y < 3:
                    trace = t_ref[0:48, lanes(col + 1)]
                elif direction == 4:
                    trace = jnp.where(lane == 0, 0.0, pltpu.roll(t_ref[144:192, lanes(col)], 1, 1))
                elif direction == 5:
                    trace = jnp.where(
                        lane == LANES - 1, 0.0, pltpu.roll(t_ref[96:144, lanes(col)], LANES - 1, 1)
                    )
                at = BLOCK + 96 * direction
                if trace is None:
                    x_ref[at : at + 96, lanes(col)] = jnp.zeros((96, LANES), BF16)
                    continue
                row = COLS * direction + col
                picked = ori_ref[row : row + 1, :] == 1
                x_ref[at : at + 48, lanes(col)] = jnp.where(picked, 0.0, trace).astype(BF16)
                x_ref[at + 48 : at + 96, lanes(col)] = jnp.where(picked, trace, 0.0).astype(BF16)
    for half in range(2):
        span = slice(512 * half, 512 * (half + 1))
        out_ref[:, span] = dot3(wh_ref[...], wl_ref[...], xh_ref[:, span], xl_ref[:, span])


def ahead(scales, r_ref, d_ref, part_ref, coef_ref, sel_ref, pres):
    keep, gain = scales

    def w_of(col):
        at = lanes(col)
        step = gain * (r_ref[:, at] - part_ref[:, at])
        if keep:
            step = keep * d_ref[:, at] + step
        return step * tile_coef(coef_ref, col)

    for pre, value in zip(pres, edge_traces(w_of, sel_ref)):
        pre[...] = value


def start_kernel(
    scales, r_ref, d_ref, coef_ref, ori_ref, wh_ref, wl_ref, sel_ref, *rest,
):
    part_ref, *pres, xh_ref, xl_ref, t_ref = rest
    interior(d_ref, coef_ref, ori_ref, wh_ref, wl_ref, sel_ref, part_ref, xh_ref, xl_ref, t_ref)
    ahead(scales, r_ref, d_ref, part_ref, coef_ref, sel_ref, pres)


def lifted_kernel(
    scales, part_ref, r_ref, x_ref, each_ref, coef_ref, ori_ref, wh_ref, wl_ref, sel_ref,
    halo_ref, lift_ref, lx_ref, ux_ref, ly_ref, uy_ref, r_out, x_out, part_out, *rest,
):
    *pres, xh_ref, xl_ref, t_ref, d_ref = rest
    add_halo(d_ref, part_ref, halo_ref, [v[...] for v in (lx_ref, ux_ref, ly_ref, uy_ref)])
    r_out[...] = r_ref[...] - d_ref[...]
    lift = dot(lift_ref[...], stacked3(each_ref[...]))
    d_ref[...] = lift
    x_out[...] = x_ref[...] + lift
    interior(d_ref, coef_ref, ori_ref, wh_ref, wl_ref, sel_ref, part_out, xh_ref, xl_ref, t_ref)
    ahead(scales, r_out, d_ref, part_out, coef_ref, sel_ref, pres)


def halo_stacks(ori_ref, gets):
    gx_in, gx_out, gy_in, gy_out = gets
    even_x, even_y, found = sides()
    stacks = []
    for direction, cols in enumerate(((0, 1, 2, 3), (4, 5, 6, 7), (0, 4), (3, 7))):
        inside, outside, even = (gx_in, gx_out, even_x) if direction < 2 else (gy_in, gy_out, even_y)
        from_outside = even if direction % 2 == 0 else jnp.logical_not(even)
        parts = []
        for n, col in enumerate(cols):
            trace = jnp.where(from_outside, outside[:, lanes(n)], inside[:, lanes(n)])
            trace = jnp.where(found[direction], trace, 0.0)
            row = COLS * direction + col
            picked = ori_ref[row : row + 1, :] == 1
            both = jnp.concatenate(
                [jnp.where(picked, 0.0, trace), jnp.where(picked, trace, 0.0)], axis=0
            )
            high, low = split(both)
            parts.append(jnp.concatenate([high, low, high], axis=0))
        stacks.append(jnp.concatenate(parts, axis=1))
    return stacks


def send_kernel(gain, coef_ref, ori_ref, rim_ref, *rest):
    gets, pres, sends, stacks = rest[0:4], rest[4:8], rest[8:12], rest[12:16]
    values = halo_stacks(ori_ref, gets)
    for stack, value in zip(stacks, values):
        stack[...] = value
    from_x = [dot(rim_ref[n], values[n]) for n in range(2)]
    from_y = [dot(rim_ref[n], values[n]) for n in range(2, 4)]
    lower_x, upper_x, lower_y, upper_y = pres
    xs = []
    for x, pre in enumerate((lower_x, upper_x)):
        cols = []
        for y in range(4):
            halo = from_x[x][0:48, lanes(y)]
            if y in (0, 3):
                halo = halo + from_y[y // 3][48 * x : 48 * x + 48, lanes(x)]
            cols.append(pre[:, lanes(y)] - halo * (gain * tile_coef(coef_ref, 4 * x + y)))
        xs.append(jnp.concatenate(cols, axis=1))
    ys = []
    for end, pre in enumerate((lower_y, upper_y)):
        cols = []
        for x in range(2):
            halo = from_y[end][96:144, lanes(x)]
            halo = halo + from_x[x][48 + 48 * end : 96 + 48 * end, lanes(3 * end)]
            cols.append(pre[:, lanes(x)] - halo * (gain * tile_coef(coef_ref, 4 * x + 3 * end)))
        ys.append(jnp.concatenate(cols, axis=1))
    post(*xs, *ys, sends)


def add_halo(ad_ref, part_ref, halo_ref, values):
    ad_ref[:, 0:512] = part_ref[:, 0:512] + dot(halo_ref[0], values[0])
    ad_ref[:, 512:1024] = part_ref[:, 512:1024] + dot(halo_ref[1], values[1])
    for end in range(2):
        both = dot(halo_ref[2 + end], values[2 + end])
        for x in range(2):
            ad_ref[:, lanes(4 * x + 3 * end)] += both[:, lanes(x)]


def step_kernel(
    scales, onward, then, part_ref, r_ref, d_ref, x_ref, coef_ref, ori_ref, wh_ref, wl_ref, sel_ref,
    halo_ref, lx_ref, ux_ref, ly_ref, uy_ref, *rest,
):
    if then == "hots":
        te_ref, *rest = rest
    elif then == "restrict":
        pt_ref, tall_ref, *rest = rest
    r_out, d_out, x_out, part_out, *outs, xh_ref, xl_ref, t_ref, ad_ref = rest
    add_halo(ad_ref, part_ref, halo_ref, [v[...] for v in (lx_ref, ux_ref, ly_ref, uy_ref)])
    keep, gain = scales
    for col in range(COLS):
        at = lanes(col)
        resid = r_ref[:, at] - ad_ref[:, at]
        step = gain * resid
        if keep:
            step = keep * d_ref[:, at] + step
        r_out[:, at] = resid
        d_out[:, at] = step
        total = x_ref[:, at] + step
        if then == "close":
            x_out[pl.ds(col, BLOCK, stride=COLS), :] = total
        else:
            x_out[:, at] = total
    interior(d_out, coef_ref, ori_ref, wh_ref, wl_ref, sel_ref, part_out, xh_ref, xl_ref, t_ref)
    if onward is not None:
        ahead(onward, r_out, d_out, part_out, coef_ref, sel_ref, outs[0:4])
    if then == "hots":
        one_hots(te_ref, *outs[4:6])
    elif then == "restrict":
        high, low = split(r_out[...] - part_out[...])
        both = dot(pt_ref[...], high)
        proj = both[0:CW] + both[CW:] + dot(pt_ref[0:CW, :], low)
        outs[0][...] = routed(proj, tall_ref)


def routed(v, one_hot_ref):
    both = dot(stacked(v), one_hot_ref[...])
    return both[0:CW] + both[CW:]


def last_kernel(
    part_ref, r_ref, ori_ref, halo_ref, gx_in, gx_out, gy_in, gy_out, r_hbm, ad_ref, out_ref, sems
):
    add_halo(ad_ref, part_ref, halo_ref, halo_stacks(ori_ref, (gx_in, gx_out, gy_in, gy_out)))
    copies = []
    for piece in range(3):
        rows = slice(64 * piece, 64 * (piece + 1))
        for col in range(COLS):
            at = lanes(col)
            out_ref[pl.ds(512 * piece + col, 64, stride=COLS), :] = r_ref[rows, at] - ad_ref[rows, at]
        span = pl.ds(512 * piece, 512)
        copies.append(pltpu.make_async_copy(out_ref.at[span], r_hbm.at[span], sems.at[piece]))
        copies[-1].start()
    for copy in copies:
        copy.wait()


def restrict_kernel(
    pre_ref, ori_ref, pf_ref, tall_ref, gx_in, gx_out, gy_in, gy_out,
    out_ref, lx_ref, ux_ref, ly_ref, uy_ref, rhs_ref,
):
    values = halo_stacks(ori_ref, (gx_in, gx_out, gy_in, gy_out))
    for stack, value in zip((lx_ref, ux_ref, ly_ref, uy_ref), values):
        stack[...] = value
    parts = [dot(pf_ref[n], value) for n, value in enumerate(values)]
    cols = []
    for col in range(COLS):
        x, y = col // 4, col % 4
        part = parts[x][:, lanes(y)]
        if y in (0, 3):
            part = part + parts[2 + y // 3][:, lanes(x)]
        cols.append(part)
    rhs_ref[...] = pre_ref[...] - routed(jnp.concatenate(cols, axis=1), tall_ref)
    group = lax.broadcasted_iota(jnp.int32, (8, LANES), 1) >> 5
    for o in range(OWNERS):
        total = jnp.zeros((8, LANES), F32)
        for q in range(3):
            moved = rhs_ref[8 * q : 8 * q + 8, lanes(o // 4)]
            if q != o % 4:
                moved = pltpu.roll(moved, 32 * ((q - o) % 4), 1)
            total = jnp.where(group == q, moved, total)
        out_ref[o] = total


def solve_kernel(rhs_ref, inv_ref, out_ref):
    pad = jnp.zeros((8, CAP), F32)
    for s in range(OWNERS):
        tile = rhs_ref[s]
        rhs = jnp.concatenate([tile[:, CAP * q : CAP * (q + 1)] for q in range(3)], axis=0)
        rows = [jnp.sum(inv_ref[s, 8 * q : 8 * q + 8] * rhs[None], axis=1) for q in range(3)]
        out_ref[s] = jnp.concatenate([*rows, pad], axis=1)


def lift_kernel(
    sol_in, coef_ref, hot_ref, edge_ref, each_ref, sx_in, sx_out, sy_in, sy_out, sol_ref
):
    group = lax.broadcasted_iota(jnp.int32, (8, LANES), 1) >> 5
    for q in range(3):
        for j in range(8):
            total = jnp.zeros((8, LANES), F32)
            for g in range(4):
                moved = sol_in[4 * j + g]
                if g != q:
                    moved = pltpu.roll(moved, 32 * ((g - q) % 4), 1)
                total = jnp.where(group == g, moved, total)
            sol_ref[8 * q : 8 * q + 8, lanes(j)] = total
    each = routed(sol_ref[...], hot_ref)
    each_ref[...] = each
    stack = stacked3(each)
    sides_of = []
    for n, cols in enumerate(((0, 1, 2, 3), (4, 5, 6, 7), (0, 4), (3, 7))):
        values = jnp.concatenate([stack[:, lanes(col)] for col in cols], axis=1)
        traces = dot(edge_ref[48 * n : 48 * n + 48, :], values)
        scale = jnp.concatenate([tile_coef(coef_ref, col) for col in cols], axis=1)
        sides_of.append(traces * scale)
    post(*sides_of, (sx_in, sx_out, sy_in, sy_out))


def field(*shape, dtype=F32):
    return pltpu.VMEM(shape, dtype)


def call(kernel, outs, args, scratch=(), hbm=(), limit=20, out_space=pltpu.VMEM):
    specs, placed = [], []
    for n, a in enumerate(args):
        space = pltpu.HBM if n in hbm else pltpu.VMEM
        specs.append(pl.BlockSpec(memory_space=space))
        placed.append(pltpu.with_memory_space_constraint(a, space))
    return pl.pallas_call(
        kernel,
        out_shape=outs,
        in_specs=specs,
        out_specs=[pl.BlockSpec(memory_space=out_space)] * len(outs),
        scratch_shapes=list(scratch),
        compiler_params=pltpu.CompilerParams(vmem_limit_bytes=limit << 20),
    )(*placed)


def swap_even(v, axis):
    count = lax.axis_size(axis)
    return lax.ppermute(v, axis, [(i, i ^ 1) for i in range(count)])


def swap_odd(v, axis):
    count = lax.axis_size(axis)
    return lax.ppermute(
        v, axis, [(i, (i + 1 if i % 2 else i - 1) % count) for i in range(count)]
    )


def exchange(sends):
    return (
        swap_even(sends[0], "gx"),
        swap_odd(sends[1], "gx"),
        swap_even(sends[2], "gy"),
        swap_odd(sends[3], "gy"),
    )


SENDS = [field(48, 512), field(48, 512), field(48, 256), field(48, 256)]


def shards(
    right_side,
    coefficient,
    orientation,
    aggregate_map,
    owner_map,
    stiffness,
    face_blocks,
    prolong_basis,
    coarse_inverse,
):
    shape = right_side.shape
    dma = pltpu.SemaphoreType.DMA
    ints = functools.partial(field, dtype=jnp.int32)
    halves = functools.partial(field, dtype=BF16)
    full = field(BLOCK, ELEMS)
    rows = (BLOCK * COLS, LANES)
    r, d, coef, ori, sel, agg, owner, *sends = call(
        first_kernel,
        [full, full, field(COLS, LANES), ints(6 * COLS, LANES), halves(BLOCK, BLOCK),
         ints(COLS, LANES), ints(1, AGG), *SENDS],
        [right_side.reshape(rows), coefficient.reshape(COLS, LANES),
         orientation.reshape(6 * COLS, LANES), jnp.asarray(selection()),
         aggregate_map.reshape(COLS, LANES), owner_map.reshape(1, AGG)],
        scratch=[field(*rows), dma((6,))],
        hbm=(0, 1, 2, 3, 4, 5),
    )
    wide, hots = halves(BLOCK, 768), halves(ELEMS, ELEMS)
    wh, wl, halo, rim, pf, pt, lift, edge, te = call(
        weights_kernel,
        [wide, wide, halves(4, BLOCK, 288), halves(4, 144, 288), halves(4, CW, 288),
         halves(2 * CW, BLOCK), halves(BLOCK, 3 * CW), halves(BLOCK, 3 * CW), ints(COLS, LANES)],
        [stiffness, jnp.transpose(face_blocks, (0, 1, 3, 2)).reshape(576, BLOCK), prolong_basis.T,
         sel, agg, owner],
        scratch=[field(BLOCK, BLOCK), field(576, BLOCK), field(CW, BLOCK), dma((3,))],
        hbm=(0, 1, 2),
    )

    products = [halves(768, ELEMS), halves(768, ELEMS), full]
    stacks = [halves(288, 512), halves(288, 512), halves(288, 256), halves(288, 256)]
    tables = [coef, ori, wh, wl, sel]

    def step(scales, onward, part, r, d, x, gets, pres, then=None, extra=(), extra_outs=()):
        *sends, lx, ux, ly, uy = call(
            functools.partial(send_kernel, scales[1]),
            [*SENDS, *stacks],
            [coef, ori, rim, *gets, *pres],
        )
        gets = exchange(sends)
        x_out = jax.ShapeDtypeStruct(rows, F32) if then == "close" else full
        r, d, x, part, *outs = call(
            functools.partial(step_kernel, scales, onward, then),
            [full, full, x_out, full, *([] if onward is None else SENDS), *extra_outs],
            [part, r, d, x, *tables, halo, lx, ux, ly, uy, *extra],
            [*products, full],
        )
        return part, r, d, x, gets, outs

    second, third = chebyshev()
    opening = (0.0, 1.0 / THETA)
    gets = exchange(sends)
    part, *pres = call(
        functools.partial(start_kernel, second), [full, *SENDS], [r, d, *tables], products
    )
    part, r, d, x, gets, (*pres, hot, tall) = step(
        second, third, part, r, d, d, gets, pres, "hots", [te], [hots, hots]
    )
    coarse = field(CW, ELEMS)
    part, r, d, x, gets, (pre,) = step(
        third, None, part, r, d, x, gets, pres, "restrict", [pt, tall], [coarse]
    )
    packets = field(OWNERS, 8, LANES)
    rhs, *near = call(
        restrict_kernel, [packets, *stacks], [pre, ori, pf, tall, *gets], [coarse]
    )
    rhs = lax.all_to_all(rhs, "gx", split_axis=0, concat_axis=0, tiled=True)
    inverse = jnp.transpose(coarse_inverse[0], (0, 2, 3, 1))
    sol = call(solve_kernel, [packets], [rhs, inverse])[0]
    sol = lax.all_to_all(sol, "gx", split_axis=0, concat_axis=0, tiled=True)
    each, *sends = call(lift_kernel, [coarse, *SENDS], [sol, coef, hot, edge], [coarse])
    gets = exchange(sends)
    r, x, part, *pres = call(
        functools.partial(lifted_kernel, opening),
        [full, full, full, *SENDS],
        [part, r, x, each, *tables, halo, lift, *near],
        [*products, full],
    )
    part, r, d, x, gets, pres = step(opening, second, part, r, r, x, gets, pres)
    part, r, d, x, gets, pres = step(second, third, part, r, d, x, gets, pres)
    part, r, _, x, gets, _ = step(third, None, part, r, d, x, gets, pres, "close")
    r = call(
        last_kernel,
        [jax.ShapeDtypeStruct(rows, F32)],
        [part, r, ori, halo, *gets],
        [full, field(*rows), dma((3,))],
        out_space=pltpu.HBM,
    )[0]
    return x.reshape(shape), r.reshape(shape)


def solution(mesh):
    in_specs = (
        P(None, "gx", "gy", None),
        P("gx", "gy", None),
        P(None, "gx", "gy", None),
        P("gx", "gy", None),
        P(("gx", "gy"), None),
        P(),
        P(),
        P(),
        P(("gx", "gy"), None, None, None, None),
    )
    out_specs = (P(None, "gx", "gy", None), P(None, "gx", "gy", None))
    return jax.shard_map(shards, mesh=mesh, in_specs=in_specs, out_specs=out_specs, check_vma=False)
```

```python
import functools

import jax
import jax.numpy as jnp
import ml_dtypes
import numpy as np
from jax import lax
from jax.experimental import pallas as pl
from jax.experimental.pallas import tpu as pltpu
from jax.sharding import PartitionSpec as P

BLOCK = 192
TRACE = 48
CW = 24
DEGREE = 3
COLS = 8
LANES = 128
ELEMS = COLS * LANES
OWNERS = 32
CAP = 32
AGG = 512

F32 = jnp.float32
BF16 = jnp.bfloat16

THETA = 0.5 * (4.0 + 0.25)
DELTA = 0.5 * (4.0 - 0.25)
SIGMA = THETA / DELTA


def chebyshev():
    rho = 1.0 / SIGMA
    steps = []
    for _ in range(DEGREE - 1):
        rho_new = 1.0 / (2.0 * SIGMA - rho)
        steps.append((rho_new * rho, 2.0 * rho_new / DELTA))
        rho = rho_new
    return steps


def selection():
    sel = np.zeros((192, 192), np.float32)
    t = np.arange(48)
    for group, rows in enumerate(
        (16 * (t // 4) + t % 4, 16 * (t // 4) + t % 4 + 12, 4 * t, 4 * t + 3)
    ):
        sel[48 * group + t, rows] = 1.0
    return sel.astype(ml_dtypes.bfloat16)


def dot(a, b):
    return jnp.dot(a, b, preferred_element_type=F32)


def dot_nt(a, b):
    return lax.dot_general(a, b, (((1,), (1,)), ((), ())), preferred_element_type=F32)


def split(v):
    high = v.astype(BF16)
    return high, (v - high.astype(F32)).astype(BF16)


def dot3(a_high, a_low, b_high, b_low):
    return dot(a_high, b_high) + dot(a_high, b_low) + dot(a_low, b_high)


def lanes(col):
    return slice(LANES * col, LANES * (col + 1))


def face_rows(v, node):
    at = 16 * node
    return jnp.concatenate([v[64 * c + at : 64 * c + at + 16] for c in range(3)], axis=0)


def tile_coef(coef_ref, col):
    return coef_ref[col : col + 1, :]


def sides():
    at_x, at_y = lax.axis_index("gx"), lax.axis_index("gy")
    last_x, last_y = lax.axis_size("gx") - 1, lax.axis_size("gy") - 1
    return at_x % 2 == 0, at_y % 2 == 0, (at_x > 0, at_x < last_x, at_y > 0, at_y < last_y)


def y_traces(w_of, sel_ref):
    ends = []
    for y, rows in ((0, slice(0, 48)), (3, slice(48, 96))):
        high, low = split(jnp.concatenate([w_of(y), w_of(4 + y)], axis=1))
        pick = sel_ref[rows, :]
        ends.append(dot(pick, high) + dot(pick, low))
    return ends


def post(lower_x, upper_x, lower_y, upper_y, sends):
    sx_in, sx_out, sy_in, sy_out = sends
    even_x, even_y, _ = sides()
    sx_in[...] = jnp.where(even_x, upper_x, lower_x)
    sx_out[...] = jnp.where(even_x, lower_x, upper_x)
    sy_in[...] = jnp.where(even_y, upper_y, lower_y)
    sy_out[...] = jnp.where(even_y, lower_y, upper_y)


def edge_traces(w_of, sel_ref):
    lower_x = jnp.concatenate([face_rows(w_of(y), 0) for y in range(4)], axis=1)
    upper_x = jnp.concatenate([face_rows(w_of(4 + y), 3) for y in range(4)], axis=1)
    return (lower_x, upper_x, *y_traces(w_of, sel_ref))


def fetch(pairs, sems):
    copies = [pltpu.make_async_copy(a, b, sems.at[n]) for n, (a, b) in enumerate(pairs)]
    for copy in copies:
        copy.start()
    return copies


def first_kernel(
    rs_hbm, coef_hbm, ori_hbm, sel_hbm, agg_hbm, owner_hbm, stiff_hbm, faces_hbm, pt_hbm,
    r_ref, d_ref, coef_ref, ori_ref, sel_ref, agg_ref, owner_ref, stiff_ref, faces_ref, pt_ref,
    sx_in, sx_out, sy_in, sy_out, rs_ref, sems,
):
    pieces = [pl.ds(512 * c, 512) for c in range(3)]
    copies = fetch(
        [(rs_hbm.at[piece], rs_ref.at[piece]) for piece in pieces]
        + [
            (coef_hbm, coef_ref),
            (sel_hbm, sel_ref),
            (agg_hbm, agg_ref),
            (owner_hbm, owner_ref),
            (ori_hbm, ori_ref),
            (stiff_hbm, stiff_ref),
            (pt_hbm, pt_ref),
            (faces_hbm, faces_ref),
        ],
        sems,
    )
    for c in range(3):
        copies[c].wait()
        rows = slice(64 * c, 64 * (c + 1))
        for col in range(COLS):
            v = rs_ref[pl.ds(512 * c + col, 64, stride=COLS), :]
            r_ref[rows, lanes(col)] = v
            d_ref[rows, lanes(col)] = v * (1.0 / THETA)
    for copy in copies[3:5]:
        copy.wait()
    post(
        *edge_traces(lambda col: d_ref[:, lanes(col)] * tile_coef(coef_ref, col), sel_ref),
        (sx_in, sx_out, sy_in, sy_out),
    )
    for copy in copies[5:]:
        copy.wait()


def stacked(v):
    high = v.astype(BF16).astype(F32)
    return jnp.concatenate([high, v - high], axis=0).astype(BF16)


def stacked3(v):
    high = v.astype(BF16).astype(F32)
    return jnp.concatenate([high, v - high, high], axis=0).astype(BF16)


def beside(v):
    high, low = split(v)
    return jnp.concatenate([high, high, low], axis=1)


def slot_table(agg_ref, owner_ref, te_ref):
    owner = owner_ref[...]
    owner_hot = lax.broadcasted_iota(jnp.int32, (OWNERS, AGG), 0) == owner
    before = lax.broadcasted_iota(jnp.int32, (AGG, AGG), 0) < lax.broadcasted_iota(
        jnp.int32, (AGG, AGG), 1
    )
    counts = dot(owner_hot.astype(BF16), before.astype(BF16))
    slot = jnp.sum(jnp.where(owner_hot, counts, 0.0), axis=0, keepdims=True)
    first = lax.broadcasted_iota(jnp.int32, (8, AGG), 0) == 0
    table = jnp.where(first, owner.astype(F32), slot).astype(BF16)
    for col in range(COLS):
        member = lax.broadcasted_iota(jnp.int32, (AGG, LANES), 0) == agg_ref[col : col + 1, :]
        found = dot(table, member.astype(BF16))
        te_ref[col : col + 1, :] = (found[0:1] * float(CAP) + found[1:2]).astype(jnp.int32)


def one_hots(te_ref, hot_ref, tall_ref):
    for col in range(COLS):
        te = te_ref[col : col + 1, :]
        hot = lax.broadcasted_iota(jnp.int32, (OWNERS * CAP, LANES), 0) == te
        hot = hot.astype(F32).astype(BF16)
        hot_ref[:, lanes(col)] = hot
        tall_ref[lanes(col), :] = hot.T


def weights_kernel(
    stiff_ref, faces_ref, basis_ref, sel_ref, agg_ref, owner_ref,
    wh_ref, wl_ref, halo_ref, rim_ref, pf_ref, pt_ref, lift_ref, edge_ref, te_ref,
):
    slot_table(agg_ref, owner_ref, te_ref)
    high, low = split(stiff_ref[...])
    wh_ref[:, 0:BLOCK] = high
    wl_ref[:, 0:BLOCK] = low
    pt = basis_ref[...]
    pt_ref[...] = stacked(pt)
    lift = beside(pt.T)
    lift_ref[...] = lift
    edge_ref[0:48, :] = face_rows(lift, 0)
    edge_ref[48:96, :] = face_rows(lift, 3)
    edge_ref[96:192, :] = dot(sel_ref[0:96, :], lift).astype(BF16)
    for piece in range(3):
        high, low = split(faces_ref[192 * piece : 192 * (piece + 1), :].T)
        wh_ref[:, 192 * (piece + 1) : 192 * (piece + 2)] = high
        wl_ref[:, 192 * (piece + 1) : 192 * (piece + 2)] = low
    pt_high, pt_low = split(pt)
    for direction in range(4):
        at = BLOCK + 96 * direction
        high, low = wh_ref[:, at : at + 96], wl_ref[:, at : at + 96]
        stack = jnp.concatenate([high, high, low], axis=1)
        halo_ref[direction] = stack
        pf_ref[direction] = beside(dot3(pt_high, pt_low, high, low))
        if direction < 2:
            rim_ref[direction, 0:48, :] = face_rows(stack, 3 * direction)
            rim_ref[direction, 48:144, :] = dot(sel_ref[0:96, :], stack).astype(BF16)
        else:
            rim_ref[direction, 0:48, :] = face_rows(stack, 0)
            rim_ref[direction, 48:96, :] = face_rows(stack, 3)
            pick = sel_ref[48 * (direction - 2) : 48 * (direction - 1), :]
            rim_ref[direction, 96:144, :] = dot(pick, stack).astype(BF16)


def interior(d_ref, coef_ref, ori_ref, wh_ref, wl_ref, sel_ref, out_ref, xh_ref, xl_ref, t_ref):
    for col in range(COLS):
        high, low = split(d_ref[:, lanes(col)] * tile_coef(coef_ref, col))
        xh_ref[0:BLOCK, lanes(col)] = high
        xl_ref[0:BLOCK, lanes(col)] = low
    lane = lax.broadcasted_iota(jnp.int32, (48, LANES), 1)
    for x_ref in (xh_ref, xl_ref):
        t_ref[...] = dot(sel_ref[...], x_ref[0:BLOCK, :])
        for col in range(COLS):
            x, y = col // 4, col % 4
            for direction in range(6):
                trace = None
                if direction == 0 and x == 1:
                    trace = face_rows(x_ref[0:BLOCK, lanes(col - 4)], 3).astype(F32)
                elif direction == 1 and x == 0:
                    trace = face_rows(x_ref[0:BLOCK, lanes(col + 4)], 0).astype(F32)
                elif direction == 2 and y > 0:
                    trace = t_ref[48:96, lanes(col - 1)]
                elif direction == 3 and y < 3:
                    trace = t_ref[0:48, lanes(col + 1)]
                elif direction == 4:
                    trace = jnp.where(lane == 0, 0.0, pltpu.roll(t_ref[144:192, lanes(col)], 1, 1))
                elif direction == 5:
                    trace = jnp.where(
                        lane == LANES - 1, 0.0, pltpu.roll(t_ref[96:144, lanes(col)], LANES - 1, 1)
                    )
                at = BLOCK + 96 * direction
                if trace is None:
                    x_ref[at : at + 96, lanes(col)] = jnp.zeros((96, LANES), BF16)
                    continue
                row = COLS * direction + col
                picked = ori_ref[row : row + 1, :] == 1
                x_ref[at : at + 48, lanes(col)] = jnp.where(picked, 0.0, trace).astype(BF16)
                x_ref[at + 48 : at + 96, lanes(col)] = jnp.where(picked, trace, 0.0).astype(BF16)
    for half in range(2):
        span = slice(512 * half, 512 * (half + 1))
        out_ref[:, span] = dot3(wh_ref[...], wl_ref[...], xh_ref[:, span], xl_ref[:, span])


def ahead(scales, r_ref, d_ref, part_ref, coef_ref, sel_ref, pres):
    keep, gain = scales

    def w_of(col):
        at = lanes(col)
        step = gain * (r_ref[:, at] - part_ref[:, at])
        if keep:
            step = keep * d_ref[:, at] + step
        return step * tile_coef(coef_ref, col)

    for pre, value in zip(pres, edge_traces(w_of, sel_ref)):
        pre[...] = value


def start_kernel(
    scales, r_ref, d_ref, coef_ref, ori_ref, wh_ref, wl_ref, sel_ref, *rest,
):
    part_ref, *pres, xh_ref, xl_ref, t_ref = rest
    interior(d_ref, coef_ref, ori_ref, wh_ref, wl_ref, sel_ref, part_ref, xh_ref, xl_ref, t_ref)
    ahead(scales, r_ref, d_ref, part_ref, coef_ref, sel_ref, pres)


def lifted_kernel(
    scales, part_ref, r_ref, x_ref, each_ref, coef_ref, ori_ref, wh_ref, wl_ref, sel_ref,
    halo_ref, lift_ref, lx_ref, ux_ref, ly_ref, uy_ref, r_out, x_out, part_out, *rest,
):
    *pres, xh_ref, xl_ref, t_ref, d_ref = rest
    add_halo(d_ref, part_ref, halo_ref, [v[...] for v in (lx_ref, ux_ref, ly_ref, uy_ref)])
    r_out[...] = r_ref[...] - d_ref[...]
    lift = dot(lift_ref[...], stacked3(each_ref[...]))
    d_ref[...] = lift
    x_out[...] = x_ref[...] + lift
    interior(d_ref, coef_ref, ori_ref, wh_ref, wl_ref, sel_ref, part_out, xh_ref, xl_ref, t_ref)
    ahead(scales, r_out, d_ref, part_out, coef_ref, sel_ref, pres)


def halo_stacks(ori_ref, gets):
    gx_in, gx_out, gy_in, gy_out = gets
    even_x, even_y, found = sides()
    stacks = []
    for direction, cols in enumerate(((0, 1, 2, 3), (4, 5, 6, 7), (0, 4), (3, 7))):
        inside, outside, even = (gx_in, gx_out, even_x) if direction < 2 else (gy_in, gy_out, even_y)
        from_outside = even if direction % 2 == 0 else jnp.logical_not(even)
        parts = []
        for n, col in enumerate(cols):
            trace = jnp.where(from_outside, outside[:, lanes(n)], inside[:, lanes(n)])
            trace = jnp.where(found[direction], trace, 0.0)
            row = COLS * direction + col
            picked = ori_ref[row : row + 1, :] == 1
            both = jnp.concatenate(
                [jnp.where(picked, 0.0, trace), jnp.where(picked, trace, 0.0)], axis=0
            )
            high, low = split(both)
            parts.append(jnp.concatenate([high, low, high], axis=0))
        stacks.append(jnp.concatenate(parts, axis=1))
    return stacks


def send_kernel(gain, coef_ref, ori_ref, rim_ref, *rest):
    gets, pres, sends, stacks = rest[0:4], rest[4:8], rest[8:12], rest[12:16]
    values = halo_stacks(ori_ref, gets)
    for stack, value in zip(stacks, values):
        stack[...] = value
    from_x = [dot(rim_ref[n], values[n]) for n in range(2)]
    from_y = [dot(rim_ref[n], values[n]) for n in range(2, 4)]
    lower_x, upper_x, lower_y, upper_y = pres
    xs = []
    for x, pre in enumerate((lower_x, upper_x)):
        cols = []
        for y in range(4):
            halo = from_x[x][0:48, lanes(y)]
            if y in (0, 3):
                halo = halo + from_y[y // 3][48 * x : 48 * x + 48, lanes(x)]
            cols.append(pre[:, lanes(y)] - halo * (gain * tile_coef(coef_ref, 4 * x + y)))
        xs.append(jnp.concatenate(cols, axis=1))
    ys = []
    for end, pre in enumerate((lower_y, upper_y)):
        cols = []
        for x in range(2):
            halo = from_y[end][96:144, lanes(x)]
            halo = halo + from_x[x][48 + 48 * end : 96 + 48 * end, lanes(3 * end)]
            cols.append(pre[:, lanes(x)] - halo * (gain * tile_coef(coef_ref, 4 * x + 3 * end)))
        ys.append(jnp.concatenate(cols, axis=1))
    post(*xs, *ys, sends)


def add_halo(ad_ref, part_ref, halo_ref, values):
    ad_ref[:, 0:512] = part_ref[:, 0:512] + dot(halo_ref[0], values[0])
    ad_ref[:, 512:1024] = part_ref[:, 512:1024] + dot(halo_ref[1], values[1])
    for end in range(2):
        both = dot(halo_ref[2 + end], values[2 + end])
        for x in range(2):
            ad_ref[:, lanes(4 * x + 3 * end)] += both[:, lanes(x)]


def step_kernel(
    scales, onward, then, part_ref, r_ref, d_ref, x_ref, coef_ref, ori_ref, wh_ref, wl_ref, sel_ref,
    halo_ref, lx_ref, ux_ref, ly_ref, uy_ref, *rest,
):
    if then == "hots":
        te_ref, *rest = rest
    elif then == "restrict":
        pt_ref, tall_ref, *rest = rest
    r_out, d_out, x_out, part_out, *outs, xh_ref, xl_ref, t_ref, ad_ref = rest
    add_halo(ad_ref, part_ref, halo_ref, [v[...] for v in (lx_ref, ux_ref, ly_ref, uy_ref)])
    keep, gain = scales
    for col in range(COLS):
        at = lanes(col)
        resid = r_ref[:, at] - ad_ref[:, at]
        step = gain * resid
        if keep:
            step = keep * d_ref[:, at] + step
        r_out[:, at] = resid
        d_out[:, at] = step
        total = x_ref[:, at] + step
        if then == "close":
            x_out[pl.ds(col, BLOCK, stride=COLS), :] = total
        else:
            x_out[:, at] = total
    interior(d_out, coef_ref, ori_ref, wh_ref, wl_ref, sel_ref, part_out, xh_ref, xl_ref, t_ref)
    if onward is not None:
        ahead(onward, r_out, d_out, part_out, coef_ref, sel_ref, outs[0:4])
    if then == "hots":
        one_hots(te_ref, *outs[4:6])
    elif then == "restrict":
        high, low = split(r_out[...] - part_out[...])
        both = dot(pt_ref[...], high)
        proj = both[0:CW] + both[CW:] + dot(pt_ref[0:CW, :], low)
        outs[0][...] = routed(proj, tall_ref)


def routed(v, one_hot_ref):
    both = dot(stacked(v), one_hot_ref[...])
    return both[0:CW] + both[CW:]


def last_kernel(
    part_ref, r_ref, ori_ref, halo_ref, gx_in, gx_out, gy_in, gy_out, r_hbm, ad_ref, out_ref, sems
):
    add_halo(ad_ref, part_ref, halo_ref, halo_stacks(ori_ref, (gx_in, gx_out, gy_in, gy_out)))
    copies = []
    for piece in range(3):
        rows = slice(64 * piece, 64 * (piece + 1))
        for col in range(COLS):
            at = lanes(col)
            out_ref[pl.ds(512 * piece + col, 64, stride=COLS), :] = r_ref[rows, at] - ad_ref[rows, at]
        span = pl.ds(512 * piece, 512)
        copies.append(pltpu.make_async_copy(out_ref.at[span], r_hbm.at[span], sems.at[piece]))
        copies[-1].start()
    for copy in copies:
        copy.wait()


def restrict_kernel(
    pre_ref, ori_ref, pf_ref, tall_ref, gx_in, gx_out, gy_in, gy_out,
    out_ref, lx_ref, ux_ref, ly_ref, uy_ref, rhs_ref,
):
    values = halo_stacks(ori_ref, (gx_in, gx_out, gy_in, gy_out))
    for stack, value in zip((lx_ref, ux_ref, ly_ref, uy_ref), values):
        stack[...] = value
    parts = [dot(pf_ref[n], value) for n, value in enumerate(values)]
    cols = []
    for col in range(COLS):
        x, y = col // 4, col % 4
        part = parts[x][:, lanes(y)]
        if y in (0, 3):
            part = part + parts[2 + y // 3][:, lanes(x)]
        cols.append(part)
    rhs_ref[...] = pre_ref[...] - routed(jnp.concatenate(cols, axis=1), tall_ref)
    group = lax.broadcasted_iota(jnp.int32, (8, LANES), 1) >> 5
    for o in range(OWNERS):
        total = jnp.zeros((8, LANES), F32)
        for q in range(3):
            moved = rhs_ref[8 * q : 8 * q + 8, lanes(o // 4)]
            if q != o % 4:
                moved = pltpu.roll(moved, 32 * ((q - o) % 4), 1)
            total = jnp.where(group == q, moved, total)
        out_ref[o] = total


def row_sums(tiles):
    row = lax.broadcasted_iota(jnp.int32, tiles[0].shape, 0)
    low = row < 4
    tiles = [
        jnp.where(low, p, q) + pltpu.roll(jnp.where(low, q, p), 4, 0)
        for p, q in zip(tiles[:4], tiles[4:])
    ]
    for bit in (2, 1):
        tiles = [
            jnp.where((row & bit) == 0, p + pltpu.roll(p, 8 - bit, 0), q + pltpu.roll(q, bit, 0))
            for p, q in zip(tiles[:bit], tiles[bit:])
        ]
    return tiles[0]


def solve_kernel(rhs_ref, inv_ref, out_ref):
    pad = jnp.zeros((8, CAP), F32)
    for s in range(OWNERS):
        tile = rhs_ref[s]
        parts = [tile[:, CAP * q : CAP * (q + 1)] for q in range(3)]
        rows = []
        for q in range(3):
            tiles = []
            for a in range(8 * q, 8 * q + 8):
                terms = [inv_ref[s, a, 8 * b : 8 * b + 8, :] * parts[b] for b in range(3)]
                tiles.append(terms[0] + terms[1] + terms[2])
            rows.append(row_sums(tiles))
        out_ref[s] = jnp.concatenate([*rows, pad], axis=1)


def lift_kernel(
    sol_in, coef_ref, hot_ref, edge_ref, each_ref, sx_in, sx_out, sy_in, sy_out, sol_ref
):
    group = lax.broadcasted_iota(jnp.int32, (8, LANES), 1) >> 5
    for q in range(3):
        for j in range(8):
            total = jnp.zeros((8, LANES), F32)
            for g in range(4):
                moved = sol_in[4 * j + g]
                if g != q:
                    moved = pltpu.roll(moved, 32 * ((g - q) % 4), 1)
                total = jnp.where(group == g, moved, total)
            sol_ref[8 * q : 8 * q + 8, lanes(j)] = total
    each = routed(sol_ref[...], hot_ref)
    each_ref[...] = each
    stack = stacked3(each)
    sides_of = []
    for n, cols in enumerate(((0, 1, 2, 3), (4, 5, 6, 7), (0, 4), (3, 7))):
        values = jnp.concatenate([stack[:, lanes(col)] for col in cols], axis=1)
        traces = dot(edge_ref[48 * n : 48 * n + 48, :], values)
        scale = jnp.concatenate([tile_coef(coef_ref, col) for col in cols], axis=1)
        sides_of.append(traces * scale)
    post(*sides_of, (sx_in, sx_out, sy_in, sy_out))


def field(*shape, dtype=F32):
    return pltpu.VMEM(shape, dtype)


def call(kernel, outs, args, scratch=(), hbm=(), limit=20, out_space=pltpu.VMEM):
    specs, placed = [], []
    for n, a in enumerate(args):
        space = pltpu.HBM if n in hbm else pltpu.VMEM
        specs.append(pl.BlockSpec(memory_space=space))
        placed.append(pltpu.with_memory_space_constraint(a, space))
    return pl.pallas_call(
        kernel,
        out_shape=outs,
        in_specs=specs,
        out_specs=[pl.BlockSpec(memory_space=out_space)] * len(outs),
        scratch_shapes=list(scratch),
        compiler_params=pltpu.CompilerParams(vmem_limit_bytes=limit << 20),
    )(*placed)


def swap_even(v, axis):
    count = lax.axis_size(axis)
    return lax.ppermute(v, axis, [(i, i ^ 1) for i in range(count)])


def swap_odd(v, axis):
    count = lax.axis_size(axis)
    return lax.ppermute(
        v, axis, [(i, (i + 1 if i % 2 else i - 1) % count) for i in range(count)]
    )


def exchange(sends):
    return (
        swap_even(sends[0], "gx"),
        swap_odd(sends[1], "gx"),
        swap_even(sends[2], "gy"),
        swap_odd(sends[3], "gy"),
    )


SENDS = [field(48, 512), field(48, 512), field(48, 256), field(48, 256)]


def shards(
    right_side,
    coefficient,
    orientation,
    aggregate_map,
    owner_map,
    stiffness,
    face_blocks,
    prolong_basis,
    coarse_inverse,
):
    shape = right_side.shape
    dma = pltpu.SemaphoreType.DMA
    ints = functools.partial(field, dtype=jnp.int32)
    halves = functools.partial(field, dtype=BF16)
    full = field(BLOCK, ELEMS)
    rows = (BLOCK * COLS, LANES)
    r, d, coef, ori, sel, agg, owner, stiff, faces, basis, *sends = call(
        first_kernel,
        [full, full, field(COLS, LANES), ints(6 * COLS, LANES), halves(BLOCK, BLOCK),
         ints(COLS, LANES), ints(1, AGG), field(BLOCK, BLOCK), field(576, BLOCK),
         field(CW, BLOCK), *SENDS],
        [right_side.reshape(rows), coefficient.reshape(COLS, LANES),
         orientation.reshape(6 * COLS, LANES), jnp.asarray(selection()),
         aggregate_map.reshape(COLS, LANES), owner_map.reshape(1, AGG), stiffness,
         jnp.transpose(face_blocks, (0, 1, 3, 2)).reshape(576, BLOCK), prolong_basis.T],
        scratch=[field(*rows), dma((11,))],
        hbm=tuple(range(9)),
    )
    wide, hots = halves(BLOCK, 768), halves(ELEMS, ELEMS)
    wh, wl, halo, rim, pf, pt, lift, edge, te = call(
        weights_kernel,
        [wide, wide, halves(4, BLOCK, 288), halves(4, 144, 288), halves(4, CW, 288),
         halves(2 * CW, BLOCK), halves(BLOCK, 3 * CW), halves(BLOCK, 3 * CW), ints(COLS, LANES)],
        [stiff, faces, basis, sel, agg, owner],
    )

    products = [halves(768, ELEMS), halves(768, ELEMS), full]
    stacks = [halves(288, 512), halves(288, 512), halves(288, 256), halves(288, 256)]
    tables = [coef, ori, wh, wl, sel]

    def step(scales, onward, part, r, d, x, gets, pres, then=None, extra=(), extra_outs=()):
        *sends, lx, ux, ly, uy = call(
            functools.partial(send_kernel, scales[1]),
            [*SENDS, *stacks],
            [coef, ori, rim, *gets, *pres],
        )
        gets = exchange(sends)
        x_out = jax.ShapeDtypeStruct(rows, F32) if then == "close" else full
        r, d, x, part, *outs = call(
            functools.partial(step_kernel, scales, onward, then),
            [full, full, x_out, full, *([] if onward is None else SENDS), *extra_outs],
            [part, r, d, x, *tables, halo, lx, ux, ly, uy, *extra],
            [*products, full],
        )
        return part, r, d, x, gets, outs

    second, third = chebyshev()
    opening = (0.0, 1.0 / THETA)
    gets = exchange(sends)
    part, *pres = call(
        functools.partial(start_kernel, second), [full, *SENDS], [r, d, *tables], products
    )
    part, r, d, x, gets, (*pres, hot, tall) = step(
        second, third, part, r, d, d, gets, pres, "hots", [te], [hots, hots]
    )
    coarse = field(CW, ELEMS)
    part, r, d, x, gets, (pre,) = step(
        third, None, part, r, d, x, gets, pres, "restrict", [pt, tall], [coarse]
    )
    packets = field(OWNERS, 8, LANES)
    rhs, *near = call(
        restrict_kernel, [packets, *stacks], [pre, ori, pf, tall, *gets], [coarse]
    )
    rhs = lax.all_to_all(rhs, "gx", split_axis=0, concat_axis=0, tiled=True)
    inverse = jnp.transpose(coarse_inverse[0], (0, 2, 3, 1))
    sol = call(solve_kernel, [packets], [rhs, inverse])[0]
    sol = lax.all_to_all(sol, "gx", split_axis=0, concat_axis=0, tiled=True)
    each, *sends = call(lift_kernel, [coarse, *SENDS], [sol, coef, hot, edge], [coarse])
    gets = exchange(sends)
    r, x, part, *pres = call(
        functools.partial(lifted_kernel, opening),
        [full, full, full, *SENDS],
        [part, r, x, each, *tables, halo, lift, *near],
        [*products, full],
    )
    part, r, d, x, gets, pres = step(opening, second, part, r, r, x, gets, pres)
    part, r, d, x, gets, pres = step(second, third, part, r, d, x, gets, pres)
    part, r, _, x, gets, _ = step(third, None, part, r, d, x, gets, pres, "close")
    r = call(
        last_kernel,
        [jax.ShapeDtypeStruct(rows, F32)],
        [part, r, ori, halo, *gets],
        [full, field(*rows), dma((3,))],
        out_space=pltpu.HBM,
    )[0]
    return x.reshape(shape), r.reshape(shape)


def solution(mesh):
    in_specs = (
        P(None, "gx", "gy", None),
        P("gx", "gy", None),
        P(None, "gx", "gy", None),
        P("gx", "gy", None),
        P(("gx", "gy"), None),
        P(),
        P(),
        P(),
        P(("gx", "gy"), None, None, None, None),
    )
    out_specs = (P(None, "gx", "gy", None), P(None, "gx", "gy", None))
    return jax.shard_map(shards, mesh=mesh, in_specs=in_specs, out_specs=out_specs, check_vma=False)
```

```python
import functools

import jax
import jax.numpy as jnp
import ml_dtypes
import numpy as np
from jax import lax
from jax.experimental import pallas as pl
from jax.experimental.pallas import tpu as pltpu
from jax.sharding import PartitionSpec as P

BLOCK = 192
TRACE = 48
CW = 24
DEGREE = 3
COLS = 8
LANES = 128
ELEMS = COLS * LANES
OWNERS = 32
CAP = 32
AGG = 512

F32 = jnp.float32
BF16 = jnp.bfloat16

THETA = 0.5 * (4.0 + 0.25)
DELTA = 0.5 * (4.0 - 0.25)
SIGMA = THETA / DELTA


def chebyshev():
    rho = 1.0 / SIGMA
    steps = []
    for _ in range(DEGREE - 1):
        rho_new = 1.0 / (2.0 * SIGMA - rho)
        steps.append((rho_new * rho, 2.0 * rho_new / DELTA))
        rho = rho_new
    return steps


def selection():
    sel = np.zeros((192, 192), np.float32)
    t = np.arange(48)
    for group, rows in enumerate(
        (16 * (t // 4) + t % 4, 16 * (t // 4) + t % 4 + 12, 4 * t, 4 * t + 3)
    ):
        sel[48 * group + t, rows] = 1.0
    return sel.astype(ml_dtypes.bfloat16)


def dot(a, b):
    return jnp.dot(a, b, preferred_element_type=F32)


def dot_nt(a, b):
    return lax.dot_general(a, b, (((1,), (1,)), ((), ())), preferred_element_type=F32)


def split(v):
    high = v.astype(BF16)
    return high, (v - high.astype(F32)).astype(BF16)


def dot3(a_high, a_low, b_high, b_low):
    return dot(a_high, b_high) + dot(a_high, b_low) + dot(a_low, b_high)


def lanes(col):
    return slice(LANES * col, LANES * (col + 1))


def face_rows(v, node):
    at = 16 * node
    return jnp.concatenate([v[64 * c + at : 64 * c + at + 16] for c in range(3)], axis=0)


def tile_coef(coef_ref, col):
    return coef_ref[col : col + 1, :]


def sides():
    at_x, at_y = lax.axis_index("gx"), lax.axis_index("gy")
    last_x, last_y = lax.axis_size("gx") - 1, lax.axis_size("gy") - 1
    return at_x % 2 == 0, at_y % 2 == 0, (at_x > 0, at_x < last_x, at_y > 0, at_y < last_y)


def y_traces(w_of, sel_ref):
    ends = []
    for y, rows in ((0, slice(0, 48)), (3, slice(48, 96))):
        high, low = split(jnp.concatenate([w_of(y), w_of(4 + y)], axis=1))
        pick = sel_ref[rows, :]
        ends.append(dot(pick, high) + dot(pick, low))
    return ends


def post(lower_x, upper_x, lower_y, upper_y, sends):
    sx_in, sx_out, sy_in, sy_out = sends
    even_x, even_y, _ = sides()
    sx_in[...] = jnp.where(even_x, upper_x, lower_x)
    sx_out[...] = jnp.where(even_x, lower_x, upper_x)
    sy_in[...] = jnp.where(even_y, upper_y, lower_y)
    sy_out[...] = jnp.where(even_y, lower_y, upper_y)


def edge_traces(w_of, sel_ref):
    lower_x = jnp.concatenate([face_rows(w_of(y), 0) for y in range(4)], axis=1)
    upper_x = jnp.concatenate([face_rows(w_of(4 + y), 3) for y in range(4)], axis=1)
    return (lower_x, upper_x, *y_traces(w_of, sel_ref))


def fetch(pairs, sems):
    copies = [pltpu.make_async_copy(a, b, sems.at[n]) for n, (a, b) in enumerate(pairs)]
    for copy in copies:
        copy.start()
    return copies


def first_kernel(
    rs_hbm, coef_hbm, ori_hbm, sel_hbm, agg_hbm, owner_hbm, stiff_hbm, faces_hbm, pt_hbm,
    r_ref, d_ref, coef_ref, ori_ref, sel_ref, agg_ref, owner_ref, stiff_ref, faces_ref, pt_ref,
    sx_in, sx_out, sy_in, sy_out, rs_ref, sems,
):
    pieces = [pl.ds(512 * c, 512) for c in range(3)]
    copies = fetch(
        [(rs_hbm.at[piece], rs_ref.at[piece]) for piece in pieces]
        + [
            (coef_hbm, coef_ref),
            (sel_hbm, sel_ref),
            (agg_hbm, agg_ref),
            (owner_hbm, owner_ref),
            (ori_hbm, ori_ref),
            (stiff_hbm, stiff_ref),
            (pt_hbm, pt_ref),
            (faces_hbm, faces_ref),
        ],
        sems,
    )
    for c in range(3):
        copies[c].wait()
        rows = slice(64 * c, 64 * (c + 1))
        for col in range(COLS):
            v = rs_ref[pl.ds(512 * c + col, 64, stride=COLS), :]
            r_ref[rows, lanes(col)] = v
            d_ref[rows, lanes(col)] = v * (1.0 / THETA)
    for copy in copies[3:5]:
        copy.wait()
    post(
        *edge_traces(lambda col: d_ref[:, lanes(col)] * tile_coef(coef_ref, col), sel_ref),
        (sx_in, sx_out, sy_in, sy_out),
    )
    for copy in copies[5:]:
        copy.wait()


def stacked(v):
    high = v.astype(BF16).astype(F32)
    return jnp.concatenate([high, v - high], axis=0).astype(BF16)


def stacked3(v):
    high = v.astype(BF16).astype(F32)
    return jnp.concatenate([high, v - high, high], axis=0).astype(BF16)


def beside(v):
    high, low = split(v)
    return jnp.concatenate([high, high, low], axis=1)


def slot_table(agg_ref, owner_ref, te_ref):
    owner = owner_ref[...]
    owner_hot = lax.broadcasted_iota(jnp.int32, (OWNERS, AGG), 0) == owner
    before = lax.broadcasted_iota(jnp.int32, (AGG, AGG), 0) < lax.broadcasted_iota(
        jnp.int32, (AGG, AGG), 1
    )
    counts = dot(owner_hot.astype(BF16), before.astype(BF16))
    slot = jnp.sum(jnp.where(owner_hot, counts, 0.0), axis=0, keepdims=True)
    first = lax.broadcasted_iota(jnp.int32, (8, AGG), 0) == 0
    table = jnp.where(first, owner.astype(F32), slot).astype(BF16)
    for col in range(COLS):
        member = lax.broadcasted_iota(jnp.int32, (AGG, LANES), 0) == agg_ref[col : col + 1, :]
        found = dot(table, member.astype(BF16))
        te_ref[col : col + 1, :] = (found[0:1] * float(CAP) + found[1:2]).astype(jnp.int32)


def one_hots(te_ref, hot_ref, tall_ref):
    for col in range(COLS):
        te = te_ref[col : col + 1, :]
        hot = lax.broadcasted_iota(jnp.int32, (OWNERS * CAP, LANES), 0) == te
        hot = hot.astype(F32).astype(BF16)
        hot_ref[:, lanes(col)] = hot
        tall_ref[lanes(col), :] = hot.T


def weights_kernel(
    stiff_ref, faces_ref, basis_ref, sel_ref, agg_ref, owner_ref,
    wh_ref, wl_ref, halo_ref, rim_ref, pf_ref, pt_ref, lift_ref, edge_ref, te_ref,
):
    slot_table(agg_ref, owner_ref, te_ref)
    high, low = split(stiff_ref[...])
    wh_ref[:, 0:BLOCK] = high
    wl_ref[:, 0:BLOCK] = low
    pt = basis_ref[...]
    pt_ref[...] = stacked(pt)
    lift = beside(pt.T)
    lift_ref[...] = lift
    edge_ref[0:48, :] = face_rows(lift, 0)
    edge_ref[48:96, :] = face_rows(lift, 3)
    edge_ref[96:192, :] = dot(sel_ref[0:96, :], lift).astype(BF16)
    for piece in range(3):
        high, low = split(faces_ref[192 * piece : 192 * (piece + 1), :].T)
        wh_ref[:, 192 * (piece + 1) : 192 * (piece + 2)] = high
        wl_ref[:, 192 * (piece + 1) : 192 * (piece + 2)] = low
    pt_high, pt_low = split(pt)
    for direction in range(4):
        at = BLOCK + 96 * direction
        high, low = wh_ref[:, at : at + 96], wl_ref[:, at : at + 96]
        stack = jnp.concatenate([high, high, low], axis=1)
        halo_ref[direction] = stack
        pf_ref[direction] = beside(dot3(pt_high, pt_low, high, low))
        if direction < 2:
            rim_ref[direction, 0:48, :] = face_rows(stack, 3 * direction)
            rim_ref[direction, 48:144, :] = dot(sel_ref[0:96, :], stack).astype(BF16)
        else:
            rim_ref[direction, 0:48, :] = face_rows(stack, 0)
            rim_ref[direction, 48:96, :] = face_rows(stack, 3)
            pick = sel_ref[48 * (direction - 2) : 48 * (direction - 1), :]
            rim_ref[direction, 96:144, :] = dot(pick, stack).astype(BF16)


def interior(d_ref, coef_ref, ori_ref, wh_ref, wl_ref, sel_ref, out_ref, xh_ref, xl_ref, t_ref):
    for col in range(COLS):
        high, low = split(d_ref[:, lanes(col)] * tile_coef(coef_ref, col))
        xh_ref[0:BLOCK, lanes(col)] = high
        xl_ref[0:BLOCK, lanes(col)] = low
    lane = lax.broadcasted_iota(jnp.int32, (48, LANES), 1)
    for x_ref in (xh_ref, xl_ref):
        t_ref[...] = dot(sel_ref[...], x_ref[0:BLOCK, :])
        for col in range(COLS):
            x, y = col // 4, col % 4
            for direction in range(6):
                trace = None
                if direction == 0 and x == 1:
                    trace = face_rows(x_ref[0:BLOCK, lanes(col - 4)], 3).astype(F32)
                elif direction == 1 and x == 0:
                    trace = face_rows(x_ref[0:BLOCK, lanes(col + 4)], 0).astype(F32)
                elif direction == 2 and y > 0:
                    trace = t_ref[48:96, lanes(col - 1)]
                elif direction == 3 and y < 3:
                    trace = t_ref[0:48, lanes(col + 1)]
                elif direction == 4:
                    trace = jnp.where(lane == 0, 0.0, pltpu.roll(t_ref[144:192, lanes(col)], 1, 1))
                elif direction == 5:
                    trace = jnp.where(
                        lane == LANES - 1, 0.0, pltpu.roll(t_ref[96:144, lanes(col)], LANES - 1, 1)
                    )
                at = BLOCK + 96 * direction
                if trace is None:
                    x_ref[at : at + 96, lanes(col)] = jnp.zeros((96, LANES), BF16)
                    continue
                row = COLS * direction + col
                picked = ori_ref[row : row + 1, :] == 1
                x_ref[at : at + 48, lanes(col)] = jnp.where(picked, 0.0, trace).astype(BF16)
                x_ref[at + 48 : at + 96, lanes(col)] = jnp.where(picked, trace, 0.0).astype(BF16)
    for half in range(2):
        span = slice(512 * half, 512 * (half + 1))
        out_ref[:, span] = dot3(wh_ref[...], wl_ref[...], xh_ref[:, span], xl_ref[:, span])


def ahead(scales, r_ref, d_ref, part_ref, coef_ref, sel_ref, pres):
    keep, gain = scales

    def w_of(col):
        at = lanes(col)
        step = gain * (r_ref[:, at] - part_ref[:, at])
        if keep:
            step = keep * d_ref[:, at] + step
        return step * tile_coef(coef_ref, col)

    for pre, value in zip(pres, edge_traces(w_of, sel_ref)):
        pre[...] = value


def start_kernel(
    scales, r_ref, d_ref, coef_ref, ori_ref, wh_ref, wl_ref, sel_ref, inner_ref, *rest,
):
    part_ref, inner_out, *pres, xh_ref, xl_ref, t_ref = rest
    inner_out[...] = inner_ref[...]
    interior(d_ref, coef_ref, ori_ref, wh_ref, wl_ref, sel_ref, part_ref, xh_ref, xl_ref, t_ref)
    ahead(scales, r_ref, d_ref, part_ref, coef_ref, sel_ref, pres)


def lifted_kernel(
    scales, part_ref, r_ref, x_ref, each_ref, coef_ref, ori_ref, wh_ref, wl_ref, sel_ref,
    halo_ref, lift_ref, lx_ref, ux_ref, ly_ref, uy_ref, inner_ref,
    r_out, x_out, part_out, inner_out, *rest,
):
    *pres, xh_ref, xl_ref, t_ref, d_ref = rest
    inner_out[...] = inner_ref[...]
    add_halo(d_ref, part_ref, halo_ref, [v[...] for v in (lx_ref, ux_ref, ly_ref, uy_ref)])
    r_out[...] = r_ref[...] - d_ref[...]
    lift = dot(lift_ref[...], stacked3(each_ref[...]))
    d_ref[...] = lift
    x_out[...] = x_ref[...] + lift
    interior(d_ref, coef_ref, ori_ref, wh_ref, wl_ref, sel_ref, part_out, xh_ref, xl_ref, t_ref)
    ahead(scales, r_out, d_ref, part_out, coef_ref, sel_ref, pres)


def halo_stacks(ori_ref, gets):
    gx_in, gx_out, gy_in, gy_out = gets
    even_x, even_y, found = sides()
    stacks = []
    for direction, cols in enumerate(((0, 1, 2, 3), (4, 5, 6, 7), (0, 4), (3, 7))):
        inside, outside, even = (gx_in, gx_out, even_x) if direction < 2 else (gy_in, gy_out, even_y)
        from_outside = even if direction % 2 == 0 else jnp.logical_not(even)
        parts = []
        for n, col in enumerate(cols):
            trace = jnp.where(from_outside, outside[:, lanes(n)], inside[:, lanes(n)])
            trace = jnp.where(found[direction], trace, 0.0)
            row = COLS * direction + col
            picked = ori_ref[row : row + 1, :] == 1
            both = jnp.concatenate(
                [jnp.where(picked, 0.0, trace), jnp.where(picked, trace, 0.0)], axis=0
            )
            high, low = split(both)
            parts.append(jnp.concatenate([high, low, high], axis=0))
        stacks.append(jnp.concatenate(parts, axis=1))
    return stacks


def send_kernel(gain, coef_ref, ori_ref, rim_ref, *rest):
    gets, pres, sends, stacks = rest[0:4], rest[4:8], rest[8:12], rest[12:16]
    values = halo_stacks(ori_ref, gets)
    for stack, value in zip(stacks, values):
        stack[...] = value
    from_x = [dot(rim_ref[n], values[n]) for n in range(2)]
    from_y = [dot(rim_ref[n], values[n]) for n in range(2, 4)]
    lower_x, upper_x, lower_y, upper_y = pres
    xs = []
    for x, pre in enumerate((lower_x, upper_x)):
        cols = []
        for y in range(4):
            halo = from_x[x][0:48, lanes(y)]
            if y in (0, 3):
                halo = halo + from_y[y // 3][48 * x : 48 * x + 48, lanes(x)]
            cols.append(pre[:, lanes(y)] - halo * (gain * tile_coef(coef_ref, 4 * x + y)))
        xs.append(jnp.concatenate(cols, axis=1))
    ys = []
    for end, pre in enumerate((lower_y, upper_y)):
        cols = []
        for x in range(2):
            halo = from_y[end][96:144, lanes(x)]
            halo = halo + from_x[x][48 + 48 * end : 96 + 48 * end, lanes(3 * end)]
            cols.append(pre[:, lanes(x)] - halo * (gain * tile_coef(coef_ref, 4 * x + 3 * end)))
        ys.append(jnp.concatenate(cols, axis=1))
    post(*xs, *ys, sends)


def add_halo(ad_ref, part_ref, halo_ref, values):
    ad_ref[:, 0:512] = part_ref[:, 0:512] + dot(halo_ref[0], values[0])
    ad_ref[:, 512:1024] = part_ref[:, 512:1024] + dot(halo_ref[1], values[1])
    for end in range(2):
        both = dot(halo_ref[2 + end], values[2 + end])
        for x in range(2):
            ad_ref[:, lanes(4 * x + 3 * end)] += both[:, lanes(x)]


def step_kernel(
    scales, onward, then, part_ref, r_ref, d_ref, x_ref, coef_ref, ori_ref, wh_ref, wl_ref, sel_ref,
    halo_ref, lx_ref, ux_ref, ly_ref, uy_ref, inner_ref, *rest,
):
    if then == "hots":
        te_ref, *rest = rest
    elif then == "restrict":
        pt_ref, tall_ref, *rest = rest
    r_out, d_out, x_out, part_out, inner_out, *outs, xh_ref, xl_ref, t_ref, ad_ref = rest
    inner_out[...] = inner_ref[...]
    add_halo(ad_ref, part_ref, halo_ref, [v[...] for v in (lx_ref, ux_ref, ly_ref, uy_ref)])
    keep, gain = scales
    for col in range(COLS):
        at = lanes(col)
        resid = r_ref[:, at] - ad_ref[:, at]
        step = gain * resid
        if keep:
            step = keep * d_ref[:, at] + step
        r_out[:, at] = resid
        d_out[:, at] = step
        total = x_ref[:, at] + step
        if then == "close":
            x_out[pl.ds(col, BLOCK, stride=COLS), :] = total
        else:
            x_out[:, at] = total
    interior(d_out, coef_ref, ori_ref, wh_ref, wl_ref, sel_ref, part_out, xh_ref, xl_ref, t_ref)
    if onward is not None:
        ahead(onward, r_out, d_out, part_out, coef_ref, sel_ref, outs[0:4])
    if then == "hots":
        one_hots(te_ref, *outs[4:6])
    elif then == "restrict":
        high, low = split(r_out[...] - part_out[...])
        both = dot(pt_ref[...], high)
        proj = both[0:CW] + both[CW:] + dot(pt_ref[0:CW, :], low)
        outs[0][...] = routed(proj, tall_ref)


def routed(v, one_hot_ref):
    both = dot(stacked(v), one_hot_ref[...])
    return both[0:CW] + both[CW:]


def last_kernel(
    part_ref, r_ref, ori_ref, halo_ref, gx_in, gx_out, gy_in, gy_out, r_hbm, ad_ref, out_ref, sems
):
    add_halo(ad_ref, part_ref, halo_ref, halo_stacks(ori_ref, (gx_in, gx_out, gy_in, gy_out)))
    copies = []
    for piece in range(3):
        rows = slice(64 * piece, 64 * (piece + 1))
        for col in range(COLS):
            at = lanes(col)
            out_ref[pl.ds(512 * piece + col, 64, stride=COLS), :] = r_ref[rows, at] - ad_ref[rows, at]
        span = pl.ds(512 * piece, 512)
        copies.append(pltpu.make_async_copy(out_ref.at[span], r_hbm.at[span], sems.at[piece]))
        copies[-1].start()
    for copy in copies:
        copy.wait()


def restrict_kernel(
    pre_ref, ori_ref, pf_ref, tall_ref, gx_in, gx_out, gy_in, gy_out,
    out_ref, lx_ref, ux_ref, ly_ref, uy_ref, rhs_ref,
):
    values = halo_stacks(ori_ref, (gx_in, gx_out, gy_in, gy_out))
    for stack, value in zip((lx_ref, ux_ref, ly_ref, uy_ref), values):
        stack[...] = value
    parts = [dot(pf_ref[n], value) for n, value in enumerate(values)]
    cols = []
    for col in range(COLS):
        x, y = col // 4, col % 4
        part = parts[x][:, lanes(y)]
        if y in (0, 3):
            part = part + parts[2 + y // 3][:, lanes(x)]
        cols.append(part)
    rhs_ref[...] = pre_ref[...] - routed(jnp.concatenate(cols, axis=1), tall_ref)
    group = lax.broadcasted_iota(jnp.int32, (8, LANES), 1) >> 5
    for o in range(OWNERS):
        total = jnp.zeros((8, LANES), F32)
        for q in range(3):
            moved = rhs_ref[8 * q : 8 * q + 8, lanes(o // 4)]
            if q != o % 4:
                moved = pltpu.roll(moved, 32 * ((q - o) % 4), 1)
            total = jnp.where(group == q, moved, total)
        out_ref[o] = total


def row_sums(tiles):
    row = lax.broadcasted_iota(jnp.int32, tiles[0].shape, 0)
    low = row < 4
    tiles = [
        jnp.where(low, p, q) + pltpu.roll(jnp.where(low, q, p), 4, 0)
        for p, q in zip(tiles[:4], tiles[4:])
    ]
    for bit in (2, 1):
        tiles = [
            jnp.where((row & bit) == 0, p + pltpu.roll(p, 8 - bit, 0), q + pltpu.roll(q, bit, 0))
            for p, q in zip(tiles[:bit], tiles[bit:])
        ]
    return tiles[0]


def solve_kernel(rhs_ref, inv_ref, out_ref):
    pad = jnp.zeros((8, CAP), F32)
    for s in range(OWNERS):
        tile = rhs_ref[s]
        parts = [tile[:, CAP * q : CAP * (q + 1)] for q in range(3)]
        rows = []
        for q in range(3):
            tiles = []
            for a in range(8 * q, 8 * q + 8):
                terms = [inv_ref[s, a, 8 * b : 8 * b + 8, :] * parts[b] for b in range(3)]
                tiles.append(terms[0] + terms[1] + terms[2])
            rows.append(row_sums(tiles))
        out_ref[s] = jnp.concatenate([*rows, pad], axis=1)


def lift_kernel(
    sol_in, coef_ref, hot_ref, edge_ref, each_ref, sx_in, sx_out, sy_in, sy_out, sol_ref
):
    group = lax.broadcasted_iota(jnp.int32, (8, LANES), 1) >> 5
    for q in range(3):
        for j in range(8):
            total = jnp.zeros((8, LANES), F32)
            for g in range(4):
                moved = sol_in[4 * j + g]
                if g != q:
                    moved = pltpu.roll(moved, 32 * ((g - q) % 4), 1)
                total = jnp.where(group == g, moved, total)
            sol_ref[8 * q : 8 * q + 8, lanes(j)] = total
    each = routed(sol_ref[...], hot_ref)
    each_ref[...] = each
    stack = stacked3(each)
    sides_of = []
    for n, cols in enumerate(((0, 1, 2, 3), (4, 5, 6, 7), (0, 4), (3, 7))):
        values = jnp.concatenate([stack[:, lanes(col)] for col in cols], axis=1)
        traces = dot(edge_ref[48 * n : 48 * n + 48, :], values)
        scale = jnp.concatenate([tile_coef(coef_ref, col) for col in cols], axis=1)
        sides_of.append(traces * scale)
    post(*sides_of, (sx_in, sx_out, sy_in, sy_out))


def field(*shape, dtype=F32):
    return pltpu.VMEM(shape, dtype)


def call(kernel, outs, args, scratch=(), hbm=(), limit=20, out_space=pltpu.VMEM):
    specs, placed = [], []
    for n, a in enumerate(args):
        space = pltpu.HBM if n in hbm else pltpu.VMEM
        specs.append(pl.BlockSpec(memory_space=space))
        placed.append(pltpu.with_memory_space_constraint(a, space))
    return pl.pallas_call(
        kernel,
        out_shape=outs,
        in_specs=specs,
        out_specs=[pl.BlockSpec(memory_space=out_space)] * len(outs),
        scratch_shapes=list(scratch),
        compiler_params=pltpu.CompilerParams(vmem_limit_bytes=limit << 20),
    )(*placed)


def swap_even(v, axis):
    count = lax.axis_size(axis)
    return lax.ppermute(v, axis, [(i, i ^ 1) for i in range(count)])


def swap_odd(v, axis):
    count = lax.axis_size(axis)
    return lax.ppermute(
        v, axis, [(i, (i + 1 if i % 2 else i - 1) % count) for i in range(count)]
    )


def outward(sends):
    return swap_odd(sends[1], "gx"), swap_even(sends[2], "gy"), swap_odd(sends[3], "gy")


def inward(inner):
    return swap_even(inner, "gx")


INNER = pltpu.VMEM((48, 512), F32)
SENDS = [field(48, 512), field(48, 512), field(48, 256), field(48, 256)]


def shards(
    right_side,
    coefficient,
    orientation,
    aggregate_map,
    owner_map,
    stiffness,
    face_blocks,
    prolong_basis,
    coarse_inverse,
):
    shape = right_side.shape
    dma = pltpu.SemaphoreType.DMA
    ints = functools.partial(field, dtype=jnp.int32)
    halves = functools.partial(field, dtype=BF16)
    full = field(BLOCK, ELEMS)
    rows = (BLOCK * COLS, LANES)
    r, d, coef, ori, sel, agg, owner, stiff, faces, basis, *sends = call(
        first_kernel,
        [full, full, field(COLS, LANES), ints(6 * COLS, LANES), halves(BLOCK, BLOCK),
         ints(COLS, LANES), ints(1, AGG), field(BLOCK, BLOCK), field(576, BLOCK),
         field(CW, BLOCK), *SENDS],
        [right_side.reshape(rows), coefficient.reshape(COLS, LANES),
         orientation.reshape(6 * COLS, LANES), jnp.asarray(selection()),
         aggregate_map.reshape(COLS, LANES), owner_map.reshape(1, AGG), stiffness,
         jnp.transpose(face_blocks, (0, 1, 3, 2)).reshape(576, BLOCK), prolong_basis.T],
        scratch=[field(*rows), dma((11,))],
        hbm=tuple(range(9)),
    )
    wide, hots = halves(BLOCK, 768), halves(ELEMS, ELEMS)
    wh, wl, halo, rim, pf, pt, lift, edge, te = call(
        weights_kernel,
        [wide, wide, halves(4, BLOCK, 288), halves(4, 144, 288), halves(4, CW, 288),
         halves(2 * CW, BLOCK), halves(BLOCK, 3 * CW), halves(BLOCK, 3 * CW), ints(COLS, LANES)],
        [stiff, faces, basis, sel, agg, owner],
    )

    products = [halves(768, ELEMS), halves(768, ELEMS), full]
    stacks = [halves(288, 512), halves(288, 512), halves(288, 256), halves(288, 256)]
    tables = [coef, ori, wh, wl, sel]

    def step(scales, onward, part, r, d, x, gets, pres, then=None, extra=(), extra_outs=()):
        *sends, lx, ux, ly, uy = call(
            functools.partial(send_kernel, scales[1]),
            [*SENDS, *stacks],
            [coef, ori, rim, *gets, *pres],
        )
        gets = outward(sends)
        x_out = jax.ShapeDtypeStruct(rows, F32) if then == "close" else full
        r, d, x, part, inner, *outs = call(
            functools.partial(step_kernel, scales, onward, then),
            [full, full, x_out, full, INNER, *([] if onward is None else SENDS), *extra_outs],
            [part, r, d, x, *tables, halo, lx, ux, ly, uy, sends[0], *extra],
            [*products, full],
        )
        return part, r, d, x, (inward(inner), *gets), outs

    second, third = chebyshev()
    opening = (0.0, 1.0 / THETA)
    gets = outward(sends)
    part, inner, *pres = call(
        functools.partial(start_kernel, second),
        [full, INNER, *SENDS],
        [r, d, *tables, sends[0]],
        products,
    )
    gets = (inward(inner), *gets)
    part, r, d, x, gets, (*pres, hot, tall) = step(
        second, third, part, r, d, d, gets, pres, "hots", [te], [hots, hots]
    )
    coarse = field(CW, ELEMS)
    part, r, d, x, gets, (pre,) = step(
        third, None, part, r, d, x, gets, pres, "restrict", [pt, tall], [coarse]
    )
    packets = field(OWNERS, 8, LANES)
    rhs, *near = call(
        restrict_kernel, [packets, *stacks], [pre, ori, pf, tall, *gets], [coarse]
    )
    rhs = lax.all_to_all(rhs, "gx", split_axis=0, concat_axis=0, tiled=True)
    inverse = jnp.transpose(coarse_inverse[0], (0, 2, 3, 1))
    sol = call(solve_kernel, [packets], [rhs, inverse])[0]
    sol = lax.all_to_all(sol, "gx", split_axis=0, concat_axis=0, tiled=True)
    each, *sends = call(lift_kernel, [coarse, *SENDS], [sol, coef, hot, edge], [coarse])
    gets = outward(sends)
    r, x, part, inner, *pres = call(
        functools.partial(lifted_kernel, opening),
        [full, full, full, INNER, *SENDS],
        [part, r, x, each, *tables, halo, lift, *near, sends[0]],
        [*products, full],
    )
    gets = (inward(inner), *gets)
    part, r, d, x, gets, pres = step(opening, second, part, r, r, x, gets, pres)
    part, r, d, x, gets, pres = step(second, third, part, r, d, x, gets, pres)
    part, r, _, x, gets, _ = step(third, None, part, r, d, x, gets, pres, "close")
    r = call(
        last_kernel,
        [jax.ShapeDtypeStruct(rows, F32)],
        [part, r, ori, halo, *gets],
        [full, field(*rows), dma((3,))],
        out_space=pltpu.HBM,
    )[0]
    return x.reshape(shape), r.reshape(shape)


def solution(mesh):
    in_specs = (
        P(None, "gx", "gy", None),
        P("gx", "gy", None),
        P(None, "gx", "gy", None),
        P("gx", "gy", None),
        P(("gx", "gy"), None),
        P(),
        P(),
        P(),
        P(("gx", "gy"), None, None, None, None),
    )
    out_specs = (P(None, "gx", "gy", None), P(None, "gx", "gy", None))
    return jax.shard_map(shards, mesh=mesh, in_specs=in_specs, out_specs=out_specs, check_vma=False)
```

```python
import functools

import jax
import jax.numpy as jnp
import ml_dtypes
import numpy as np
from jax import lax
from jax.experimental import pallas as pl
from jax.experimental.pallas import tpu as pltpu
from jax.sharding import PartitionSpec as P

BLOCK = 192
TRACE = 48
CW = 24
DEGREE = 3
COLS = 8
LANES = 128
ELEMS = COLS * LANES
OWNERS = 32
CAP = 32
AGG = 512

F32 = jnp.float32
BF16 = jnp.bfloat16

THETA = 0.5 * (4.0 + 0.25)
DELTA = 0.5 * (4.0 - 0.25)
SIGMA = THETA / DELTA


def chebyshev():
    rho = 1.0 / SIGMA
    steps = []
    for _ in range(DEGREE - 1):
        rho_new = 1.0 / (2.0 * SIGMA - rho)
        steps.append((rho_new * rho, 2.0 * rho_new / DELTA))
        rho = rho_new
    return steps


def selection():
    sel = np.zeros((192, 192), np.float32)
    t = np.arange(48)
    for group, rows in enumerate(
        (16 * (t // 4) + t % 4, 16 * (t // 4) + t % 4 + 12, 4 * t, 4 * t + 3)
    ):
        sel[48 * group + t, rows] = 1.0
    return sel.astype(ml_dtypes.bfloat16)


def dot(a, b):
    return jnp.dot(a, b, preferred_element_type=F32)


def dot_nt(a, b):
    return lax.dot_general(a, b, (((1,), (1,)), ((), ())), preferred_element_type=F32)


def split(v):
    high = v.astype(BF16)
    return high, (v - high.astype(F32)).astype(BF16)


def dot3(a_high, a_low, b_high, b_low):
    return dot(a_high, b_high) + dot(a_high, b_low) + dot(a_low, b_high)


def lanes(col):
    return slice(LANES * col, LANES * (col + 1))


def face_rows(v, node):
    at = 16 * node
    return jnp.concatenate([v[64 * c + at : 64 * c + at + 16] for c in range(3)], axis=0)


def tile_coef(coef_ref, col):
    return coef_ref[col : col + 1, :]


def sides():
    at_x, at_y = lax.axis_index("gx"), lax.axis_index("gy")
    last_x, last_y = lax.axis_size("gx") - 1, lax.axis_size("gy") - 1
    return at_x % 2 == 0, at_y % 2 == 0, (at_x > 0, at_x < last_x, at_y > 0, at_y < last_y)


def y_traces(w_of, sel_ref):
    ends = []
    for y, rows in ((0, slice(0, 48)), (3, slice(48, 96))):
        high, low = split(jnp.concatenate([w_of(y), w_of(4 + y)], axis=1))
        pick = sel_ref[rows, :]
        ends.append(dot(pick, high) + dot(pick, low))
    return ends


def post(lower_x, upper_x, lower_y, upper_y, sends):
    sx_in, sx_out, sy_in, sy_out = sends
    even_x, even_y, _ = sides()
    sx_in[...] = jnp.where(even_x, upper_x, lower_x)
    sx_out[...] = jnp.where(even_x, lower_x, upper_x)
    sy_in[...] = jnp.where(even_y, upper_y, lower_y)
    sy_out[...] = jnp.where(even_y, lower_y, upper_y)


def edge_traces(w_of, sel_ref):
    lower_x = jnp.concatenate([face_rows(w_of(y), 0) for y in range(4)], axis=1)
    upper_x = jnp.concatenate([face_rows(w_of(4 + y), 3) for y in range(4)], axis=1)
    return (lower_x, upper_x, *y_traces(w_of, sel_ref))


def fetch(pairs, sems):
    copies = [pltpu.make_async_copy(a, b, sems.at[n]) for n, (a, b) in enumerate(pairs)]
    for copy in copies:
        copy.start()
    return copies


def first_kernel(
    rs_hbm, coef_hbm, ori_hbm, sel_hbm, agg_hbm, owner_hbm, stiff_hbm, pt_hbm,
    r_ref, d_ref, coef_ref, ori_ref, sel_ref, agg_ref, owner_ref, stiff_ref, pt_ref,
    sx_in, sx_out, sy_in, sy_out, rs_ref, sems,
):
    pieces = [pl.ds(512 * c, 512) for c in range(3)]
    copies = fetch(
        [(rs_hbm.at[piece], rs_ref.at[piece]) for piece in pieces]
        + [
            (coef_hbm, coef_ref),
            (sel_hbm, sel_ref),
            (agg_hbm, agg_ref),
            (owner_hbm, owner_ref),
            (ori_hbm, ori_ref),
            (stiff_hbm, stiff_ref),
            (pt_hbm, pt_ref),
        ],
        sems,
    )
    for c in range(3):
        copies[c].wait()
        rows = slice(64 * c, 64 * (c + 1))
        for col in range(COLS):
            v = rs_ref[pl.ds(512 * c + col, 64, stride=COLS), :]
            r_ref[rows, lanes(col)] = v
            d_ref[rows, lanes(col)] = v * (1.0 / THETA)
    for copy in copies[3:5]:
        copy.wait()
    post(
        *edge_traces(lambda col: d_ref[:, lanes(col)] * tile_coef(coef_ref, col), sel_ref),
        (sx_in, sx_out, sy_in, sy_out),
    )
    for copy in copies[5:]:
        copy.wait()


def stacked(v):
    high = v.astype(BF16).astype(F32)
    return jnp.concatenate([high, v - high], axis=0).astype(BF16)


def stacked3(v):
    high = v.astype(BF16).astype(F32)
    return jnp.concatenate([high, v - high, high], axis=0).astype(BF16)


def beside(v):
    high, low = split(v)
    return jnp.concatenate([high, high, low], axis=1)


def slot_table(agg_ref, owner_ref, te_ref):
    owner = owner_ref[...]
    owner_hot = lax.broadcasted_iota(jnp.int32, (OWNERS, AGG), 0) == owner
    before = lax.broadcasted_iota(jnp.int32, (AGG, AGG), 0) < lax.broadcasted_iota(
        jnp.int32, (AGG, AGG), 1
    )
    counts = dot(owner_hot.astype(BF16), before.astype(BF16))
    slot = jnp.sum(jnp.where(owner_hot, counts, 0.0), axis=0, keepdims=True)
    first = lax.broadcasted_iota(jnp.int32, (8, AGG), 0) == 0
    table = jnp.where(first, owner.astype(F32), slot).astype(BF16)
    for col in range(COLS):
        member = lax.broadcasted_iota(jnp.int32, (AGG, LANES), 0) == agg_ref[col : col + 1, :]
        found = dot(table, member.astype(BF16))
        te_ref[col : col + 1, :] = (found[0:1] * float(CAP) + found[1:2]).astype(jnp.int32)


def one_hots(te_ref, hot_ref, tall_ref):
    for col in range(COLS):
        te = te_ref[col : col + 1, :]
        hot = lax.broadcasted_iota(jnp.int32, (OWNERS * CAP, LANES), 0) == te
        hot = hot.astype(F32).astype(BF16)
        hot_ref[:, lanes(col)] = hot
        tall_ref[lanes(col), :] = hot.T


def weights_kernel(
    stiff_ref, faces_hbm, basis_ref, sel_ref, agg_ref, owner_ref,
    wh_ref, wl_ref, halo_ref, rim_ref, pf_ref, pt_ref, lift_ref, edge_ref, te_ref, faces_ref, sems,
):
    halves = [pl.ds(0, 384), pl.ds(384, 192)]
    copies = fetch([(faces_hbm.at[half], faces_ref.at[half]) for half in halves], sems)
    slot_table(agg_ref, owner_ref, te_ref)
    high, low = split(stiff_ref[...])
    wh_ref[:, 0:BLOCK] = high
    wl_ref[:, 0:BLOCK] = low
    pt = basis_ref[...]
    pt_ref[...] = stacked(pt)
    lift = beside(pt.T)
    lift_ref[...] = lift
    edge_ref[0:48, :] = face_rows(lift, 0)
    edge_ref[48:96, :] = face_rows(lift, 3)
    edge_ref[96:192, :] = dot(sel_ref[0:96, :], lift).astype(BF16)
    for piece in range(3):
        if piece != 1:
            copies[piece // 2].wait()
        high, low = split(faces_ref[192 * piece : 192 * (piece + 1), :].T)
        wh_ref[:, 192 * (piece + 1) : 192 * (piece + 2)] = high
        wl_ref[:, 192 * (piece + 1) : 192 * (piece + 2)] = low
    pt_high, pt_low = split(pt)
    for direction in range(4):
        at = BLOCK + 96 * direction
        high, low = wh_ref[:, at : at + 96], wl_ref[:, at : at + 96]
        stack = jnp.concatenate([high, high, low], axis=1)
        halo_ref[direction] = stack
        pf_ref[direction] = beside(dot3(pt_high, pt_low, high, low))
        if direction < 2:
            rim_ref[direction, 0:48, :] = face_rows(stack, 3 * direction)
            rim_ref[direction, 48:144, :] = dot(sel_ref[0:96, :], stack).astype(BF16)
        else:
            rim_ref[direction, 0:48, :] = face_rows(stack, 0)
            rim_ref[direction, 48:96, :] = face_rows(stack, 3)
            pick = sel_ref[48 * (direction - 2) : 48 * (direction - 1), :]
            rim_ref[direction, 96:144, :] = dot(pick, stack).astype(BF16)


def interior(d_ref, coef_ref, ori_ref, wh_ref, wl_ref, sel_ref, out_ref, xh_ref, xl_ref, t_ref):
    for col in range(COLS):
        high, low = split(d_ref[:, lanes(col)] * tile_coef(coef_ref, col))
        xh_ref[0:BLOCK, lanes(col)] = high
        xl_ref[0:BLOCK, lanes(col)] = low
    lane = lax.broadcasted_iota(jnp.int32, (48, LANES), 1)
    for x_ref in (xh_ref, xl_ref):
        t_ref[...] = dot(sel_ref[...], x_ref[0:BLOCK, :])
        for col in range(COLS):
            x, y = col // 4, col % 4
            for direction in range(6):
                trace = None
                if direction == 0 and x == 1:
                    trace = face_rows(x_ref[0:BLOCK, lanes(col - 4)], 3).astype(F32)
                elif direction == 1 and x == 0:
                    trace = face_rows(x_ref[0:BLOCK, lanes(col + 4)], 0).astype(F32)
                elif direction == 2 and y > 0:
                    trace = t_ref[48:96, lanes(col - 1)]
                elif direction == 3 and y < 3:
                    trace = t_ref[0:48, lanes(col + 1)]
                elif direction == 4:
                    trace = jnp.where(lane == 0, 0.0, pltpu.roll(t_ref[144:192, lanes(col)], 1, 1))
                elif direction == 5:
                    trace = jnp.where(
                        lane == LANES - 1, 0.0, pltpu.roll(t_ref[96:144, lanes(col)], LANES - 1, 1)
                    )
                at = BLOCK + 96 * direction
                if trace is None:
                    x_ref[at : at + 96, lanes(col)] = jnp.zeros((96, LANES), BF16)
                    continue
                row = COLS * direction + col
                picked = ori_ref[row : row + 1, :] == 1
                x_ref[at : at + 48, lanes(col)] = jnp.where(picked, 0.0, trace).astype(BF16)
                x_ref[at + 48 : at + 96, lanes(col)] = jnp.where(picked, trace, 0.0).astype(BF16)
    for half in range(2):
        span = slice(512 * half, 512 * (half + 1))
        out_ref[:, span] = dot3(wh_ref[...], wl_ref[...], xh_ref[:, span], xl_ref[:, span])


def ahead(scales, r_ref, d_ref, part_ref, coef_ref, sel_ref, pres):
    keep, gain = scales

    def w_of(col):
        at = lanes(col)
        step = gain * (r_ref[:, at] - part_ref[:, at])
        if keep:
            step = keep * d_ref[:, at] + step
        return step * tile_coef(coef_ref, col)

    for pre, value in zip(pres, edge_traces(w_of, sel_ref)):
        pre[...] = value


def start_kernel(
    scales, r_ref, d_ref, coef_ref, ori_ref, wh_ref, wl_ref, sel_ref, *rest,
):
    part_ref, *pres, xh_ref, xl_ref, t_ref = rest
    interior(d_ref, coef_ref, ori_ref, wh_ref, wl_ref, sel_ref, part_ref, xh_ref, xl_ref, t_ref)
    ahead(scales, r_ref, d_ref, part_ref, coef_ref, sel_ref, pres)


def lifted_kernel(
    scales, part_ref, r_ref, x_ref, each_ref, coef_ref, ori_ref, wh_ref, wl_ref, sel_ref,
    halo_ref, lift_ref, lx_ref, ux_ref, ly_ref, uy_ref, r_out, x_out, part_out, *rest,
):
    *pres, xh_ref, xl_ref, t_ref, d_ref = rest
    add_halo(d_ref, part_ref, halo_ref, [v[...] for v in (lx_ref, ux_ref, ly_ref, uy_ref)])
    r_out[...] = r_ref[...] - d_ref[...]
    lift = dot(lift_ref[...], stacked3(each_ref[...]))
    d_ref[...] = lift
    x_out[...] = x_ref[...] + lift
    interior(d_ref, coef_ref, ori_ref, wh_ref, wl_ref, sel_ref, part_out, xh_ref, xl_ref, t_ref)
    ahead(scales, r_out, d_ref, part_out, coef_ref, sel_ref, pres)


def halo_stacks(ori_ref, gets):
    gx_in, gx_out, gy_in, gy_out = gets
    even_x, even_y, found = sides()
    stacks = []
    for direction, cols in enumerate(((0, 1, 2, 3), (4, 5, 6, 7), (0, 4), (3, 7))):
        inside, outside, even = (gx_in, gx_out, even_x) if direction < 2 else (gy_in, gy_out, even_y)
        from_outside = even if direction % 2 == 0 else jnp.logical_not(even)
        parts = []
        for n, col in enumerate(cols):
            trace = jnp.where(from_outside, outside[:, lanes(n)], inside[:, lanes(n)])
            trace = jnp.where(found[direction], trace, 0.0)
            row = COLS * direction + col
            picked = ori_ref[row : row + 1, :] == 1
            both = jnp.concatenate(
                [jnp.where(picked, 0.0, trace), jnp.where(picked, trace, 0.0)], axis=0
            )
            high, low = split(both)
            parts.append(jnp.concatenate([high, low, high], axis=0))
        stacks.append(jnp.concatenate(parts, axis=1))
    return stacks


def send_kernel(gain, coef_ref, ori_ref, rim_ref, *rest):
    gets, pres, sends, stacks = rest[0:4], rest[4:8], rest[8:12], rest[12:16]
    values = halo_stacks(ori_ref, gets)
    for stack, value in zip(stacks, values):
        stack[...] = value
    from_x = [dot(rim_ref[n], values[n]) for n in range(2)]
    from_y = [dot(rim_ref[n], values[n]) for n in range(2, 4)]
    lower_x, upper_x, lower_y, upper_y = pres
    xs = []
    for x, pre in enumerate((lower_x, upper_x)):
        cols = []
        for y in range(4):
            halo = from_x[x][0:48, lanes(y)]
            if y in (0, 3):
                halo = halo + from_y[y // 3][48 * x : 48 * x + 48, lanes(x)]
            cols.append(pre[:, lanes(y)] - halo * (gain * tile_coef(coef_ref, 4 * x + y)))
        xs.append(jnp.concatenate(cols, axis=1))
    ys = []
    for end, pre in enumerate((lower_y, upper_y)):
        cols = []
        for x in range(2):
            halo = from_y[end][96:144, lanes(x)]
            halo = halo + from_x[x][48 + 48 * end : 96 + 48 * end, lanes(3 * end)]
            cols.append(pre[:, lanes(x)] - halo * (gain * tile_coef(coef_ref, 4 * x + 3 * end)))
        ys.append(jnp.concatenate(cols, axis=1))
    post(*xs, *ys, sends)


def add_halo(ad_ref, part_ref, halo_ref, values):
    ad_ref[:, 0:512] = part_ref[:, 0:512] + dot(halo_ref[0], values[0])
    ad_ref[:, 512:1024] = part_ref[:, 512:1024] + dot(halo_ref[1], values[1])
    for end in range(2):
        both = dot(halo_ref[2 + end], values[2 + end])
        for x in range(2):
            ad_ref[:, lanes(4 * x + 3 * end)] += both[:, lanes(x)]


def step_kernel(
    scales, onward, then, part_ref, r_ref, d_ref, x_ref, coef_ref, ori_ref, wh_ref, wl_ref, sel_ref,
    halo_ref, lx_ref, ux_ref, ly_ref, uy_ref, *rest,
):
    if then == "hots":
        te_ref, *rest = rest
    elif then == "restrict":
        pt_ref, *rest = rest
    r_out, d_out, x_out, part_out, *outs, xh_ref, xl_ref, t_ref, ad_ref = rest
    add_halo(ad_ref, part_ref, halo_ref, [v[...] for v in (lx_ref, ux_ref, ly_ref, uy_ref)])
    keep, gain = scales
    for col in range(COLS):
        at = lanes(col)
        resid = r_ref[:, at] - ad_ref[:, at]
        step = gain * resid
        if keep:
            step = keep * d_ref[:, at] + step
        r_out[:, at] = resid
        d_out[:, at] = step
        total = x_ref[:, at] + step
        if then == "close":
            x_out[pl.ds(col, BLOCK, stride=COLS), :] = total
        else:
            x_out[:, at] = total
    interior(d_out, coef_ref, ori_ref, wh_ref, wl_ref, sel_ref, part_out, xh_ref, xl_ref, t_ref)
    if onward is not None:
        ahead(onward, r_out, d_out, part_out, coef_ref, sel_ref, outs[0:4])
    if then == "hots":
        one_hots(te_ref, *outs[4:6])
    elif then == "restrict":
        high, low = split(r_out[...] - part_out[...])
        both = dot(pt_ref[...], high)
        outs[0][...] = both[0:CW] + both[CW:] + dot(pt_ref[0:CW, :], low)


def routed(v, one_hot_ref):
    both = dot(stacked(v), one_hot_ref[...])
    return both[0:CW] + both[CW:]


def last_kernel(
    part_ref, r_ref, ori_ref, halo_ref, gx_in, gx_out, gy_in, gy_out, r_hbm, ad_ref, out_ref, sems
):
    add_halo(ad_ref, part_ref, halo_ref, halo_stacks(ori_ref, (gx_in, gx_out, gy_in, gy_out)))
    copies = []
    for piece in range(3):
        rows = slice(64 * piece, 64 * (piece + 1))
        for col in range(COLS):
            at = lanes(col)
            out_ref[pl.ds(512 * piece + col, 64, stride=COLS), :] = r_ref[rows, at] - ad_ref[rows, at]
        span = pl.ds(512 * piece, 512)
        copies.append(pltpu.make_async_copy(out_ref.at[span], r_hbm.at[span], sems.at[piece]))
        copies[-1].start()
    for copy in copies:
        copy.wait()


def restrict_kernel(
    pre_ref, ori_ref, pf_ref, tall_ref, gx_in, gx_out, gy_in, gy_out,
    out_ref, lx_ref, ux_ref, ly_ref, uy_ref, rhs_ref,
):
    values = halo_stacks(ori_ref, (gx_in, gx_out, gy_in, gy_out))
    for stack, value in zip((lx_ref, ux_ref, ly_ref, uy_ref), values):
        stack[...] = value
    parts = [dot(pf_ref[n], value) for n, value in enumerate(values)]
    cols = []
    for col in range(COLS):
        x, y = col // 4, col % 4
        part = parts[x][:, lanes(y)]
        if y in (0, 3):
            part = part + parts[2 + y // 3][:, lanes(x)]
        cols.append(part)
    rhs_ref[...] = routed(pre_ref[...] - jnp.concatenate(cols, axis=1), tall_ref)
    group = lax.broadcasted_iota(jnp.int32, (8, LANES), 1) >> 5
    for o in range(OWNERS):
        total = jnp.zeros((8, LANES), F32)
        for q in range(3):
            moved = rhs_ref[8 * q : 8 * q + 8, lanes(o // 4)]
            if q != o % 4:
                moved = pltpu.roll(moved, 32 * ((q - o) % 4), 1)
            total = jnp.where(group == q, moved, total)
        out_ref[o] = total


def row_sums(tiles):
    row = lax.broadcasted_iota(jnp.int32, tiles[0].shape, 0)
    low = row < 4
    tiles = [
        jnp.where(low, p, q) + pltpu.roll(jnp.where(low, q, p), 4, 0)
        for p, q in zip(tiles[:4], tiles[4:])
    ]
    for bit in (2, 1):
        tiles = [
            jnp.where((row & bit) == 0, p + pltpu.roll(p, 8 - bit, 0), q + pltpu.roll(q, bit, 0))
            for p, q in zip(tiles[:bit], tiles[bit:])
        ]
    return tiles[0]


def solve_kernel(rhs_ref, inv_ref, out_ref):
    pad = jnp.zeros((8, CAP), F32)
    for s in range(OWNERS):
        tile = rhs_ref[s]
        parts = [tile[:, CAP * q : CAP * (q + 1)] for q in range(3)]
        rows = []
        for q in range(3):
            tiles = []
            for a in range(8 * q, 8 * q + 8):
                terms = [inv_ref[s, a, 8 * b : 8 * b + 8, :] * parts[b] for b in range(3)]
                tiles.append(terms[0] + terms[1] + terms[2])
            rows.append(row_sums(tiles))
        out_ref[s] = jnp.concatenate([*rows, pad], axis=1)


def lift_kernel(
    sol_in, coef_ref, hot_ref, edge_ref, each_ref, sx_in, sx_out, sy_in, sy_out, sol_ref
):
    group = lax.broadcasted_iota(jnp.int32, (8, LANES), 1) >> 5
    for q in range(3):
        for j in range(8):
            total = jnp.zeros((8, LANES), F32)
            for g in range(4):
                moved = sol_in[4 * j + g]
                if g != q:
                    moved = pltpu.roll(moved, 32 * ((g - q) % 4), 1)
                total = jnp.where(group == g, moved, total)
            sol_ref[8 * q : 8 * q + 8, lanes(j)] = total
    each = routed(sol_ref[...], hot_ref)
    each_ref[...] = each
    stack = stacked3(each)
    sides_of = []
    for n, cols in enumerate(((0, 1, 2, 3), (4, 5, 6, 7), (0, 4), (3, 7))):
        values = jnp.concatenate([stack[:, lanes(col)] for col in cols], axis=1)
        traces = dot(edge_ref[48 * n : 48 * n + 48, :], values)
        scale = jnp.concatenate([tile_coef(coef_ref, col) for col in cols], axis=1)
        sides_of.append(traces * scale)
    post(*sides_of, (sx_in, sx_out, sy_in, sy_out))


def field(*shape, dtype=F32):
    return pltpu.VMEM(shape, dtype)


def call(kernel, outs, args, scratch=(), hbm=(), limit=20, out_space=pltpu.VMEM):
    specs, placed = [], []
    for n, a in enumerate(args):
        space = pltpu.HBM if n in hbm else pltpu.VMEM
        specs.append(pl.BlockSpec(memory_space=space))
        placed.append(pltpu.with_memory_space_constraint(a, space))
    return pl.pallas_call(
        kernel,
        out_shape=outs,
        in_specs=specs,
        out_specs=[pl.BlockSpec(memory_space=out_space)] * len(outs),
        scratch_shapes=list(scratch),
        compiler_params=pltpu.CompilerParams(vmem_limit_bytes=limit << 20),
    )(*placed)


def swap_even(v, axis):
    count = lax.axis_size(axis)
    return lax.ppermute(v, axis, [(i, i ^ 1) for i in range(count)])


def swap_odd(v, axis):
    count = lax.axis_size(axis)
    return lax.ppermute(
        v, axis, [(i, (i + 1 if i % 2 else i - 1) % count) for i in range(count)]
    )


def exchange(sends):
    return (
        swap_even(sends[0], "gx"),
        swap_odd(sends[1], "gx"),
        swap_even(sends[2], "gy"),
        swap_odd(sends[3], "gy"),
    )


SENDS = [field(48, 512), field(48, 512), field(48, 256), field(48, 256)]


def shards(
    right_side,
    coefficient,
    orientation,
    aggregate_map,
    owner_map,
    stiffness,
    face_blocks,
    prolong_basis,
    coarse_inverse,
):
    shape = right_side.shape
    dma = pltpu.SemaphoreType.DMA
    ints = functools.partial(field, dtype=jnp.int32)
    halves = functools.partial(field, dtype=BF16)
    full = field(BLOCK, ELEMS)
    rows = (BLOCK * COLS, LANES)
    r, d, coef, ori, sel, agg, owner, stiff, basis, *sends = call(
        first_kernel,
        [full, full, field(COLS, LANES), ints(6 * COLS, LANES), halves(BLOCK, BLOCK),
         ints(COLS, LANES), ints(1, AGG), field(BLOCK, BLOCK), field(CW, BLOCK), *SENDS],
        [right_side.reshape(rows), coefficient.reshape(COLS, LANES),
         orientation.reshape(6 * COLS, LANES), jnp.asarray(selection()),
         aggregate_map.reshape(COLS, LANES), owner_map.reshape(1, AGG), stiffness,
         prolong_basis.T],
        scratch=[field(*rows), dma((10,))],
        hbm=tuple(range(8)),
    )
    wide, hots = halves(BLOCK, 768), halves(ELEMS, ELEMS)
    wh, wl, halo, rim, pf, pt, lift, edge, te = call(
        weights_kernel,
        [wide, wide, halves(4, BLOCK, 288), halves(4, 144, 288), halves(4, CW, 288),
         halves(2 * CW, BLOCK), halves(BLOCK, 3 * CW), halves(BLOCK, 3 * CW), ints(COLS, LANES)],
        [stiff, jnp.transpose(face_blocks, (0, 1, 3, 2)).reshape(576, BLOCK), basis, sel, agg, owner],
        scratch=[field(576, BLOCK), dma((2,))],
        hbm=(1,),
    )

    products = [halves(768, ELEMS), halves(768, ELEMS), full]
    stacks = [halves(288, 512), halves(288, 512), halves(288, 256), halves(288, 256)]
    tables = [coef, ori, wh, wl, sel]

    def step(scales, onward, part, r, d, x, gets, pres, then=None, extra=(), extra_outs=()):
        *sends, lx, ux, ly, uy = call(
            functools.partial(send_kernel, scales[1]),
            [*SENDS, *stacks],
            [coef, ori, rim, *gets, *pres],
        )
        gets = exchange(sends)
        x_out = jax.ShapeDtypeStruct(rows, F32) if then == "close" else full
        r, d, x, part, *outs = call(
            functools.partial(step_kernel, scales, onward, then),
            [full, full, x_out, full, *([] if onward is None else SENDS), *extra_outs],
            [part, r, d, x, *tables, halo, lx, ux, ly, uy, *extra],
            [*products, full],
        )
        return part, r, d, x, gets, outs

    second, third = chebyshev()
    opening = (0.0, 1.0 / THETA)
    gets = exchange(sends)
    part, *pres = call(
        functools.partial(start_kernel, second), [full, *SENDS], [r, d, *tables], products
    )
    part, r, d, x, gets, (*pres, hot, tall) = step(
        second, third, part, r, d, d, gets, pres, "hots", [te], [hots, hots]
    )
    coarse = field(CW, ELEMS)
    part, r, d, x, gets, (pre,) = step(
        third, None, part, r, d, x, gets, pres, "restrict", [pt], [coarse]
    )
    packets = field(OWNERS, 8, LANES)
    rhs, *near = call(
        restrict_kernel, [packets, *stacks], [pre, ori, pf, tall, *gets], [coarse]
    )
    rhs = lax.all_to_all(rhs, "gx", split_axis=0, concat_axis=0, tiled=True)
    inverse = jnp.transpose(coarse_inverse[0], (0, 2, 3, 1))
    sol = call(solve_kernel, [packets], [rhs, inverse])[0]
    sol = lax.all_to_all(sol, "gx", split_axis=0, concat_axis=0, tiled=True)
    each, *sends = call(lift_kernel, [coarse, *SENDS], [sol, coef, hot, edge], [coarse])
    gets = exchange(sends)
    r, x, part, *pres = call(
        functools.partial(lifted_kernel, opening),
        [full, full, full, *SENDS],
        [part, r, x, each, *tables, halo, lift, *near],
        [*products, full],
    )
    part, r, d, x, gets, pres = step(opening, second, part, r, r, x, gets, pres)
    part, r, d, x, gets, pres = step(second, third, part, r, d, x, gets, pres)
    part, r, _, x, gets, _ = step(third, None, part, r, d, x, gets, pres, "close")
    r = call(
        last_kernel,
        [jax.ShapeDtypeStruct(rows, F32)],
        [part, r, ori, halo, *gets],
        [full, field(*rows), dma((3,))],
        out_space=pltpu.HBM,
    )[0]
    return x.reshape(shape), r.reshape(shape)


def solution(mesh):
    in_specs = (
        P(None, "gx", "gy", None),
        P("gx", "gy", None),
        P(None, "gx", "gy", None),
        P("gx", "gy", None),
        P(("gx", "gy"), None),
        P(),
        P(),
        P(),
        P(("gx", "gy"), None, None, None, None),
    )
    out_specs = (P(None, "gx", "gy", None), P(None, "gx", "gy", None))
    return jax.shard_map(shards, mesh=mesh, in_specs=in_specs, out_specs=out_specs, check_vma=False)
```

```python
import functools

import jax
import jax.numpy as jnp
import ml_dtypes
import numpy as np
from jax import lax
from jax.experimental import pallas as pl
from jax.experimental.pallas import tpu as pltpu
from jax.sharding import PartitionSpec as P

BLOCK = 192
TRACE = 48
CW = 24
DEGREE = 3
COLS = 8
LANES = 128
ELEMS = COLS * LANES
OWNERS = 32
CAP = 32
AGG = 512

F32 = jnp.float32
BF16 = jnp.bfloat16

THETA = 0.5 * (4.0 + 0.25)
DELTA = 0.5 * (4.0 - 0.25)
SIGMA = THETA / DELTA


def chebyshev():
    rho = 1.0 / SIGMA
    steps = []
    for _ in range(DEGREE - 1):
        rho_new = 1.0 / (2.0 * SIGMA - rho)
        steps.append((rho_new * rho, 2.0 * rho_new / DELTA))
        rho = rho_new
    return steps


def selection():
    sel = np.zeros((192, 192), np.float32)
    t = np.arange(48)
    for group, rows in enumerate(
        (16 * (t // 4) + t % 4, 16 * (t // 4) + t % 4 + 12, 4 * t, 4 * t + 3)
    ):
        sel[48 * group + t, rows] = 1.0
    return sel.astype(ml_dtypes.bfloat16)


def dot(a, b):
    return jnp.dot(a, b, preferred_element_type=F32)


def dot_nt(a, b):
    return lax.dot_general(a, b, (((1,), (1,)), ((), ())), preferred_element_type=F32)


def split(v):
    high = v.astype(BF16)
    return high, (v - high.astype(F32)).astype(BF16)


def dot3(a_high, a_low, b_high, b_low):
    return dot(a_high, b_high) + dot(a_high, b_low) + dot(a_low, b_high)


def lanes(col):
    return slice(LANES * col, LANES * (col + 1))


def face_rows(v, node):
    at = 16 * node
    return jnp.concatenate([v[64 * c + at : 64 * c + at + 16] for c in range(3)], axis=0)


def tile_coef(coef_ref, col):
    return coef_ref[col : col + 1, :]


def sides():
    at_x, at_y = lax.axis_index("gx"), lax.axis_index("gy")
    last_x, last_y = lax.axis_size("gx") - 1, lax.axis_size("gy") - 1
    return at_x % 2 == 0, at_y % 2 == 0, (at_x > 0, at_x < last_x, at_y > 0, at_y < last_y)


def y_traces(w_of, sel_ref):
    ends = []
    for y, rows in ((0, slice(0, 48)), (3, slice(48, 96))):
        high, low = split(jnp.concatenate([w_of(y), w_of(4 + y)], axis=1))
        pick = sel_ref[rows, :]
        ends.append(dot(pick, high) + dot(pick, low))
    return ends


def post(lower_x, upper_x, lower_y, upper_y, sends):
    sx_in, sx_out, sy_in, sy_out = sends
    even_x, even_y, _ = sides()
    sx_in[...] = jnp.where(even_x, upper_x, lower_x)
    sx_out[...] = jnp.where(even_x, lower_x, upper_x)
    sy_in[...] = jnp.where(even_y, upper_y, lower_y)
    sy_out[...] = jnp.where(even_y, lower_y, upper_y)


def edge_traces(w_of, sel_ref):
    lower_x = jnp.concatenate([face_rows(w_of(y), 0) for y in range(4)], axis=1)
    upper_x = jnp.concatenate([face_rows(w_of(4 + y), 3) for y in range(4)], axis=1)
    return (lower_x, upper_x, *y_traces(w_of, sel_ref))


def fetch(pairs, sems):
    copies = [pltpu.make_async_copy(a, b, sems.at[n]) for n, (a, b) in enumerate(pairs)]
    for copy in copies:
        copy.start()
    return copies


def first_kernel(
    rs_hbm, coef_hbm, ori_hbm, sel_hbm, agg_hbm, owner_hbm, stiff_hbm, faces_hbm, pt_hbm,
    r_ref, d_ref, coef_ref, ori_ref, sel_ref, agg_ref, owner_ref, stiff_ref, faces_ref, pt_ref,
    sx_in, sx_out, sy_in, sy_out, rs_ref, sems,
):
    pieces = [pl.ds(512 * c, 512) for c in range(3)]
    copies = fetch(
        [(rs_hbm.at[piece], rs_ref.at[piece]) for piece in pieces]
        + [
            (coef_hbm, coef_ref),
            (sel_hbm, sel_ref),
            (agg_hbm, agg_ref),
            (owner_hbm, owner_ref),
            (ori_hbm, ori_ref),
            (stiff_hbm, stiff_ref),
            (pt_hbm, pt_ref),
            (faces_hbm, faces_ref),
        ],
        sems,
    )
    for c in range(3):
        copies[c].wait()
        rows = slice(64 * c, 64 * (c + 1))
        for col in range(COLS):
            v = rs_ref[pl.ds(512 * c + col, 64, stride=COLS), :]
            r_ref[rows, lanes(col)] = v
            d_ref[rows, lanes(col)] = v * (1.0 / THETA)
    for copy in copies[3:5]:
        copy.wait()
    post(
        *edge_traces(lambda col: d_ref[:, lanes(col)] * tile_coef(coef_ref, col), sel_ref),
        (sx_in, sx_out, sy_in, sy_out),
    )
    for copy in copies[5:]:
        copy.wait()


def stacked(v):
    high = v.astype(BF16).astype(F32)
    return jnp.concatenate([high, v - high], axis=0).astype(BF16)


def stacked3(v):
    high = v.astype(BF16).astype(F32)
    return jnp.concatenate([high, v - high, high], axis=0).astype(BF16)


def beside(v):
    high, low = split(v)
    return jnp.concatenate([high, high, low], axis=1)


def slot_table(agg_ref, owner_ref, te_ref):
    owner = owner_ref[...]
    owner_hot = lax.broadcasted_iota(jnp.int32, (OWNERS, AGG), 0) == owner
    before = lax.broadcasted_iota(jnp.int32, (AGG, AGG), 0) < lax.broadcasted_iota(
        jnp.int32, (AGG, AGG), 1
    )
    counts = dot(owner_hot.astype(BF16), before.astype(BF16))
    slot = jnp.sum(jnp.where(owner_hot, counts, 0.0), axis=0, keepdims=True)
    first = lax.broadcasted_iota(jnp.int32, (8, AGG), 0) == 0
    table = jnp.where(first, owner.astype(F32), slot).astype(BF16)
    for col in range(COLS):
        member = lax.broadcasted_iota(jnp.int32, (AGG, LANES), 0) == agg_ref[col : col + 1, :]
        found = dot(table, member.astype(BF16))
        te_ref[col : col + 1, :] = (found[0:1] * float(CAP) + found[1:2]).astype(jnp.int32)


def one_hots(te_ref, hot_ref, tall_ref):
    for col in range(COLS):
        te = te_ref[col : col + 1, :]
        hot = lax.broadcasted_iota(jnp.int32, (OWNERS * CAP, LANES), 0) == te
        hot = hot.astype(F32).astype(BF16)
        hot_ref[:, lanes(col)] = hot
        tall_ref[lanes(col), :] = hot.T


def weights_kernel(
    stiff_ref, faces_ref, basis_ref, sel_ref, agg_ref, owner_ref,
    wh_ref, wl_ref, halo_ref, rim_ref, pf_ref, pt_ref, lift_ref, edge_ref, te_ref,
):
    slot_table(agg_ref, owner_ref, te_ref)
    high, low = split(stiff_ref[...])
    wh_ref[:, 0:BLOCK] = high
    wl_ref[:, 0:BLOCK] = low
    pt = basis_ref[...]
    pt_ref[...] = stacked(pt)
    lift = beside(pt.T)
    lift_ref[...] = lift
    edge_ref[0:48, :] = face_rows(lift, 0)
    edge_ref[48:96, :] = face_rows(lift, 3)
    edge_ref[96:192, :] = dot(sel_ref[0:96, :], lift).astype(BF16)
    for piece in range(3):
        high, low = split(faces_ref[192 * piece : 192 * (piece + 1), :].T)
        wh_ref[:, 192 * (piece + 1) : 192 * (piece + 2)] = high
        wl_ref[:, 192 * (piece + 1) : 192 * (piece + 2)] = low
    pt_high, pt_low = split(pt)
    for direction in range(4):
        at = BLOCK + 96 * direction
        high, low = wh_ref[:, at : at + 96], wl_ref[:, at : at + 96]
        stack = jnp.concatenate([high, high, low], axis=1)
        halo_ref[direction] = stack
        pf_ref[direction] = beside(dot3(pt_high, pt_low, high, low))
        if direction < 2:
            rim_ref[direction, 0:48, :] = face_rows(stack, 3 * direction)
            rim_ref[direction, 48:144, :] = dot(sel_ref[0:96, :], stack).astype(BF16)
        else:
            rim_ref[direction, 0:48, :] = face_rows(stack, 0)
            rim_ref[direction, 48:96, :] = face_rows(stack, 3)
            pick = sel_ref[48 * (direction - 2) : 48 * (direction - 1), :]
            rim_ref[direction, 96:144, :] = dot(pick, stack).astype(BF16)


def interior(d_ref, coef_ref, ori_ref, wh_ref, wl_ref, sel_ref, out_ref, xh_ref, xl_ref, t_ref):
    for col in range(COLS):
        high, low = split(d_ref[:, lanes(col)] * tile_coef(coef_ref, col))
        xh_ref[0:BLOCK, lanes(col)] = high
        xl_ref[0:BLOCK, lanes(col)] = low
    lane = lax.broadcasted_iota(jnp.int32, (48, LANES), 1)
    for x_ref in (xh_ref, xl_ref):
        t_ref[...] = dot(sel_ref[...], x_ref[0:BLOCK, :])
        for col in range(COLS):
            x, y = col // 4, col % 4
            for direction in range(6):
                trace = None
                if direction == 0 and x == 1:
                    trace = face_rows(x_ref[0:BLOCK, lanes(col - 4)], 3).astype(F32)
                elif direction == 1 and x == 0:
                    trace = face_rows(x_ref[0:BLOCK, lanes(col + 4)], 0).astype(F32)
                elif direction == 2 and y > 0:
                    trace = t_ref[48:96, lanes(col - 1)]
                elif direction == 3 and y < 3:
                    trace = t_ref[0:48, lanes(col + 1)]
                elif direction == 4:
                    trace = jnp.where(lane == 0, 0.0, pltpu.roll(t_ref[144:192, lanes(col)], 1, 1))
                elif direction == 5:
                    trace = jnp.where(
                        lane == LANES - 1, 0.0, pltpu.roll(t_ref[96:144, lanes(col)], LANES - 1, 1)
                    )
                at = BLOCK + 96 * direction
                if trace is None:
                    x_ref[at : at + 96, lanes(col)] = jnp.zeros((96, LANES), BF16)
                    continue
                row = COLS * direction + col
                picked = ori_ref[row : row + 1, :] == 1
                x_ref[at : at + 48, lanes(col)] = jnp.where(picked, 0.0, trace).astype(BF16)
                x_ref[at + 48 : at + 96, lanes(col)] = jnp.where(picked, trace, 0.0).astype(BF16)
    for half in range(2):
        span = slice(512 * half, 512 * (half + 1))
        out_ref[:, span] = dot3(wh_ref[...], wl_ref[...], xh_ref[:, span], xl_ref[:, span])


def ahead(scales, r_ref, d_ref, part_ref, coef_ref, sel_ref, pres):
    keep, gain = scales

    def w_of(col):
        at = lanes(col)
        step = gain * (r_ref[:, at] - part_ref[:, at])
        if keep:
            step = keep * d_ref[:, at] + step
        return step * tile_coef(coef_ref, col)

    for pre, value in zip(pres, edge_traces(w_of, sel_ref)):
        pre[...] = value


def start_kernel(
    scales, r_ref, d_ref, coef_ref, ori_ref, wh_ref, wl_ref, sel_ref, *rest,
):
    part_ref, *pres, xh_ref, xl_ref, t_ref = rest
    interior(d_ref, coef_ref, ori_ref, wh_ref, wl_ref, sel_ref, part_ref, xh_ref, xl_ref, t_ref)
    ahead(scales, r_ref, d_ref, part_ref, coef_ref, sel_ref, pres)


def lifted_kernel(
    scales, part_ref, r_ref, x_ref, each_ref, coef_ref, ori_ref, wh_ref, wl_ref, sel_ref,
    halo_ref, lift_ref, lx_ref, ux_ref, ly_ref, uy_ref, r_out, x_out, part_out, *rest,
):
    *pres, xh_ref, xl_ref, t_ref, d_ref = rest
    add_halo(d_ref, part_ref, halo_ref, [v[...] for v in (lx_ref, ux_ref, ly_ref, uy_ref)])
    r_out[...] = r_ref[...] - d_ref[...]
    lift = dot(lift_ref[...], stacked3(each_ref[...]))
    d_ref[...] = lift
    x_out[...] = x_ref[...] + lift
    interior(d_ref, coef_ref, ori_ref, wh_ref, wl_ref, sel_ref, part_out, xh_ref, xl_ref, t_ref)
    ahead(scales, r_out, d_ref, part_out, coef_ref, sel_ref, pres)


def halo_stacks(ori_ref, gets):
    gx_in, gx_out, gy_in, gy_out = gets
    even_x, even_y, found = sides()
    stacks = []
    for direction, cols in enumerate(((0, 1, 2, 3), (4, 5, 6, 7), (0, 4), (3, 7))):
        inside, outside, even = (gx_in, gx_out, even_x) if direction < 2 else (gy_in, gy_out, even_y)
        from_outside = even if direction % 2 == 0 else jnp.logical_not(even)
        parts = []
        for n, col in enumerate(cols):
            trace = jnp.where(from_outside, outside[:, lanes(n)], inside[:, lanes(n)])
            trace = jnp.where(found[direction], trace, 0.0)
            row = COLS * direction + col
            picked = ori_ref[row : row + 1, :] == 1
            both = jnp.concatenate(
                [jnp.where(picked, 0.0, trace), jnp.where(picked, trace, 0.0)], axis=0
            )
            high, low = split(both)
            parts.append(jnp.concatenate([high, low, high], axis=0))
        stacks.append(jnp.concatenate(parts, axis=1))
    return stacks


def send_kernel(gain, coef_ref, ori_ref, rim_ref, *rest):
    gets, pres, sends, stacks = rest[0:4], rest[4:8], rest[8:12], rest[12:16]
    values = halo_stacks(ori_ref, gets)
    for stack, value in zip(stacks, values):
        stack[...] = value
    from_x = [dot(rim_ref[n], values[n]) for n in range(2)]
    from_y = [dot(rim_ref[n], values[n]) for n in range(2, 4)]
    lower_x, upper_x, lower_y, upper_y = pres
    xs = []
    for x, pre in enumerate((lower_x, upper_x)):
        cols = []
        for y in range(4):
            halo = from_x[x][0:48, lanes(y)]
            if y in (0, 3):
                halo = halo + from_y[y // 3][48 * x : 48 * x + 48, lanes(x)]
            cols.append(pre[:, lanes(y)] - halo * (gain * tile_coef(coef_ref, 4 * x + y)))
        xs.append(jnp.concatenate(cols, axis=1))
    ys = []
    for end, pre in enumerate((lower_y, upper_y)):
        cols = []
        for x in range(2):
            halo = from_y[end][96:144, lanes(x)]
            halo = halo + from_x[x][48 + 48 * end : 96 + 48 * end, lanes(3 * end)]
            cols.append(pre[:, lanes(x)] - halo * (gain * tile_coef(coef_ref, 4 * x + 3 * end)))
        ys.append(jnp.concatenate(cols, axis=1))
    post(*xs, *ys, sends)


def add_halo(ad_ref, part_ref, halo_ref, values):
    ad_ref[:, 0:512] = part_ref[:, 0:512] + dot(halo_ref[0], values[0])
    ad_ref[:, 512:1024] = part_ref[:, 512:1024] + dot(halo_ref[1], values[1])
    for end in range(2):
        both = dot(halo_ref[2 + end], values[2 + end])
        for x in range(2):
            ad_ref[:, lanes(4 * x + 3 * end)] += both[:, lanes(x)]


def step_kernel(
    scales, onward, then, part_ref, r_ref, d_ref, x_ref, coef_ref, ori_ref, wh_ref, wl_ref, sel_ref,
    halo_ref, lx_ref, ux_ref, ly_ref, uy_ref, *rest,
):
    if then == "hots":
        te_ref, *rest = rest
    elif then == "restrict":
        pt_ref, *rest = rest
    r_out, d_out, x_out, part_out, *outs, xh_ref, xl_ref, t_ref, ad_ref = rest
    add_halo(ad_ref, part_ref, halo_ref, [v[...] for v in (lx_ref, ux_ref, ly_ref, uy_ref)])
    keep, gain = scales
    for col in range(COLS):
        at = lanes(col)
        resid = r_ref[:, at] - ad_ref[:, at]
        step = gain * resid
        if keep:
            step = keep * d_ref[:, at] + step
        r_out[:, at] = resid
        d_out[:, at] = step
        total = x_ref[:, at] + step
        if then == "close":
            x_out[pl.ds(col, BLOCK, stride=COLS), :] = total
        else:
            x_out[:, at] = total
    interior(d_out, coef_ref, ori_ref, wh_ref, wl_ref, sel_ref, part_out, xh_ref, xl_ref, t_ref)
    if onward is not None:
        ahead(onward, r_out, d_out, part_out, coef_ref, sel_ref, outs[0:4])
    if then == "hots":
        one_hots(te_ref, *outs[4:6])
    elif then == "restrict":
        high, low = split(r_out[...] - part_out[...])
        both = dot(pt_ref[...], high)
        outs[0][...] = both[0:CW] + both[CW:] + dot(pt_ref[0:CW, :], low)
    elif then == "close":
        r_out[...] = r_out[...] - part_out[...]


def routed(v, one_hot_ref):
    both = dot(stacked(v), one_hot_ref[...])
    return both[0:CW] + both[CW:]


def last_kernel(
    base_ref, ori_ref, halo_ref, gx_in, gx_out, gy_in, gy_out, r_hbm, out_ref, sems
):
    values = halo_stacks(ori_ref, (gx_in, gx_out, gy_in, gy_out))
    parts = [dot(halo_ref[n], value) for n, value in enumerate(values)]
    copies = []
    for piece in range(3):
        rows = slice(64 * piece, 64 * (piece + 1))
        for col in range(COLS):
            x, y = col // 4, col % 4
            resid = base_ref[rows, lanes(col)] - parts[x][rows, lanes(y)]
            if y in (0, 3):
                resid = resid - parts[2 + y // 3][rows, lanes(x)]
            out_ref[pl.ds(512 * piece + col, 64, stride=COLS), :] = resid
        span = pl.ds(512 * piece, 512)
        copies.append(pltpu.make_async_copy(out_ref.at[span], r_hbm.at[span], sems.at[piece]))
        copies[-1].start()
    for copy in copies:
        copy.wait()


def restrict_kernel(
    pre_ref, ori_ref, pf_ref, tall_ref, gx_in, gx_out, gy_in, gy_out,
    out_ref, lx_ref, ux_ref, ly_ref, uy_ref, rhs_ref,
):
    values = halo_stacks(ori_ref, (gx_in, gx_out, gy_in, gy_out))
    for stack, value in zip((lx_ref, ux_ref, ly_ref, uy_ref), values):
        stack[...] = value
    parts = [dot(pf_ref[n], value) for n, value in enumerate(values)]
    cols = []
    for col in range(COLS):
        x, y = col // 4, col % 4
        part = parts[x][:, lanes(y)]
        if y in (0, 3):
            part = part + parts[2 + y // 3][:, lanes(x)]
        cols.append(part)
    rhs_ref[...] = routed(pre_ref[...] - jnp.concatenate(cols, axis=1), tall_ref)
    group = lax.broadcasted_iota(jnp.int32, (8, LANES), 1) >> 5
    for o in range(OWNERS):
        total = jnp.zeros((8, LANES), F32)
        for q in range(3):
            moved = rhs_ref[8 * q : 8 * q + 8, lanes(o // 4)]
            if q != o % 4:
                moved = pltpu.roll(moved, 32 * ((q - o) % 4), 1)
            total = jnp.where(group == q, moved, total)
        out_ref[o] = total


def row_sums(tiles):
    row = lax.broadcasted_iota(jnp.int32, tiles[0].shape, 0)
    low = row < 4
    tiles = [
        jnp.where(low, p, q) + pltpu.roll(jnp.where(low, q, p), 4, 0)
        for p, q in zip(tiles[:4], tiles[4:])
    ]
    for bit in (2, 1):
        tiles = [
            jnp.where((row & bit) == 0, p + pltpu.roll(p, 8 - bit, 0), q + pltpu.roll(q, bit, 0))
            for p, q in zip(tiles[:bit], tiles[bit:])
        ]
    return tiles[0]


def solve_kernel(rhs_ref, inv_ref, out_ref):
    pad = jnp.zeros((8, CAP), F32)
    for s in range(OWNERS):
        tile = rhs_ref[s]
        parts = [tile[:, CAP * q : CAP * (q + 1)] for q in range(3)]
        rows = []
        for q in range(3):
            tiles = []
            for a in range(8 * q, 8 * q + 8):
                terms = [inv_ref[s, a, 8 * b : 8 * b + 8, :] * parts[b] for b in range(3)]
                tiles.append(terms[0] + terms[1] + terms[2])
            rows.append(row_sums(tiles))
        out_ref[s] = jnp.concatenate([*rows, pad], axis=1)


def lift_kernel(
    sol_in, coef_ref, hot_ref, edge_ref, each_ref, sx_in, sx_out, sy_in, sy_out, sol_ref
):
    group = lax.broadcasted_iota(jnp.int32, (8, LANES), 1) >> 5
    for q in range(3):
        for j in range(8):
            total = jnp.zeros((8, LANES), F32)
            for g in range(4):
                moved = sol_in[4 * j + g]
                if g != q:
                    moved = pltpu.roll(moved, 32 * ((g - q) % 4), 1)
                total = jnp.where(group == g, moved, total)
            sol_ref[8 * q : 8 * q + 8, lanes(j)] = total
    each = routed(sol_ref[...], hot_ref)
    each_ref[...] = each
    stack = stacked3(each)
    sides_of = []
    for n, cols in enumerate(((0, 1, 2, 3), (4, 5, 6, 7), (0, 4), (3, 7))):
        values = jnp.concatenate([stack[:, lanes(col)] for col in cols], axis=1)
        traces = dot(edge_ref[48 * n : 48 * n + 48, :], values)
        scale = jnp.concatenate([tile_coef(coef_ref, col) for col in cols], axis=1)
        sides_of.append(traces * scale)
    post(*sides_of, (sx_in, sx_out, sy_in, sy_out))


def field(*shape, dtype=F32):
    return pltpu.VMEM(shape, dtype)


def call(kernel, outs, args, scratch=(), hbm=(), limit=20, out_space=pltpu.VMEM):
    specs, placed = [], []
    for n, a in enumerate(args):
        space = pltpu.HBM if n in hbm else pltpu.VMEM
        specs.append(pl.BlockSpec(memory_space=space))
        placed.append(pltpu.with_memory_space_constraint(a, space))
    return pl.pallas_call(
        kernel,
        out_shape=outs,
        in_specs=specs,
        out_specs=[pl.BlockSpec(memory_space=out_space)] * len(outs),
        scratch_shapes=list(scratch),
        compiler_params=pltpu.CompilerParams(vmem_limit_bytes=limit << 20),
    )(*placed)


def swap_even(v, axis):
    count = lax.axis_size(axis)
    return lax.ppermute(v, axis, [(i, i ^ 1) for i in range(count)])


def swap_odd(v, axis):
    count = lax.axis_size(axis)
    return lax.ppermute(
        v, axis, [(i, (i + 1 if i % 2 else i - 1) % count) for i in range(count)]
    )


def exchange(sends):
    return (
        swap_even(sends[0], "gx"),
        swap_odd(sends[1], "gx"),
        swap_even(sends[2], "gy"),
        swap_odd(sends[3], "gy"),
    )


SENDS = [field(48, 512), field(48, 512), field(48, 256), field(48, 256)]


def shards(
    right_side,
    coefficient,
    orientation,
    aggregate_map,
    owner_map,
    stiffness,
    face_blocks,
    prolong_basis,
    coarse_inverse,
):
    shape = right_side.shape
    dma = pltpu.SemaphoreType.DMA
    ints = functools.partial(field, dtype=jnp.int32)
    halves = functools.partial(field, dtype=BF16)
    full = field(BLOCK, ELEMS)
    rows = (BLOCK * COLS, LANES)
    r, d, coef, ori, sel, agg, owner, stiff, faces, basis, *sends = call(
        first_kernel,
        [full, full, field(COLS, LANES), ints(6 * COLS, LANES), halves(BLOCK, BLOCK),
         ints(COLS, LANES), ints(1, AGG), field(BLOCK, BLOCK), field(576, BLOCK),
         field(CW, BLOCK), *SENDS],
        [right_side.reshape(rows), coefficient.reshape(COLS, LANES),
         orientation.reshape(6 * COLS, LANES), jnp.asarray(selection()),
         aggregate_map.reshape(COLS, LANES), owner_map.reshape(1, AGG), stiffness,
         jnp.transpose(face_blocks, (0, 1, 3, 2)).reshape(576, BLOCK), prolong_basis.T],
        scratch=[field(*rows), dma((11,))],
        hbm=tuple(range(9)),
    )
    wide, hots = halves(BLOCK, 768), halves(ELEMS, ELEMS)
    wh, wl, halo, rim, pf, pt, lift, edge, te = call(
        weights_kernel,
        [wide, wide, halves(4, BLOCK, 288), halves(4, 144, 288), halves(4, CW, 288),
         halves(2 * CW, BLOCK), halves(BLOCK, 3 * CW), halves(BLOCK, 3 * CW), ints(COLS, LANES)],
        [stiff, faces, basis, sel, agg, owner],
    )

    products = [halves(768, ELEMS), halves(768, ELEMS), full]
    stacks = [halves(288, 512), halves(288, 512), halves(288, 256), halves(288, 256)]
    tables = [coef, ori, wh, wl, sel]

    def step(scales, onward, part, r, d, x, gets, pres, then=None, extra=(), extra_outs=()):
        *sends, lx, ux, ly, uy = call(
            functools.partial(send_kernel, scales[1]),
            [*SENDS, *stacks],
            [coef, ori, rim, *gets, *pres],
        )
        gets = exchange(sends)
        x_out = jax.ShapeDtypeStruct(rows, F32) if then == "close" else full
        r, d, x, part, *outs = call(
            functools.partial(step_kernel, scales, onward, then),
            [full, full, x_out, full, *([] if onward is None else SENDS), *extra_outs],
            [part, r, d, x, *tables, halo, lx, ux, ly, uy, *extra],
            [*products, full],
        )
        return part, r, d, x, gets, outs

    second, third = chebyshev()
    opening = (0.0, 1.0 / THETA)
    gets = exchange(sends)
    part, *pres = call(
        functools.partial(start_kernel, second), [full, *SENDS], [r, d, *tables], products
    )
    part, r, d, x, gets, (*pres, hot, tall) = step(
        second, third, part, r, d, d, gets, pres, "hots", [te], [hots, hots]
    )
    coarse = field(CW, ELEMS)
    part, r, d, x, gets, (pre,) = step(
        third, None, part, r, d, x, gets, pres, "restrict", [pt], [coarse]
    )
    packets = field(OWNERS, 8, LANES)
    rhs, *near = call(
        restrict_kernel, [packets, *stacks], [pre, ori, pf, tall, *gets], [coarse]
    )
    rhs = lax.all_to_all(rhs, "gx", split_axis=0, concat_axis=0, tiled=True)
    inverse = jnp.transpose(coarse_inverse[0], (0, 2, 3, 1))
    sol = call(solve_kernel, [packets], [rhs, inverse])[0]
    sol = lax.all_to_all(sol, "gx", split_axis=0, concat_axis=0, tiled=True)
    each, *sends = call(lift_kernel, [coarse, *SENDS], [sol, coef, hot, edge], [coarse])
    gets = exchange(sends)
    r, x, part, *pres = call(
        functools.partial(lifted_kernel, opening),
        [full, full, full, *SENDS],
        [part, r, x, each, *tables, halo, lift, *near],
        [*products, full],
    )
    part, r, d, x, gets, pres = step(opening, second, part, r, r, x, gets, pres)
    part, r, d, x, gets, pres = step(second, third, part, r, d, x, gets, pres)
    part, r, _, x, gets, _ = step(third, None, part, r, d, x, gets, pres, "close")
    r = call(
        last_kernel,
        [jax.ShapeDtypeStruct(rows, F32)],
        [r, ori, halo, *gets],
        [field(*rows), dma((3,))],
        out_space=pltpu.HBM,
    )[0]
    return x.reshape(shape), r.reshape(shape)


def solution(mesh):
    in_specs = (
        P(None, "gx", "gy", None),
        P("gx", "gy", None),
        P(None, "gx", "gy", None),
        P("gx", "gy", None),
        P(("gx", "gy"), None),
        P(),
        P(),
        P(),
        P(("gx", "gy"), None, None, None, None),
    )
    out_specs = (P(None, "gx", "gy", None), P(None, "gx", "gy", None))
    return jax.shard_map(shards, mesh=mesh, in_specs=in_specs, out_specs=out_specs, check_vma=False)
```

```python
import functools

import jax
import jax.numpy as jnp
import ml_dtypes
import numpy as np
from jax import lax
from jax.experimental import pallas as pl
from jax.experimental.pallas import tpu as pltpu
from jax.sharding import PartitionSpec as P

BLOCK = 192
TRACE = 48
CW = 24
DEGREE = 3
COLS = 8
LANES = 128
ELEMS = COLS * LANES
OWNERS = 32
CAP = 32
AGG = 512

F32 = jnp.float32
BF16 = jnp.bfloat16

THETA = 0.5 * (4.0 + 0.25)
DELTA = 0.5 * (4.0 - 0.25)
SIGMA = THETA / DELTA


def chebyshev():
    rho = 1.0 / SIGMA
    steps = []
    for _ in range(DEGREE - 1):
        rho_new = 1.0 / (2.0 * SIGMA - rho)
        steps.append((rho_new * rho, 2.0 * rho_new / DELTA))
        rho = rho_new
    return steps


def selection():
    sel = np.zeros((192, 192), np.float32)
    t = np.arange(48)
    for group, rows in enumerate(
        (16 * (t // 4) + t % 4, 16 * (t // 4) + t % 4 + 12, 4 * t, 4 * t + 3)
    ):
        sel[48 * group + t, rows] = 1.0
    return sel.astype(ml_dtypes.bfloat16)


def dot(a, b):
    return jnp.dot(a, b, preferred_element_type=F32)


def dot_nt(a, b):
    return lax.dot_general(a, b, (((1,), (1,)), ((), ())), preferred_element_type=F32)


def split(v):
    high = v.astype(BF16)
    return high, (v - high.astype(F32)).astype(BF16)


def dot3(a_high, a_low, b_high, b_low):
    return dot(a_high, b_high) + dot(a_high, b_low) + dot(a_low, b_high)


def lanes(col):
    return slice(LANES * col, LANES * (col + 1))


def face_rows(v, node):
    at = 16 * node
    return jnp.concatenate([v[64 * c + at : 64 * c + at + 16] for c in range(3)], axis=0)


def tile_coef(coef_ref, col):
    return coef_ref[col : col + 1, :]


def sides():
    at_x, at_y = lax.axis_index("gx"), lax.axis_index("gy")
    last_x, last_y = lax.axis_size("gx") - 1, lax.axis_size("gy") - 1
    return at_x % 2 == 0, at_y % 2 == 0, (at_x > 0, at_x < last_x, at_y > 0, at_y < last_y)


def y_traces(w_of, sel_ref):
    ends = []
    for y, rows in ((0, slice(0, 48)), (3, slice(48, 96))):
        high, low = split(jnp.concatenate([w_of(y), w_of(4 + y)], axis=1))
        pick = sel_ref[rows, :]
        ends.append(dot(pick, high) + dot(pick, low))
    return ends


def post(lower_x, upper_x, lower_y, upper_y, sends):
    sx_in, sx_out, sy_in, sy_out = sends
    even_x, even_y, _ = sides()
    sx_in[...] = jnp.where(even_x, upper_x, lower_x)
    sx_out[...] = jnp.where(even_x, lower_x, upper_x)
    sy_in[...] = jnp.where(even_y, upper_y, lower_y)
    sy_out[...] = jnp.where(even_y, lower_y, upper_y)


def edge_traces(w_of, sel_ref):
    lower_x = jnp.concatenate([face_rows(w_of(y), 0) for y in range(4)], axis=1)
    upper_x = jnp.concatenate([face_rows(w_of(4 + y), 3) for y in range(4)], axis=1)
    return (lower_x, upper_x, *y_traces(w_of, sel_ref))


def fetch(pairs, sems):
    copies = [pltpu.make_async_copy(a, b, sems.at[n]) for n, (a, b) in enumerate(pairs)]
    for copy in copies:
        copy.start()
    return copies


def first_kernel(
    rs_hbm, coef_hbm, ori_hbm, sel_hbm, agg_hbm, owner_hbm, stiff_hbm, faces_hbm, pt_hbm,
    r_ref, d_ref, coef_ref, ori_ref, sel_ref, agg_ref, owner_ref, stiff_ref, faces_ref, pt_ref,
    sx_in, sx_out, sy_in, sy_out, rs_ref, sems,
):
    pieces = [pl.ds(512 * c, 512) for c in range(3)]
    copies = fetch(
        [(rs_hbm.at[piece], rs_ref.at[piece]) for piece in pieces]
        + [
            (coef_hbm, coef_ref),
            (sel_hbm, sel_ref),
            (agg_hbm, agg_ref),
            (owner_hbm, owner_ref),
            (ori_hbm, ori_ref),
            (stiff_hbm, stiff_ref),
            (pt_hbm, pt_ref),
            (faces_hbm, faces_ref),
        ],
        sems,
    )
    for c in range(3):
        copies[c].wait()
        rows = slice(64 * c, 64 * (c + 1))
        for col in range(COLS):
            v = rs_ref[pl.ds(512 * c + col, 64, stride=COLS), :]
            r_ref[rows, lanes(col)] = v
            d_ref[rows, lanes(col)] = v * (1.0 / THETA)
    for copy in copies[3:5]:
        copy.wait()
    post(
        *edge_traces(lambda col: d_ref[:, lanes(col)] * tile_coef(coef_ref, col), sel_ref),
        (sx_in, sx_out, sy_in, sy_out),
    )
    for copy in copies[5:]:
        copy.wait()


def stacked(v):
    high = v.astype(BF16).astype(F32)
    return jnp.concatenate([high, v - high], axis=0).astype(BF16)


def stacked3(v):
    high = v.astype(BF16).astype(F32)
    return jnp.concatenate([high, v - high, high], axis=0).astype(BF16)


def beside(v):
    high, low = split(v)
    return jnp.concatenate([high, high, low], axis=1)


def slot_table(agg_ref, owner_ref, te_ref):
    owner = owner_ref[...]
    owner_hot = lax.broadcasted_iota(jnp.int32, (OWNERS, AGG), 0) == owner
    before = lax.broadcasted_iota(jnp.int32, (AGG, AGG), 0) < lax.broadcasted_iota(
        jnp.int32, (AGG, AGG), 1
    )
    counts = dot(owner_hot.astype(BF16), before.astype(BF16))
    slot = jnp.sum(jnp.where(owner_hot, counts, 0.0), axis=0, keepdims=True)
    first = lax.broadcasted_iota(jnp.int32, (8, AGG), 0) == 0
    table = jnp.where(first, owner.astype(F32), slot).astype(BF16)
    for col in range(COLS):
        member = lax.broadcasted_iota(jnp.int32, (AGG, LANES), 0) == agg_ref[col : col + 1, :]
        found = dot(table, member.astype(BF16))
        te_ref[col : col + 1, :] = (found[0:1] * float(CAP) + found[1:2]).astype(jnp.int32)


def one_hots(te_ref, hot_ref, tall_ref):
    for col in range(COLS):
        te = te_ref[col : col + 1, :]
        hot = lax.broadcasted_iota(jnp.int32, (OWNERS * CAP, LANES), 0) == te
        hot = hot.astype(F32).astype(BF16)
        hot_ref[:, lanes(col)] = hot
        tall_ref[lanes(col), :] = hot.T


def weights_kernel(
    stiff_ref, faces_ref, basis_ref, sel_ref, agg_ref, owner_ref,
    wh_ref, wl_ref, halo_ref, rim_ref, pf_ref, pt_ref, lift_ref, edge_ref, te_ref,
):
    slot_table(agg_ref, owner_ref, te_ref)
    high, low = split(stiff_ref[...])
    wh_ref[:, 0:BLOCK] = high
    wl_ref[:, 0:BLOCK] = low
    pt = basis_ref[...]
    pt_ref[...] = stacked(pt)
    lift = beside(pt.T)
    lift_ref[...] = lift
    edge_ref[0:48, :] = face_rows(lift, 0)
    edge_ref[48:96, :] = face_rows(lift, 3)
    edge_ref[96:192, :] = dot(sel_ref[0:96, :], lift).astype(BF16)
    for piece in range(3):
        high, low = split(faces_ref[192 * piece : 192 * (piece + 1), :].T)
        wh_ref[:, 192 * (piece + 1) : 192 * (piece + 2)] = high
        wl_ref[:, 192 * (piece + 1) : 192 * (piece + 2)] = low
    pt_high, pt_low = split(pt)
    for direction in range(4):
        at = BLOCK + 96 * direction
        high, low = wh_ref[:, at : at + 96], wl_ref[:, at : at + 96]
        stack = jnp.concatenate([high, high, low], axis=1)
        halo_ref[direction] = stack
        pf_ref[direction] = beside(dot3(pt_high, pt_low, high, low))
        if direction < 2:
            rim_ref[direction, 0:48, :] = face_rows(stack, 3 * direction)
            rim_ref[direction, 48:144, :] = dot(sel_ref[0:96, :], stack).astype(BF16)
        else:
            rim_ref[direction, 0:48, :] = face_rows(stack, 0)
            rim_ref[direction, 48:96, :] = face_rows(stack, 3)
            pick = sel_ref[48 * (direction - 2) : 48 * (direction - 1), :]
            rim_ref[direction, 96:144, :] = dot(pick, stack).astype(BF16)


def interior(d_ref, coef_ref, ori_ref, wh_ref, wl_ref, sel_ref, out_ref, xh_ref, xl_ref, t_ref):
    for col in range(COLS):
        high, low = split(d_ref[:, lanes(col)] * tile_coef(coef_ref, col))
        xh_ref[0:BLOCK, lanes(col)] = high
        xl_ref[0:BLOCK, lanes(col)] = low
    lane = lax.broadcasted_iota(jnp.int32, (48, LANES), 1)
    for x_ref in (xh_ref, xl_ref):
        t_ref[...] = dot(sel_ref[...], x_ref[0:BLOCK, :])
        for col in range(COLS):
            x, y = col // 4, col % 4
            for direction in range(6):
                trace = None
                if direction == 0 and x == 1:
                    trace = face_rows(x_ref[0:BLOCK, lanes(col - 4)], 3).astype(F32)
                elif direction == 1 and x == 0:
                    trace = face_rows(x_ref[0:BLOCK, lanes(col + 4)], 0).astype(F32)
                elif direction == 2 and y > 0:
                    trace = t_ref[48:96, lanes(col - 1)]
                elif direction == 3 and y < 3:
                    trace = t_ref[0:48, lanes(col + 1)]
                elif direction == 4:
                    trace = jnp.where(lane == 0, 0.0, pltpu.roll(t_ref[144:192, lanes(col)], 1, 1))
                elif direction == 5:
                    trace = jnp.where(
                        lane == LANES - 1, 0.0, pltpu.roll(t_ref[96:144, lanes(col)], LANES - 1, 1)
                    )
                at = BLOCK + 96 * direction
                if trace is None:
                    x_ref[at : at + 96, lanes(col)] = jnp.zeros((96, LANES), BF16)
                    continue
                row = COLS * direction + col
                picked = ori_ref[row : row + 1, :] == 1
                x_ref[at : at + 48, lanes(col)] = jnp.where(picked, 0.0, trace).astype(BF16)
                x_ref[at + 48 : at + 96, lanes(col)] = jnp.where(picked, trace, 0.0).astype(BF16)
    for half in range(2):
        span = slice(512 * half, 512 * (half + 1))
        out_ref[:, span] = dot3(wh_ref[...], wl_ref[...], xh_ref[:, span], xl_ref[:, span])


def ahead(scales, r_ref, d_ref, part_ref, coef_ref, sel_ref, pres):
    keep, gain = scales

    def w_of(col):
        at = lanes(col)
        step = gain * (r_ref[:, at] - part_ref[:, at])
        if keep:
            step = keep * d_ref[:, at] + step
        return step * tile_coef(coef_ref, col)

    for pre, value in zip(pres, edge_traces(w_of, sel_ref)):
        pre[...] = value


def start_kernel(
    scales, r_ref, d_ref, coef_ref, ori_ref, wh_ref, wl_ref, sel_ref, *rest,
):
    part_ref, *pres, xh_ref, xl_ref, t_ref = rest
    interior(d_ref, coef_ref, ori_ref, wh_ref, wl_ref, sel_ref, part_ref, xh_ref, xl_ref, t_ref)
    ahead(scales, r_ref, d_ref, part_ref, coef_ref, sel_ref, pres)


def lifted_kernel(
    scales, part_ref, r_ref, x_ref, each_ref, coef_ref, ori_ref, wh_ref, wl_ref, sel_ref,
    halo_ref, lift_ref, lx_ref, ux_ref, ly_ref, uy_ref, r_out, x_out, part_out, *rest,
):
    *pres, xh_ref, xl_ref, t_ref, d_ref = rest
    add_halo(d_ref, part_ref, halo_ref, [v[...] for v in (lx_ref, ux_ref, ly_ref, uy_ref)])
    r_out[...] = r_ref[...] - d_ref[...]
    lift = dot(lift_ref[...], stacked3(each_ref[...]))
    d_ref[...] = lift
    x_out[...] = x_ref[...] + lift
    interior(d_ref, coef_ref, ori_ref, wh_ref, wl_ref, sel_ref, part_out, xh_ref, xl_ref, t_ref)
    ahead(scales, r_out, d_ref, part_out, coef_ref, sel_ref, pres)


def halo_stacks(ori_ref, gets):
    gx_in, gx_out, gy_in, gy_out = gets
    even_x, even_y, found = sides()
    stacks = []
    for direction, cols in enumerate(((0, 1, 2, 3), (4, 5, 6, 7), (0, 4), (3, 7))):
        inside, outside, even = (gx_in, gx_out, even_x) if direction < 2 else (gy_in, gy_out, even_y)
        from_outside = even if direction % 2 == 0 else jnp.logical_not(even)
        parts = []
        for n, col in enumerate(cols):
            trace = jnp.where(from_outside, outside[:, lanes(n)], inside[:, lanes(n)])
            trace = jnp.where(found[direction], trace, 0.0)
            row = COLS * direction + col
            picked = ori_ref[row : row + 1, :] == 1
            both = jnp.concatenate(
                [jnp.where(picked, 0.0, trace), jnp.where(picked, trace, 0.0)], axis=0
            )
            high, low = split(both)
            parts.append(jnp.concatenate([high, low, high], axis=0))
        stacks.append(jnp.concatenate(parts, axis=1))
    return stacks


def send_kernel(gain, coef_ref, ori_ref, rim_ref, *rest):
    gets, pres, sends, stacks = rest[0:4], rest[4:8], rest[8:12], rest[12:16]
    values = halo_stacks(ori_ref, gets)
    for stack, value in zip(stacks, values):
        stack[...] = value
    from_x = [dot(rim_ref[n], values[n]) for n in range(2)]
    from_y = [dot(rim_ref[n], values[n]) for n in range(2, 4)]
    lower_x, upper_x, lower_y, upper_y = pres
    xs = []
    for x, pre in enumerate((lower_x, upper_x)):
        cols = []
        for y in range(4):
            halo = from_x[x][0:48, lanes(y)]
            if y in (0, 3):
                halo = halo + from_y[y // 3][48 * x : 48 * x + 48, lanes(x)]
            cols.append(pre[:, lanes(y)] - halo * (gain * tile_coef(coef_ref, 4 * x + y)))
        xs.append(jnp.concatenate(cols, axis=1))
    ys = []
    for end, pre in enumerate((lower_y, upper_y)):
        cols = []
        for x in range(2):
            halo = from_y[end][96:144, lanes(x)]
            halo = halo + from_x[x][48 + 48 * end : 96 + 48 * end, lanes(3 * end)]
            cols.append(pre[:, lanes(x)] - halo * (gain * tile_coef(coef_ref, 4 * x + 3 * end)))
        ys.append(jnp.concatenate(cols, axis=1))
    post(*xs, *ys, sends)


def add_halo(ad_ref, part_ref, halo_ref, values):
    ad_ref[:, 0:512] = part_ref[:, 0:512] + dot(halo_ref[0], values[0])
    ad_ref[:, 512:1024] = part_ref[:, 512:1024] + dot(halo_ref[1], values[1])
    for end in range(2):
        both = dot(halo_ref[2 + end], values[2 + end])
        for x in range(2):
            ad_ref[:, lanes(4 * x + 3 * end)] += both[:, lanes(x)]


def step_kernel(
    scales, onward, then, part_ref, r_ref, d_ref, x_ref, coef_ref, ori_ref, wh_ref, wl_ref, sel_ref,
    halo_ref, lx_ref, ux_ref, ly_ref, uy_ref, *rest,
):
    if then == "hots":
        te_ref, *rest = rest
    elif then == "restrict":
        pt_ref, *rest = rest
    if then == "close":
        r_out, x_hbm, xh_ref, xl_ref, t_ref, ad_ref, d_out, part_out, x_out, sems = rest
        outs = ()
    elif then == "restrict":
        r_out, x_out, part_out, *outs, xh_ref, xl_ref, t_ref, ad_ref, d_out = rest
    else:
        r_out, d_out, x_out, part_out, *outs, xh_ref, xl_ref, t_ref, ad_ref = rest
    add_halo(ad_ref, part_ref, halo_ref, [v[...] for v in (lx_ref, ux_ref, ly_ref, uy_ref)])
    keep, gain = scales
    for col in range(COLS):
        at = lanes(col)
        resid = r_ref[:, at] - ad_ref[:, at]
        step = gain * resid
        if keep:
            step = keep * d_ref[:, at] + step
        r_out[:, at] = resid
        d_out[:, at] = step
        total = x_ref[:, at] + step
        if then == "close":
            x_out[pl.ds(col, BLOCK, stride=COLS), :] = total
        else:
            x_out[:, at] = total
    if then == "close":
        leaving = pltpu.make_async_copy(x_out, x_hbm, sems.at[0])
        leaving.start()
    interior(d_out, coef_ref, ori_ref, wh_ref, wl_ref, sel_ref, part_out, xh_ref, xl_ref, t_ref)
    if onward is not None:
        ahead(onward, r_out, d_out, part_out, coef_ref, sel_ref, outs[0:4])
    if then == "hots":
        one_hots(te_ref, *outs[4:6])
    elif then == "restrict":
        high, low = split(r_out[...] - part_out[...])
        both = dot(pt_ref[...], high)
        outs[0][...] = both[0:CW] + both[CW:] + dot(pt_ref[0:CW, :], low)
    elif then == "close":
        r_out[...] = r_out[...] - part_out[...]
        leaving.wait()


def routed(v, one_hot_ref):
    both = dot(stacked(v), one_hot_ref[...])
    return both[0:CW] + both[CW:]


def last_kernel(
    base_ref, ori_ref, halo_ref, gx_in, gx_out, gy_in, gy_out, r_hbm, out_ref, sems
):
    values = halo_stacks(ori_ref, (gx_in, gx_out, gy_in, gy_out))
    parts = [dot(halo_ref[n], value) for n, value in enumerate(values)]
    copies = []
    for piece in range(3):
        rows = slice(64 * piece, 64 * (piece + 1))
        for col in range(COLS):
            x, y = col // 4, col % 4
            resid = base_ref[rows, lanes(col)] - parts[x][rows, lanes(y)]
            if y in (0, 3):
                resid = resid - parts[2 + y // 3][rows, lanes(x)]
            out_ref[pl.ds(512 * piece + col, 64, stride=COLS), :] = resid
        span = pl.ds(512 * piece, 512)
        copies.append(pltpu.make_async_copy(out_ref.at[span], r_hbm.at[span], sems.at[piece]))
        copies[-1].start()
    for copy in copies:
        copy.wait()


def restrict_kernel(
    pre_ref, ori_ref, pf_ref, tall_ref, gx_in, gx_out, gy_in, gy_out,
    out_ref, lx_ref, ux_ref, ly_ref, uy_ref, rhs_ref,
):
    values = halo_stacks(ori_ref, (gx_in, gx_out, gy_in, gy_out))
    for stack, value in zip((lx_ref, ux_ref, ly_ref, uy_ref), values):
        stack[...] = value
    parts = [dot(pf_ref[n], value) for n, value in enumerate(values)]
    cols = []
    for col in range(COLS):
        x, y = col // 4, col % 4
        part = parts[x][:, lanes(y)]
        if y in (0, 3):
            part = part + parts[2 + y // 3][:, lanes(x)]
        cols.append(part)
    rhs_ref[...] = routed(pre_ref[...] - jnp.concatenate(cols, axis=1), tall_ref)
    group = lax.broadcasted_iota(jnp.int32, (8, LANES), 1) >> 5
    for o in range(OWNERS):
        total = jnp.zeros((8, LANES), F32)
        for q in range(3):
            moved = rhs_ref[8 * q : 8 * q + 8, lanes(o // 4)]
            if q != o % 4:
                moved = pltpu.roll(moved, 32 * ((q - o) % 4), 1)
            total = jnp.where(group == q, moved, total)
        out_ref[o] = total


def row_sums(tiles):
    row = lax.broadcasted_iota(jnp.int32, tiles[0].shape, 0)
    low = row < 4
    tiles = [
        jnp.where(low, p, q) + pltpu.roll(jnp.where(low, q, p), 4, 0)
        for p, q in zip(tiles[:4], tiles[4:])
    ]
    for bit in (2, 1):
        tiles = [
            jnp.where((row & bit) == 0, p + pltpu.roll(p, 8 - bit, 0), q + pltpu.roll(q, bit, 0))
            for p, q in zip(tiles[:bit], tiles[bit:])
        ]
    return tiles[0]


def solve_kernel(rhs_ref, inv_ref, out_ref):
    pad = jnp.zeros((8, CAP), F32)
    for s in range(OWNERS):
        tile = rhs_ref[s]
        parts = [tile[:, CAP * q : CAP * (q + 1)] for q in range(3)]
        rows = []
        for q in range(3):
            tiles = []
            for a in range(8 * q, 8 * q + 8):
                terms = [inv_ref[s, a, 8 * b : 8 * b + 8, :] * parts[b] for b in range(3)]
                tiles.append(terms[0] + terms[1] + terms[2])
            rows.append(row_sums(tiles))
        out_ref[s] = jnp.concatenate([*rows, pad], axis=1)


def lift_kernel(
    sol_in, coef_ref, hot_ref, edge_ref, each_ref, sx_in, sx_out, sy_in, sy_out, sol_ref
):
    group = lax.broadcasted_iota(jnp.int32, (8, LANES), 1) >> 5
    for q in range(3):
        for j in range(8):
            total = jnp.zeros((8, LANES), F32)
            for g in range(4):
                moved = sol_in[4 * j + g]
                if g != q:
                    moved = pltpu.roll(moved, 32 * ((g - q) % 4), 1)
                total = jnp.where(group == g, moved, total)
            sol_ref[8 * q : 8 * q + 8, lanes(j)] = total
    each = routed(sol_ref[...], hot_ref)
    each_ref[...] = each
    stack = stacked3(each)
    sides_of = []
    for n, cols in enumerate(((0, 1, 2, 3), (4, 5, 6, 7), (0, 4), (3, 7))):
        values = jnp.concatenate([stack[:, lanes(col)] for col in cols], axis=1)
        traces = dot(edge_ref[48 * n : 48 * n + 48, :], values)
        scale = jnp.concatenate([tile_coef(coef_ref, col) for col in cols], axis=1)
        sides_of.append(traces * scale)
    post(*sides_of, (sx_in, sx_out, sy_in, sy_out))


def field(*shape, dtype=F32):
    return pltpu.VMEM(shape, dtype)


def call(kernel, outs, args, scratch=(), hbm=(), limit=20, out_space=pltpu.VMEM):
    specs, placed = [], []
    for n, a in enumerate(args):
        space = pltpu.HBM if n in hbm else pltpu.VMEM
        specs.append(pl.BlockSpec(memory_space=space))
        placed.append(pltpu.with_memory_space_constraint(a, space))
    return pl.pallas_call(
        kernel,
        out_shape=outs,
        in_specs=specs,
        out_specs=[
            pl.BlockSpec(memory_space=out_space[n] if isinstance(out_space, tuple) else out_space)
            for n in range(len(outs))
        ],
        scratch_shapes=list(scratch),
        compiler_params=pltpu.CompilerParams(vmem_limit_bytes=limit << 20),
    )(*placed)


def swap_even(v, axis):
    count = lax.axis_size(axis)
    return lax.ppermute(v, axis, [(i, i ^ 1) for i in range(count)])


def swap_odd(v, axis):
    count = lax.axis_size(axis)
    return lax.ppermute(
        v, axis, [(i, (i + 1 if i % 2 else i - 1) % count) for i in range(count)]
    )


def exchange(sends):
    return (
        swap_even(sends[0], "gx"),
        swap_odd(sends[1], "gx"),
        swap_even(sends[2], "gy"),
        swap_odd(sends[3], "gy"),
    )


SENDS = [field(48, 512), field(48, 512), field(48, 256), field(48, 256)]


def shards(
    right_side,
    coefficient,
    orientation,
    aggregate_map,
    owner_map,
    stiffness,
    face_blocks,
    prolong_basis,
    coarse_inverse,
):
    shape = right_side.shape
    dma = pltpu.SemaphoreType.DMA
    ints = functools.partial(field, dtype=jnp.int32)
    halves = functools.partial(field, dtype=BF16)
    full = field(BLOCK, ELEMS)
    rows = (BLOCK * COLS, LANES)
    r, d, coef, ori, sel, agg, owner, stiff, faces, basis, *sends = call(
        first_kernel,
        [full, full, field(COLS, LANES), ints(6 * COLS, LANES), halves(BLOCK, BLOCK),
         ints(COLS, LANES), ints(1, AGG), field(BLOCK, BLOCK), field(576, BLOCK),
         field(CW, BLOCK), *SENDS],
        [right_side.reshape(rows), coefficient.reshape(COLS, LANES),
         orientation.reshape(6 * COLS, LANES), jnp.asarray(selection()),
         aggregate_map.reshape(COLS, LANES), owner_map.reshape(1, AGG), stiffness,
         jnp.transpose(face_blocks, (0, 1, 3, 2)).reshape(576, BLOCK), prolong_basis.T],
        scratch=[field(*rows), dma((11,))],
        hbm=tuple(range(9)),
    )
    wide, hots = halves(BLOCK, 768), halves(ELEMS, ELEMS)
    wh, wl, halo, rim, pf, pt, lift, edge, te = call(
        weights_kernel,
        [wide, wide, halves(4, BLOCK, 288), halves(4, 144, 288), halves(4, CW, 288),
         halves(2 * CW, BLOCK), halves(BLOCK, 3 * CW), halves(BLOCK, 3 * CW), ints(COLS, LANES)],
        [stiff, faces, basis, sel, agg, owner],
    )

    products = [halves(768, ELEMS), halves(768, ELEMS), full]
    stacks = [halves(288, 512), halves(288, 512), halves(288, 256), halves(288, 256)]
    tables = [coef, ori, wh, wl, sel]

    def step(scales, onward, part, r, d, x, gets, pres, then=None, extra=(), extra_outs=()):
        *sends, lx, ux, ly, uy = call(
            functools.partial(send_kernel, scales[1]),
            [*SENDS, *stacks],
            [coef, ori, rim, *gets, *pres],
        )
        gets = exchange(sends)
        scratch = [*products, full]
        spaces = pltpu.VMEM
        if then == "close":
            shapes = [full, jax.ShapeDtypeStruct(rows, F32)]
            scratch = [*scratch, full, full, field(*rows), dma((1,))]
            spaces = (pltpu.VMEM, pltpu.HBM)
        elif then == "restrict":
            shapes, scratch = [full, full, full, *extra_outs], [*scratch, full]
        else:
            shapes = [full, full, full, full, *SENDS, *extra_outs]
        outs = call(
            functools.partial(step_kernel, scales, onward, then),
            shapes,
            [part, r, d, x, *tables, halo, lx, ux, ly, uy, *extra],
            scratch,
            out_space=spaces,
        )
        if then in ("close", "restrict"):
            return *outs, gets
        r, d, x, part, *outs = outs
        return part, r, d, x, gets, outs

    second, third = chebyshev()
    opening = (0.0, 1.0 / THETA)
    gets = exchange(sends)
    part, *pres = call(
        functools.partial(start_kernel, second), [full, *SENDS], [r, d, *tables], products
    )
    part, r, d, x, gets, (*pres, hot, tall) = step(
        second, third, part, r, d, d, gets, pres, "hots", [te], [hots, hots]
    )
    coarse = field(CW, ELEMS)
    r, x, part, pre, gets = step(
        third, None, part, r, d, x, gets, pres, "restrict", [pt], [coarse]
    )
    packets = field(OWNERS, 8, LANES)
    rhs, *near = call(
        restrict_kernel, [packets, *stacks], [pre, ori, pf, tall, *gets], [coarse]
    )
    rhs = lax.all_to_all(rhs, "gx", split_axis=0, concat_axis=0, tiled=True)
    inverse = jnp.transpose(coarse_inverse[0], (0, 2, 3, 1))
    sol = call(solve_kernel, [packets], [rhs, inverse])[0]
    sol = lax.all_to_all(sol, "gx", split_axis=0, concat_axis=0, tiled=True)
    each, *sends = call(lift_kernel, [coarse, *SENDS], [sol, coef, hot, edge], [coarse])
    gets = exchange(sends)
    r, x, part, *pres = call(
        functools.partial(lifted_kernel, opening),
        [full, full, full, *SENDS],
        [part, r, x, each, *tables, halo, lift, *near],
        [*products, full],
    )
    part, r, d, x, gets, pres = step(opening, second, part, r, r, x, gets, pres)
    part, r, d, x, gets, pres = step(second, third, part, r, d, x, gets, pres)
    r, x, gets = step(third, None, part, r, d, x, gets, pres, "close")
    r = call(
        last_kernel,
        [jax.ShapeDtypeStruct(rows, F32)],
        [r, ori, halo, *gets],
        [field(*rows), dma((3,))],
        out_space=pltpu.HBM,
    )[0]
    return x.reshape(shape), r.reshape(shape)


def solution(mesh):
    in_specs = (
        P(None, "gx", "gy", None),
        P("gx", "gy", None),
        P(None, "gx", "gy", None),
        P("gx", "gy", None),
        P(("gx", "gy"), None),
        P(),
        P(),
        P(),
        P(("gx", "gy"), None, None, None, None),
    )
    out_specs = (P(None, "gx", "gy", None), P(None, "gx", "gy", None))
    return jax.shard_map(shards, mesh=mesh, in_specs=in_specs, out_specs=out_specs, check_vma=False)
```
